32 devices in a mesh: dp: 2 (over core), expert: 4 (over y, x), mp: 4 (over z).
Axes of the slice: x: 2, y: 2, z: 4, core: 2. Of those that a mesh axis runs over, the one named last changes fastest.
Arguments:
- hidden: bfloat16 [3072, 2, 7168], P(('dp', 'expert'), None, 'mp'), may hold values from -6 to 6
- cotangent: bfloat16 [3072, 2048], P(('dp', 'expert'), 'mp'), may hold values from -6 to 6
- routes: int32 [3072, 2], P(('dp', 'expert')), may hold values from 0 to 3, all different within a row; in each aligned block of 384 rows (0 to 383, 384 to 767, ...) at most 288 rows name the same one
- combine: float32 [3072, 2], P(('dp', 'expert')), may hold values from 0.1 to 0.9
- block_pair: int32 [8, 12], P(('dp', 'expert')), may hold values from 0 to 11, each once within a row
- lengths: int32 [8, 12], P(('dp', 'expert')), may hold values from 4 to 32
- log_ratio: float32 [8, 12], P(('dp', 'expert')), may hold values from -30 to 30
Outputs:
- grad_down: float32 [4, 7168, 2048], P('expert', ('mp', 'dp'))
- expert_load: float32 [4], replicated
The draws below stay inside these ranges and needn't reach their ends.
Inputs may be any that keep to these rules, and one draw needn't show every extreme that they name: `routes`: each row names 2 different experts; in each aligned block of 384 rows (the rows of one device) no expert is named more than 288 times, and in some blocks one expert is named exactly 288 times. `block_pair`: each row holds every number of 0 to 11 once; value v marks the chosen response of the row's pair v // 2 if v is even, its rejected response if v is odd.
All inputs are finite; a program needn't handle non-finite values.
Results may differ from the reference program's by a relative error of at most 0.0029.
Values may be sent and summed in bfloat16 or wider, within the bound.
A program may use at most 128 MiB of HBM per device.

```python
import math
import jax
import jax.numpy as jnp
import numpy as np
from jax import lax

FFW = 7168
DW = 2048
EXPERTS = 4
TOP = 2
LEN = 32
PAIRS_DEV = 6
TOK_DEV = 384
MOST = 288
GROUPS = 8
TOKENS = 3072
N_DP = 2
N_EXPERT = 4


def draw_lengths(key, part):
    first, second, third = jax.random.split(jax.random.fold_in(key, 17), 3)
    lowest = LEN // 8
    blocks = 2 * PAIRS_DEV
    row_cap = jax.random.randint(first, (GROUPS, 1), lowest, LEN + 1)
    values = jax.random.randint(second, (GROUPS, blocks), lowest, row_cap + 1)
    marked = jax.random.randint(third, (), 0, GROUPS)
    values = values.at[marked, 0].set(LEN)
    values = values.at[(marked + 1) % GROUPS, 1].set(lowest)
    return values.astype(jnp.int32)


def levels(key, dims, cuts, low, high):
    loudness = 1.0
    for axis_at, shards_of in cuts:
        steps = jax.random.uniform(jax.random.fold_in(jax.random.fold_in(key, 6), axis_at), (shards_of,), jnp.float32, low / len(cuts), high / len(cuts))
        loudness = loudness * jnp.repeat(jnp.exp(steps), dims[axis_at] // shards_of).reshape((-1,) + (1,) * (len(dims) - 1 - axis_at))
    return loudness


def deal_out(own_key, own, number, rows, number_of, top, limit, slope):
    sequence = jax.random.permutation(own_key, number_of)
    heavy_load, ordinary = load_shares(number_of, rows * top, limit, slope, True), load_shares(number_of, rows * top, limit, slope, False)
    places = jnp.arange(number_of)

    def named(tallies, rotation):
        used = int((tallies > 0).sum())
        fixed = max(1, used // 4)
        passed = fixed + (places - fixed + rotation * (used - fixed)) % max(1, number_of - fixed)
        return jnp.zeros((number_of,), jnp.int32).at[sequence[jnp.where(places < fixed, places, passed)]].set(jnp.asarray(tallies, jnp.int32))

    tallies = jnp.where(number % 4 == 0, named(heavy_load, number // 4), named(ordinary, number - number // 4 - 1))
    mixed = jax.random.permutation(jax.random.fold_in(own, 3), number_of)
    donor, sink = mixed[0:number_of // 2 * 2:2], mixed[1:number_of // 2 * 2:2]
    slack = jnp.minimum(tallies[donor] - 1, limit - tallies[sink]) // 2
    slack = jnp.where((donor == sequence[0]) | (sink == sequence[0]) | (tallies[sink] == 0), 0, jnp.maximum(slack, 0))
    passed = jax.random.randint(jax.random.fold_in(own, 4), (number_of // 2,), 0, 1 << 20) % (slack + 1)
    tallies = tallies.at[donor].add(-passed).at[sink].add(passed)
    members = jnp.searchsorted(jnp.cumsum(tallies), jnp.arange(rows * top), side="right").astype(jnp.int32)
    listing = members.reshape(top, rows).T
    listing = listing[jax.random.permutation(jax.random.fold_in(own, 1), rows)]
    rotation = jax.random.randint(jax.random.fold_in(own, 2), (rows, 1), 0, top)
    return jnp.take_along_axis(listing, (jnp.arange(top)[None, :] + rotation) % top, axis=1)


def load_shares(number_of, total, limit, slope, full):
    portions = [(1 << 20) // math.isqrt(standing ** slope) + 1 for standing in range(1, number_of + 1)]
    largest = limit if full else min(limit, max(-(-total // number_of), total * portions[0] // sum(portions)))
    least = 1 if total - largest >= number_of - 1 else 0
    counts, surplus = [largest] + [least] * (number_of - 1), total - largest - least * (number_of - 1)
    while surplus > 0:
        movable = [i for i in range(1, number_of) if counts[i] < largest] or [i for i in range(1, number_of) if counts[i] < limit]
        whole, remaining = sum([portions[i] for i in movable]), surplus
        for i in movable:
            addition = min(limit - counts[i], max(1, remaining * portions[i] // whole), surplus)
            counts[i] = counts[i] + addition
            surplus = surplus - addition
    return np.array(counts)


def centred(rng, shape, scale, bound, cuts=(), held_as=jnp.bfloat16):
    level = levels(rng, shape, cuts, -0.22, 0.18) if cuts else 1.0
    values = jax.random.normal(rng, shape, jnp.float32) * scale * level
    return jnp.minimum(jnp.maximum(values, -bound), bound).astype(held_as)


def setup_inputs(seed: int = 0) -> dict:
    splits = jax.random.split(jax.random.key(seed), 8)
    hidden = centred(splits[0], (TOKENS, TOP, FFW), 1.0, 6.0, ((0, 8), (2, 4)))
    cotangent = centred(splits[1], (TOKENS, DW), 1.0, 6.0, ((0, 8), (1, 4)))
    routes_keys = jax.random.split(jax.random.fold_in(splits[2], 1), TOKENS // TOK_DEV)
    routes_turns = jax.random.permutation(jax.random.fold_in(splits[2], 3), TOKENS // TOK_DEV)
    routes = jax.vmap(lambda own, number: deal_out(jax.random.fold_in(splits[2], 2), own, number, TOK_DEV, EXPERTS, TOP, MOST, 2))(routes_keys, routes_turns).reshape((TOKENS, TOP))
    combine = jnp.clip(0.1 + 0.79999997 * jax.random.uniform(splits[3], (TOKENS, TOP), jnp.float32) ** levels(splits[3], (TOKENS, TOP), ((0, 8),), -0.2, 0.2), 0.1, 0.9)
    block_pair = jax.vmap(lambda own: jax.random.permutation(own, 2 * PAIRS_DEV))(jax.random.split(splits[4], GROUPS)).reshape((GROUPS, 2 * PAIRS_DEV)).astype(jnp.int32)
    lengths = draw_lengths(jax.random.fold_in(splits[7], 71), 0)
    log_ratio = jnp.clip(jax.random.uniform(splits[6], (GROUPS, 2 * PAIRS_DEV), jnp.float32, -30.0, 30.0) * levels(splits[6], (GROUPS, 2 * PAIRS_DEV), ((0, 8),), -0.4, 0.0), -30.0, 30.0)
    return dict(hidden=hidden, cotangent=cotangent, routes=routes, combine=combine, block_pair=block_pair, lengths=lengths, log_ratio=log_ratio)


beta_scale = 0.1


def token_weights(combine, block_pair, lengths, log_ratio, block_len):
    blocks = block_pair.shape[1]
    labels = jnp.arange(blocks, dtype=jnp.int32)
    matches = block_pair[:, :, None] == labels[None, None, :]
    by_label = jnp.sum(jnp.where(matches, log_ratio[:, :, None], 0.0), axis=1)
    margin = by_label[:, 0::2] - by_label[:, 1::2]
    pair_coef = beta_scale * jax.nn.sigmoid(-beta_scale * margin)
    owners = block_pair // 2
    pair_ids = jnp.arange(blocks // 2, dtype=jnp.int32)
    picked = owners[:, :, None] == pair_ids[None, None, :]
    block_coef = jnp.sum(jnp.where(picked, pair_coef[:, None, :], 0.0), axis=2)
    block_weight = jnp.where(block_pair % 2 == 0, -block_coef, block_coef)
    position = jnp.arange(block_len, dtype=jnp.int32)
    within = position[None, None, :] < lengths[:, :, None]
    per_token = jnp.where(within, block_weight[:, :, None], 0.0).reshape(-1)
    return combine * per_token[:, None], within.reshape(-1)


def reference(hidden, cotangent, routes, combine, block_pair, lengths, log_ratio):
    weight, within = token_weights(combine, block_pair, lengths, log_ratio, LEN)
    labels = jnp.arange(EXPERTS, dtype=jnp.int32)
    routed = routes[:, :, None] == labels[None, None, :]
    expert_load = jnp.sum(jnp.where(routed & within[:, None, None], 1.0, 0.0), axis=(0, 1)).astype(jnp.float32)
    scaled = (weight[:, :, None] * cotangent[:, None, :].astype(jnp.float32)).astype(jnp.bfloat16)
    slice_rows = TOK_DEV * N_EXPERT * TOP
    room = N_EXPERT * MOST
    hidden_rows = hidden.reshape(N_DP, slice_rows, FFW)
    scaled_rows = scaled.reshape(N_DP, slice_rows, DW)
    route_rows = routes.reshape(N_DP, slice_rows)

    def one_expert(operands, expert_idx):
        slice_hidden, slice_scaled, slice_routes = operands
        chosen = slice_routes == expert_idx
        rank_of = jnp.cumsum(chosen.astype(jnp.int32)) - 1
        target = jnp.where(chosen, rank_of, room)
        source = jnp.zeros((room,), jnp.int32).at[target].set(jnp.arange(slice_rows, dtype=jnp.int32), mode="drop")
        filled = jnp.zeros((room,), jnp.int32).at[target].set(1, mode="drop")
        packed_h = jnp.take(slice_hidden, source, axis=0).astype(jnp.float32)
        packed_s = jnp.where(filled[:, None] > 0, jnp.take(slice_scaled, source, axis=0).astype(jnp.float32), 0.0)
        return jnp.dot(packed_h.T, packed_s, preferred_element_type=jnp.float32)

    def add_slice(running, operands):
        partial_sum = lax.map(lambda expert_idx: one_expert(operands, expert_idx), labels)
        return running + partial_sum, None

    start_total = jnp.zeros((EXPERTS, FFW, DW), jnp.float32)
    grad_down, unused = lax.scan(add_slice, start_total, (hidden_rows, scaled_rows, route_rows))
    return grad_down, expert_load
```

```python
import functools

import jax
import jax.numpy as jnp
from jax import lax
from jax.experimental import pallas as pl
from jax.experimental.pallas import tpu as pltpu
from jax.sharding import PartitionSpec as P

EXP_DEV = 1
LEN = 32
LANES = 128
VMEM_ROOM = 48 * 1024 * 1024
VMEM_MOST = 67043328
MESH = pl.DeviceIdType.MESH


beta_scale = 0.1


def token_factors(block_pair, lengths, log_ratio, block_len):
    blocks = block_pair.shape[1]
    labels = jnp.arange(blocks, dtype=jnp.int32)
    matches = block_pair[:, :, None] == labels[None, None, :]
    by_label = jnp.sum(jnp.where(matches, log_ratio[:, :, None], 0.0), axis=1)
    margin = by_label[:, 0::2] - by_label[:, 1::2]
    pair_coef = beta_scale * jax.nn.sigmoid(-beta_scale * margin)
    owners = block_pair // 2
    pair_ids = jnp.arange(blocks // 2, dtype=jnp.int32)
    picked = owners[:, :, None] == pair_ids[None, None, :]
    block_coef = jnp.sum(jnp.where(picked, pair_coef[:, None, :], 0.0), axis=2)
    block_weight = jnp.where(block_pair % 2 == 0, -block_coef, block_coef)
    position = jnp.arange(block_len, dtype=jnp.int32)
    within = position[None, None, :] < lengths[:, :, None]
    per_token = jnp.where(within, block_weight[:, :, None], 0.0).reshape(-1)
    return per_token, within.reshape(-1)


def exchange_kernel(
    dims, h_hbm, cot_hbm, routes_hbm, combine_hbm, pair_hbm, len_hbm, ratio_hbm,
    acc_a, acc_b, load_ref,
    h_in, cot_ref, routes_ref, combine_ref, pair_ref, len_ref, ratio_ref,
    hr, sa, sb, hs, sas, sbs, cotb, lbuf, relay_h, relay_a, relay_b, ht, ht_end, in_sem,
    xa_s, a_r, ra_s, ra_r, up_s, dn_s, dd_s, cb_s, cb_r, xb_s, b_r, rb_s, rb_r, db_s,
    h_s, h_r, hp_s, hp_r, rh_s, rh_r, l_s, l_r,
):
    nd, ne, nm, most, ca, cb = dims
    d, e, m = lax.axis_index("dp"), lax.axis_index("expert"), lax.axis_index("mp")
    toks, top, ff = h_in.shape
    half = ff // nd
    side = 1 - d
    ex, ey, eg = e + 1 - 2 * lax.rem(e, 2), lax.rem(e + 2, ne), ne - 1 - e
    first, second = ex + d * (ey - ex), ey + d * (ex - ey)
    dests = (e, first, second, eg)

    def slot(dd, ee):
        return ee * nd + dd

    me = slot(d, e)

    def dev(dd=None, ee=None, mm=None):
        return {"dp": d if dd is None else dd, "expert": e if ee is None else ee, "mp": m if mm is None else mm}

    sends, guarded = [], []

    def remote(src, dst, ssem, rsem, where):
        return pltpu.make_async_remote_copy(
            src_ref=src, dst_ref=dst, send_sem=ssem, recv_sem=rsem, device_id=where, device_id_type=MESH
        )

    def send(src, dst, ssem, rsem, where):
        copy = remote(src, dst, ssem, rsem, where)
        copy.start()
        sends.append(copy)

    def send_if(go, src, dst, ssem, rsem, where):
        copy = remote(src, dst, ssem, rsem, where)
        pl.when(go)(copy.start)
        guarded.append((go, copy))

    def wait_in(buf, sem, guard=None):
        c = pltpu.make_async_copy(buf, buf, sem)
        if guard is None:
            c.wait()
        else:
            pl.when(guard)(c.wait)

    loads = [
        pltpu.make_async_copy(src, dst, in_sem.at[i])
        for i, (src, dst) in enumerate((
            (routes_hbm, routes_ref), (cot_hbm, cot_ref), (pair_hbm, pair_ref), (len_hbm, len_ref),
            (ratio_hbm, ratio_ref), (combine_hbm, combine_ref), (h_hbm, h_in),
        ))
    ]
    for load in loads:
        load.start()
    barrier = pltpu.get_barrier_semaphore()
    peers = [
        dev(dd=lax.rem(d + i, nd), ee=lax.rem(e + j, ne)) for i in range(nd) for j in range(ne) if i or j
    ] + [dev(mm=lax.rem(m + i, nm)) for i in range(1, nm)]
    for peer in peers:
        pl.semaphore_signal(barrier, inc=1, device_id=peer, device_id_type=MESH)

    loads[0].wait()
    rows8 = -(-ne // 8) * 8
    row_id = lax.broadcasted_iota(jnp.int32, (rows8, 1), 0)
    owner = jnp.full((rows8, 1), -1, jnp.int32)
    for j, to in enumerate(dests):
        owner = jnp.where(row_id == j, to, owner)
    hit0 = routes_ref[0:1, :] == owner
    hit1 = routes_ref[1:2, :] == owner
    named = hit0 | hit1
    before = lax.broadcasted_iota(jnp.int32, (toks, toks), 0) < lax.broadcasted_iota(jnp.int32, (toks, toks), 1)
    tok_rank = jnp.dot(
        jnp.where(named, 1.0, 0.0).astype(jnp.bfloat16),
        jnp.where(before, 1.0, 0.0).astype(jnp.bfloat16),
        preferred_element_type=jnp.float32,
    )
    tok_rank = jnp.where(named, tok_rank, -1.0)
    tok_pos = tok_rank.astype(jnp.int32)

    for load in loads[2:-1]:
        load.wait()

    blocks = pair_ref.shape[1]
    block_len = toks // blocks
    square = (blocks, blocks)
    diagonal = lax.broadcasted_iota(jnp.int32, square, 0) == lax.broadcasted_iota(jnp.int32, square, 1)

    def column(row):
        return jnp.sum(jnp.where(diagonal, row, 0.0), axis=1, keepdims=True)

    pair, ratio = pair_ref[...], ratio_ref[...]
    chosen = lax.rem(pair, 2) == 0
    other_side = jnp.where(chosen, pair + 1, pair - 1)
    is_other = column(pair.astype(jnp.float32)) == other_side.astype(jnp.float32)
    other_ratio = jnp.sum(jnp.where(is_other, column(ratio), 0.0), axis=0, keepdims=True)
    margin = jnp.where(chosen, ratio - other_ratio, other_ratio - ratio)
    coef = beta_scale * (1.0 / (1.0 + jnp.exp(beta_scale * margin)))
    block_weight = column(jnp.where(chosen, -coef, coef))
    token_id = lax.broadcasted_iota(jnp.int32, (blocks, toks), 1)
    place = token_id - block_len * lax.broadcasted_iota(jnp.int32, (blocks, toks), 0)
    inside = (place >= 0) & (place < block_len)
    alive = inside & (place.astype(jnp.float32) < column(len_ref[...].astype(jnp.float32)))
    live = jnp.sum(jnp.where(alive, 1.0, 0.0), axis=0, keepdims=True)
    per_token = jnp.sum(jnp.where(alive, block_weight, 0.0), axis=0, keepdims=True)
    weight = combine_ref[...] * per_token
    tok_weight = jnp.where(hit0, weight[0:1, :], 0.0) + jnp.where(hit1, weight[1:2, :], 0.0)

    loads[1].wait()
    cotb[m] = cot_ref[:, ca:]
    slot_tok = lax.broadcasted_iota(jnp.int32, (most, toks), 0)
    picks, scales = {}, {}

    def pack_s(j, rows):
        if j not in picks:
            hit = slot_tok == tok_pos[j : j + 1, :]
            picks[j] = jnp.where(hit, 1.0, 0.0).astype(jnp.bfloat16)
            scales[j] = jnp.sum(jnp.where(hit, tok_weight[j : j + 1, :], 0.0), axis=1, keepdims=True)
        rows = jnp.dot(picks[j], rows, preferred_element_type=jnp.float32)
        return (scales[j] * rows).astype(jnp.bfloat16)

    sas[3] = pack_s(3, cot_ref[:, :ca])
    pl.semaphore_wait(barrier, len(peers))
    for i in range(1, nm):
        send(cot_ref.at[:, pl.ds(ca, cb)], cotb.at[m], cb_s.at[i], cb_r.at[m], dev(mm=lax.rem(m + i, nm)))
    send(sas.at[3], relay_a, xa_s.at[3], ra_r.at[0], dev(ee=first))
    sas[2] = pack_s(2, cot_ref[:, :ca])
    send(sas.at[2], sa.at[m, me], xa_s.at[2], a_r.at[m, me], dev(ee=second))
    sas[1] = pack_s(1, cot_ref[:, :ca])
    send(sas.at[1], sa.at[m, me], xa_s.at[1], a_r.at[m, me], dev(ee=first))
    sa[m, me] = pack_s(0, cot_ref[:, :ca])

    def to_partner(q, src, ek, guard=None):
        go = (guard is None) or guard
        args = (sa.at[q, src], sa.at[q, src], dd_s.at[q, ek], a_r.at[q, src], dev(dd=side))
        if guard is None:
            send(*args)
        else:
            send_if(go, *args)

    def spread(ej):
        src = slot(d, ej)
        block = sa.at[m, src]
        send_if(m + 1 < nm, block, block, up_s.at[m, ej], a_r.at[m, src], dev(mm=lax.rem(m + 1, nm)))
        send_if(m > 0, block, block, dn_s.at[m, ej], a_r.at[m, src], dev(mm=lax.rem(m + nm - 1, nm)))
        to_partner(m, src, ej)

    def pass_on(k, ej):
        below, above = m - k, m + k
        ql, qh = lax.rem(below + nm, nm), lax.rem(above, nm)
        src = slot(d, ej)
        low, high = sa.at[ql, src], sa.at[qh, src]
        wait_in(low, a_r.at[ql, src], below >= 0)
        go = (below >= 0) & (m + 1 < nm)
        send_if(go, low, low, up_s.at[ql, ej], a_r.at[ql, src], dev(mm=lax.rem(m + 1, nm)))
        to_partner(ql, src, ej, below >= 0)
        wait_in(high, a_r.at[qh, src], above < nm)
        go = (above < nm) & (m > 0)
        send_if(go, high, high, dn_s.at[qh, ej], a_r.at[qh, src], dev(mm=lax.rem(m + nm - 1, nm)))
        to_partner(qh, src, ej, above < nm)

    spread(e)

    slot_flat = lax.broadcasted_iota(jnp.int32, (most, 2 * toks), 0)
    gap = lax.broadcasted_iota(jnp.int32, (toks, 2 * toks), 1) - 2 * lax.broadcasted_iota(
        jnp.int32, (toks, 2 * toks), 0
    )
    flat_pos = -1.0
    for k, hit in enumerate((hit0, hit1)):
        place_k = jnp.where(gap == k, 1.0, 0.0).astype(jnp.bfloat16)
        value = jnp.where(hit, tok_rank + 1.0, 0.0)
        high = jnp.floor(value * (1.0 / 16.0))
        for part, unit in ((high, 16.0), (value - 16.0 * high, 1.0)):
            flat_pos += unit * jnp.dot(part.astype(jnp.bfloat16), place_k, preferred_element_type=jnp.float32)
    flat_pos = flat_pos.astype(jnp.int32)
    loads[-1].wait()
    flat = (2 * toks, half)
    h_rows = [h_in[:, :, c * half : (c + 1) * half].reshape(flat) for c in range(nd)]

    def pack_h(j):
        pick = jnp.where(slot_flat == flat_pos[j : j + 1, :], 1.0, 0.0).astype(jnp.bfloat16)
        for c in range(nd):
            hs[j, c] = jnp.dot(pick, h_rows[c], preferred_element_type=jnp.float32).astype(jnp.bfloat16)

    pack_h(3)
    for c in range(nd):
        send(hs.at[3, c], relay_h.at[c], h_s.at[3, c], rh_r.at[c], dev(ee=first))
    pack_h(2)
    send(hs.at[2, d], hr.at[me], h_s.at[2, 0], h_r.at[me], dev(dd=d, ee=second))
    pack_h(0)
    send(hs.at[0, side], hr.at[me], h_s.at[0, 0], h_r.at[me], dev(dd=side))
    hr[me] = hs[0, d]

    wait_in(sa.at[m, slot(d, second)], a_r.at[m, slot(d, second)])
    spread(second)
    wait_in(relay_a, ra_r.at[0])
    from_first = slot(d, first)
    send(relay_a, sa.at[m, from_first], ra_s.at[0], a_r.at[m, from_first], dev(ee=second))
    pack_h(1)
    wait_in(sa.at[m, slot(d, first)], a_r.at[m, slot(d, first)])
    spread(first)

    in_order = (routes_ref[0:1, :] == row_id) | (routes_ref[1:2, :] == row_id)
    counts = jnp.sum(jnp.where(in_order, live, 0.0), axis=1, keepdims=True)
    lanes8 = lax.broadcasted_iota(jnp.int32, (rows8, LANES), 1) == row_id
    lbuf[me] = jnp.broadcast_to(jnp.sum(jnp.where(lanes8, counts, 0.0), axis=0, keepdims=True), (rows8, LANES))

    for i in range(1, nm):
        q = lax.rem(m + i, nm)
        wait_in(cotb.at[q], cb_r.at[q])
    dense = jnp.concatenate([cotb[q] for q in range(nm)], axis=1)
    sbs[3] = pack_s(3, dense)
    send(sbs.at[3], relay_b, xb_s.at[3], rb_r.at[0], dev(ee=first))
    sbs[2] = pack_s(2, dense)
    send(sbs.at[2], sb.at[me], xb_s.at[2], b_r.at[me], dev(ee=second))
    sbs[1] = pack_s(1, dense)
    send(sbs.at[1], sb.at[me], xb_s.at[1], b_r.at[me], dev(ee=first))
    sb[me] = pack_s(0, dense)
    send(sb.at[me], sb.at[me], db_s.at[0], b_r.at[me], dev(dd=side))

    def share_b(ej, n):
        src = slot(d, ej)
        wait_in(sb.at[src], b_r.at[src])
        send(sb.at[src], sb.at[src], db_s.at[n], b_r.at[src], dev(dd=side))

    n = 0
    for i in range(nd):
        for j in range(ne):
            if i or j:
                to = dev(dd=lax.rem(d + i, nd), ee=lax.rem(e + j, ne))
                send(lbuf.at[me], lbuf.at[me], l_s.at[n], l_r.at[me], to)
                n += 1

    whole = most // 256 * 256
    part = whole // 2
    pieces = ((0, part), (part, part), (whole, most - whole))
    send(hs.at[1, d], hr.at[me], h_s.at[1, 0], h_r.at[me], dev(dd=d, ee=first))

    def send_last(j, to, axis):
        for p, (at, rows) in enumerate(pieces):
            send(
                hs.at[j, side, pl.ds(at, rows)], hr.at[me, pl.ds(at, rows)], hp_s.at[j - 1, p], hp_r.at[axis, p],
                dev(dd=side, ee=to),
            )

    send_last(1, first, d)

    def nearest(r):
        near = jnp.minimum(m, nm - 1 - m)
        both = m + (r + 1) // 2 * (1 if r % 2 == 0 else -1)
        far = jnp.where(m < nm - 1 - m, m + r - near, m - r + near)
        return jnp.where(r <= 2 * near, both, far)

    def put(ref, index, value, fresh):
        if fresh:
            ref[index] = value
        else:
            ref[index] = ref[index] + value

    def unit(r, left, cut, fresh=False):
        if r < nm:
            q = nearest(r)
            put(acc_a, q, jnp.dot(left[...], cut(sa.at[q]), preferred_element_type=jnp.float32), fresh)
        else:
            put(acc_b, ..., jnp.dot(left[...], cut(sb), preferred_element_type=jnp.float32), fresh)

    def rows_of(s0, s1, at, rows):
        def cut(ref):
            return jnp.concatenate([ref[s0, at : at + rows], ref[s1, at : at + rows]], axis=0)

        return cut

    def turn(s0, s1, at, rows):
        return jnp.concatenate([hr[s0, at : at + rows], hr[s1, at : at + rows]], axis=0).T

    def partner_a(r, ej):
        q = nearest(r)
        src = slot(side, ej)
        wait_in(sa.at[q, src], a_r.at[q, src])

    def partner_b(ej):
        src = slot(side, ej)
        wait_in(sb.at[src], b_r.at[src])

    def wait_h(src):
        wait_in(hr.at[src], h_r.at[src])

    B = nm
    own = rows_of(slot(0, e), slot(1, e), 0, whole)
    diag = rows_of(slot(0, eg), slot(1, eg), 0, whole)
    same = rows_of(slot(d, ex), slot(d, ey), 0, whole)

    pass_on(1, e)
    wait_in(sa.at[m, slot(d, eg)], a_r.at[m, slot(d, eg)])
    spread(eg)
    pass_on(1, second)
    pass_on(1, first)
    wait_h(slot(side, e))
    ht[0] = turn(slot(0, e), slot(1, e), 0, whole)
    partner_a(0, e)
    unit(0, ht.at[0], own, True)
    wait_in(relay_h.at[0], rh_r.at[0])
    send(relay_h.at[0], hr.at[from_first], rh_s.at[0], h_r.at[from_first], dev(dd=0, ee=second))
    partner_b(e)
    unit(B, ht.at[0], own, True)
    pass_on(1, eg)
    share_b(second, 1)
    partner_a(1, e)
    unit(1, ht.at[0], own, True)
    pass_on(2, e)
    wait_in(relay_h.at[1], rh_r.at[1])
    send(relay_h.at[1], hr.at[from_first], rh_s.at[1], h_r.at[from_first], dev(dd=1, ee=second))
    pass_on(2, second)
    wait_in(relay_b, rb_r.at[0])
    send(relay_b, sb.at[from_first], rb_s.at[0], b_r.at[from_first], dev(ee=second))
    send_last(2, second, side)
    pass_on(2, first)
    pass_on(2, eg)
    partner_a(2, e)
    unit(2, ht.at[0], own, True)
    share_b(first, 2)
    pass_on(3, e)
    partner_a(3, e)
    unit(3, ht.at[0], own, True)
    wait_h(slot(0, eg))
    wait_h(slot(1, eg))
    ht[1] = turn(slot(0, eg), slot(1, eg), 0, whole)
    for r in range(nm - 2):
        partner_a(r, eg)
        unit(r, ht.at[1], diag)
    pass_on(3, second)
    partner_a(nm - 2, eg)
    unit(nm - 2, ht.at[1], diag)
    share_b(eg, 3)
    wait_h(slot(d, ex))
    wait_h(slot(d, ey))
    ht[2] = turn(slot(d, ex), slot(d, ey), 0, whole)
    for r in range(nm - 1):
        unit(r, ht.at[2], same)
    unit(B, ht.at[2], same)
    pass_on(3, first)
    unit(nm - 1, ht.at[2], same)
    partner_b(eg)
    unit(B, ht.at[1], diag)
    x_far, y_far = slot(side, ex), slot(side, ey)

    def last_piece(p):
        at, rows = pieces[p]
        for axis, src in ((0, x_far), (1, y_far)):
            wait_in(hr.at[src, pl.ds(at, rows)], hp_r.at[axis, p])

    last_piece(0)
    ht_end[...] = turn(x_far, y_far, 0, part)
    for r in range(nm):
        partner_a(r, first)
        partner_a(r, second)
        unit(r, ht_end, rows_of(x_far, y_far, 0, part))
    partner_b(first)
    partner_b(second)
    unit(B, ht_end, rows_of(x_far, y_far, 0, part))
    pass_on(3, eg)
    partner_a(nm - 1, eg)
    unit(nm - 1, ht.at[1], diag)
    last_piece(1)
    ht_end[...] = turn(x_far, y_far, part, part)
    for r in range(nm + 1):
        unit(r, ht_end, rows_of(x_far, y_far, part, part))
    last_piece(2)
    rest = nd * ne * (most - whole)
    ht_end[...] = hr[:, whole:, :].reshape(rest, half).T
    for r in range(nm + 1):
        unit(r, ht_end, lambda ref: ref[:, whole:, :].reshape(rest, ref.shape[2]))

    for i in range(nd):
        for j in range(ne):
            if i or j:
                src = slot(lax.rem(d + i, nd), lax.rem(e + j, ne))
                wait_in(lbuf.at[src], l_r.at[src])
    total = lbuf[0]
    for k in range(1, nd * ne):
        total = total + lbuf[k]
    load_ref[...] = total

    for c in sends:
        c.wait_send()
    for go, c in guarded:
        pl.when(go)(c.wait_send)


def finish_kernel(nm, a_ref, b_ref, load_ref, out_ref, total_ref, sem):
    ca, cb = a_ref.shape[2], b_ref.shape[1] // nm
    width = ca + cb
    copies = []
    for q in range(nm):
        copies.append((a_ref.at[q], out_ref.at[0, :, pl.ds(q * width, ca)]))
        copies.append((b_ref.at[:, pl.ds(q * cb, cb)], out_ref.at[0, :, pl.ds(q * width + ca, cb)]))
    copies = [pltpu.make_async_copy(src, dst, sem.at[i]) for i, (src, dst) in enumerate(copies)]
    for copy in copies:
        copy.start()
    total_ref[...] = load_ref[0:1, : total_ref.shape[1]]
    for copy in copies:
        copy.wait()


def fast_body(hidden, cotangent, routes, combine, block_pair, lengths, log_ratio):
    nd, ne, nm = lax.axis_size("dp"), lax.axis_size("expert"), lax.axis_size("mp")
    toks, top, ff = hidden.shape
    width = cotangent.shape[1]
    most = 3 * toks // 4
    cb = width // 4 // LANES * LANES
    ca = width - cb
    half = ff // nd
    srcs = nd * ne
    rows8 = -(-ne // 8) * 8
    whole = most // 256 * 256
    dims = (nd, ne, nm, most, ca, cb)
    bf16, f32 = jnp.bfloat16, jnp.float32
    vmem = pl.BlockSpec(memory_space=pltpu.VMEM)
    hbm = pl.BlockSpec(memory_space=pltpu.HBM)
    dma = pltpu.SemaphoreType.DMA
    acc_a, acc_b, load = pl.pallas_call(
        functools.partial(exchange_kernel, dims),
        out_shape=(
            pltpu.VMEM((nm, half, ca), f32),
            pltpu.VMEM((half, nm * cb), f32),
            pltpu.VMEM((rows8, LANES), f32),
        ),
        in_specs=[hbm] * 7,
        out_specs=(vmem,) * 3,
        scratch_shapes=[
            pltpu.VMEM((toks, top, ff), bf16),
            pltpu.VMEM(cotangent.shape, bf16),
            pltpu.VMEM((top, toks), jnp.int32),
            pltpu.VMEM((top, toks), f32),
            pltpu.VMEM(block_pair.shape, jnp.int32),
            pltpu.VMEM(lengths.shape, jnp.int32),
            pltpu.VMEM(log_ratio.shape, f32),
            pltpu.VMEM((srcs, most, half), bf16),
            pltpu.VMEM((nm, srcs, most, ca), bf16),
            pltpu.VMEM((srcs, most, nm * cb), bf16),
            pltpu.VMEM((ne, nd, most, half), bf16),
            pltpu.VMEM((ne, most, ca), bf16),
            pltpu.VMEM((ne, most, nm * cb), bf16),
            pltpu.VMEM((nm, toks, cb), bf16),
            pltpu.VMEM((srcs, rows8, LANES), f32),
            pltpu.VMEM((nd, most, half), bf16),
            pltpu.VMEM((most, ca), bf16),
            pltpu.VMEM((most, nm * cb), bf16),
            pltpu.VMEM((3, half, 2 * whole), bf16),
            pltpu.VMEM((half, whole), bf16),
            dma((7,)),
            dma((ne,)),
            dma((nm, srcs)),
            dma((1,)),
            dma((1,)),
            dma((nm, ne)),
            dma((nm, ne)),
            dma((nm, ne)),
            dma((nm,)),
            dma((nm,)),
            dma((ne,)),
            dma((srcs,)),
            dma((1,)),
            dma((1,)),
            dma((ne,)),
            dma((ne, nd)),
            dma((srcs,)),
            dma((2, 3)),
            dma((2, 3)),
            dma((nd,)),
            dma((nd,)),
            dma((srcs,)),
            dma((srcs,)),
        ],
        compiler_params=pltpu.CompilerParams(
            collective_id=0, has_side_effects=True, vmem_limit_bytes=VMEM_MOST - 10 * 1024 * 1024
        ),
    )(hidden, cotangent, routes.T, combine.T, block_pair, lengths, log_ratio)
    grad_down, total = pl.pallas_call(
        functools.partial(finish_kernel, nm),
        out_shape=(jax.ShapeDtypeStruct((1, half, nm * width), f32), jax.ShapeDtypeStruct((1, ne), f32)),
        in_specs=[vmem] * 3,
        out_specs=(hbm, vmem),
        scratch_shapes=[dma((2 * nm,))],
        compiler_params=pltpu.CompilerParams(vmem_limit_bytes=1024 * 1024),
    )(acc_a, acc_b, load)
    return grad_down, total.reshape(ne)


def plain_body(hidden, cotangent, routes, combine, block_pair, lengths, log_ratio):
    per_token, within = token_factors(block_pair, lengths, log_ratio, LEN)
    weight = combine * per_token[:, None]
    tok_rows = routes.shape[0]
    route_top = routes.shape[1]
    ff_local = hidden.shape[2]
    groups = lax.axis_size("expert")
    experts = groups * EXP_DEV
    most_rows = 3 * tok_rows // 4
    labels = jnp.arange(experts, dtype=jnp.int32)
    routed = routes[:, :, None] == labels[None, None, :]
    local_load = jnp.sum(jnp.where(routed & within[:, None, None], 1.0, 0.0), axis=(0, 1)).astype(
        jnp.float32
    )
    flat_rows = tok_rows * route_top
    flat_hits = routed.reshape(flat_rows, experts).astype(jnp.int32)
    rank_of = jnp.sum((jnp.cumsum(flat_hits, axis=0) - 1) * flat_hits, axis=1)
    slot_of = routes.reshape(flat_rows) * most_rows + rank_of
    source = (
        jnp.zeros((experts * most_rows,), jnp.int32)
        .at[slot_of]
        .set(jnp.arange(flat_rows, dtype=jnp.int32))
    )
    filled = jnp.zeros((experts * most_rows,), jnp.float32).at[slot_of].set(1.0)
    token_of = source // route_top
    slot_weight = jnp.take(weight.reshape(flat_rows), source) * filled
    packed_h = jnp.take(hidden.reshape(flat_rows, ff_local), source, axis=0).reshape(
        groups, EXP_DEV * most_rows, ff_local
    )
    narrow_s = (
        slot_weight[:, None] * jnp.take(cotangent, token_of, axis=0).astype(jnp.float32)
    ).astype(jnp.bfloat16)
    moved_h, narrow = (
        lax.all_to_all(packed_h, "expert", split_axis=0, concat_axis=0, tiled=True),
        lax.all_to_all(
            narrow_s.reshape(groups, EXP_DEV * most_rows, cotangent.shape[1]),
            "expert",
            split_axis=0,
            concat_axis=0,
            tiled=True,
        ),
    )
    moved_s = lax.all_gather(narrow, "mp", axis=2, tiled=True)
    moved_h = moved_h.reshape(groups, EXP_DEV, most_rows, ff_local)
    moved_s = moved_s.reshape(groups, EXP_DEV, most_rows, moved_s.shape[2])
    products = [
        lax.dot_general(
            moved_h[:, 0],
            moved_s[:, 0],
            (((0, 1), (0, 1)), ((), ())),
            preferred_element_type=jnp.float32,
        )
    ]
    owned = lax.psum_scatter(jnp.stack(products, axis=1), "dp", scatter_dimension=0, tiled=True)
    grad_down = jnp.transpose(owned, (1, 0, 2))
    expert_load = lax.psum(local_load, ("dp", "expert"))
    return (grad_down, expert_load)


def solution(mesh):
    in_specs = (
        P(("dp", "expert"), None, "mp"),
        P(("dp", "expert"), "mp"),
        P(("dp", "expert"), None),
        P(("dp", "expert"), None),
        P(("dp", "expert"), None),
        P(("dp", "expert"), None),
        P(("dp", "expert"), None),
    )
    out_specs = (P("expert", ("mp", "dp"), None), P())

    def body(hidden, cotangent, *rest):
        rows = mesh.shape["dp"] * mesh.shape["expert"] * (3 * hidden.shape[0] // 4)
        bytes_in = 2 * rows * (cotangent.shape[1] * mesh.shape["mp"] + hidden.shape[2])
        most = 3 * hidden.shape[0] // 4
        whole = most // 256 * 256
        square = mesh.shape["dp"] == 2 and mesh.shape["expert"] == 4 and mesh.shape["mp"] == 4
        fits = square and whole and 8 * (most - whole) == whole
        run = fast_body if fits and 2 * bytes_in < VMEM_ROOM else plain_body
        return run(hidden, cotangent, *rest)

    return jax.shard_map(body, mesh=mesh, in_specs=in_specs, out_specs=out_specs, check_vma=False)
```

```python
import functools

import jax
import jax.numpy as jnp
from jax import lax
from jax.experimental import pallas as pl
from jax.experimental.pallas import tpu as pltpu
from jax.sharding import PartitionSpec as P

EXP_DEV = 1
LEN = 32
LANES = 128
VMEM_ROOM = 48 * 1024 * 1024
VMEM_MOST = 67043328
MESH = pl.DeviceIdType.MESH


beta_scale = 0.1


def token_factors(block_pair, lengths, log_ratio, block_len):
    blocks = block_pair.shape[1]
    labels = jnp.arange(blocks, dtype=jnp.int32)
    matches = block_pair[:, :, None] == labels[None, None, :]
    by_label = jnp.sum(jnp.where(matches, log_ratio[:, :, None], 0.0), axis=1)
    margin = by_label[:, 0::2] - by_label[:, 1::2]
    pair_coef = beta_scale * jax.nn.sigmoid(-beta_scale * margin)
    owners = block_pair // 2
    pair_ids = jnp.arange(blocks // 2, dtype=jnp.int32)
    picked = owners[:, :, None] == pair_ids[None, None, :]
    block_coef = jnp.sum(jnp.where(picked, pair_coef[:, None, :], 0.0), axis=2)
    block_weight = jnp.where(block_pair % 2 == 0, -block_coef, block_coef)
    position = jnp.arange(block_len, dtype=jnp.int32)
    within = position[None, None, :] < lengths[:, :, None]
    per_token = jnp.where(within, block_weight[:, :, None], 0.0).reshape(-1)
    return per_token, within.reshape(-1)


def exchange_kernel(
    dims, h_hbm, cot_hbm, routes_hbm, combine_hbm, pair_hbm, len_hbm, ratio_hbm,
    acc_a, acc_b, ht_end, end_a, end_b, load_ref,
    h_in, cot_ref, routes_ref, combine_ref, pair_ref, len_ref, ratio_ref,
    hr, sa, sb, hs, sas, sbs, cotb, lbuf, relay_h, relay_a, relay_b, raw_a, raw_b, meta_out, meta_in, ht, ht_far,
    in_sem, xa_s, a_r, ra_s, rw_s, rw_r, up_s, dn_s, dd_s, cb_s, cb_r, xb_s, b_r, rb_s, db_s,
    h_s, h_r, he_s, he_r, rh_s, rh_r, re_s, l_s, l_r,
):
    nd, ne, nm, most, ca, cb = dims
    d, e, m = lax.axis_index("dp"), lax.axis_index("expert"), lax.axis_index("mp")
    toks, top, ff = h_in.shape
    half = ff // nd
    side = 1 - d
    ex, ey, eg = e + 1 - 2 * lax.rem(e, 2), lax.rem(e + 2, ne), ne - 1 - e
    first, second = ex + d * (ey - ex), ey + d * (ex - ey)
    dests = (e, first, second, eg)

    def slot(dd, ee):
        return ee * nd + dd

    me = slot(d, e)

    def dev(dd=None, ee=None, mm=None):
        return {"dp": d if dd is None else dd, "expert": e if ee is None else ee, "mp": m if mm is None else mm}

    sends, guarded = [], []

    def remote(src, dst, ssem, rsem, where):
        return pltpu.make_async_remote_copy(
            src_ref=src, dst_ref=dst, send_sem=ssem, recv_sem=rsem, device_id=where, device_id_type=MESH
        )

    def send(src, dst, ssem, rsem, where):
        copy = remote(src, dst, ssem, rsem, where)
        copy.start()
        sends.append(copy)

    def send_if(go, src, dst, ssem, rsem, where):
        copy = remote(src, dst, ssem, rsem, where)
        pl.when(go)(copy.start)
        guarded.append((go, copy))

    def wait_in(buf, sem, guard=None):
        c = pltpu.make_async_copy(buf, buf, sem)
        if guard is None:
            c.wait()
        else:
            pl.when(guard)(c.wait)

    loads = [
        pltpu.make_async_copy(src, dst, in_sem.at[i])
        for i, (src, dst) in enumerate((
            (routes_hbm, routes_ref), (cot_hbm, cot_ref), (pair_hbm, pair_ref), (len_hbm, len_ref),
            (ratio_hbm, ratio_ref), (combine_hbm, combine_ref), (h_hbm, h_in),
        ))
    ]
    for load in loads:
        load.start()
    barrier = pltpu.get_barrier_semaphore()
    peers = [
        dev(dd=lax.rem(d + i, nd), ee=lax.rem(e + j, ne)) for i in range(nd) for j in range(ne) if i or j
    ] + [dev(mm=lax.rem(m + i, nm)) for i in range(1, nm)]
    for peer in peers:
        pl.semaphore_signal(barrier, inc=1, device_id=peer, device_id_type=MESH)

    loads[0].wait()
    rows8 = -(-ne // 8) * 8
    row_id = lax.broadcasted_iota(jnp.int32, (rows8, 1), 0)
    owner = jnp.full((rows8, 1), -1, jnp.int32)
    for j, to in enumerate(dests):
        owner = jnp.where(row_id == j, to, owner)
    hit0 = routes_ref[0:1, :] == owner
    hit1 = routes_ref[1:2, :] == owner
    named = hit0 | hit1
    before = lax.broadcasted_iota(jnp.int32, (toks, toks), 0) < lax.broadcasted_iota(jnp.int32, (toks, toks), 1)
    tok_rank = jnp.dot(
        jnp.where(named, 1.0, 0.0).astype(jnp.bfloat16),
        jnp.where(before, 1.0, 0.0).astype(jnp.bfloat16),
        preferred_element_type=jnp.float32,
    )
    tok_rank = jnp.where(named, tok_rank, -1.0)
    tok_pos = tok_rank.astype(jnp.int32)

    for load in loads[2:-1]:
        load.wait()

    blocks = pair_ref.shape[1]
    block_len = toks // blocks
    square = (blocks, blocks)
    diagonal = lax.broadcasted_iota(jnp.int32, square, 0) == lax.broadcasted_iota(jnp.int32, square, 1)

    def column(row):
        return jnp.sum(jnp.where(diagonal, row, 0.0), axis=1, keepdims=True)

    pair, ratio = pair_ref[...], ratio_ref[...]
    chosen = lax.rem(pair, 2) == 0
    other_side = jnp.where(chosen, pair + 1, pair - 1)
    is_other = column(pair.astype(jnp.float32)) == other_side.astype(jnp.float32)
    other_ratio = jnp.sum(jnp.where(is_other, column(ratio), 0.0), axis=0, keepdims=True)
    margin = jnp.where(chosen, ratio - other_ratio, other_ratio - ratio)
    coef = beta_scale * (1.0 / (1.0 + jnp.exp(beta_scale * margin)))
    block_weight = column(jnp.where(chosen, -coef, coef))
    token_id = lax.broadcasted_iota(jnp.int32, (blocks, toks), 1)
    place = token_id - block_len * lax.broadcasted_iota(jnp.int32, (blocks, toks), 0)
    inside = (place >= 0) & (place < block_len)
    alive = inside & (place.astype(jnp.float32) < column(len_ref[...].astype(jnp.float32)))
    live = jnp.sum(jnp.where(alive, 1.0, 0.0), axis=0, keepdims=True)
    per_token = jnp.sum(jnp.where(alive, block_weight, 0.0), axis=0, keepdims=True)
    weight = combine_ref[...] * per_token
    tok_weight = jnp.where(hit0, weight[0:1, :], 0.0) + jnp.where(hit1, weight[1:2, :], 0.0)

    loads[1].wait()
    cotb[m] = cot_ref[:, ca:]
    meta_out[...] = jnp.concatenate([tok_rank[:ne], tok_weight[:ne]], axis=0)
    slot_tok = lax.broadcasted_iota(jnp.int32, (most, toks), 0)
    pl.semaphore_wait(barrier, len(peers))
    send(cot_ref.at[:, pl.ds(0, ca)], raw_a, rw_s.at[0], rw_r.at[0], dev(ee=first))
    for i in range(1, nm):
        send(cot_ref.at[:, pl.ds(ca, cb)], cotb.at[m], cb_s.at[i], cb_r.at[m], dev(mm=lax.rem(m + i, nm)))
    send(meta_out, meta_in, rw_s.at[1], rw_r.at[1], dev(ee=first))

    def picker(position, factor):
        hit = slot_tok == position
        pick = jnp.where(hit, 1.0, 0.0).astype(jnp.bfloat16)
        scale = jnp.sum(jnp.where(hit, factor, 0.0), axis=1, keepdims=True)

        def pack(rows):
            rows = jnp.dot(pick, rows, preferred_element_type=jnp.float32)
            return (scale * rows).astype(jnp.bfloat16)

        return pack

    pack_own = picker(tok_pos[0:1, :], tok_weight[0:1, :])
    sa[m, me] = pack_own(cot_ref[:, :ca])

    def to_partner(q, src, ek, guard=None):
        go = (guard is None) or guard
        args = (sa.at[q, src], sa.at[q, src], dd_s.at[q, ek], a_r.at[q, src], dev(dd=side))
        if guard is None:
            send(*args)
        else:
            send_if(go, *args)

    def spread(ej):
        src = slot(d, ej)
        block = sa.at[m, src]
        send_if(m + 1 < nm, block, block, up_s.at[m, ej], a_r.at[m, src], dev(mm=lax.rem(m + 1, nm)))
        send_if(m > 0, block, block, dn_s.at[m, ej], a_r.at[m, src], dev(mm=lax.rem(m + nm - 1, nm)))
        to_partner(m, src, ej)

    def pass_on(k, ej):
        below, above = m - k, m + k
        ql, qh = lax.rem(below + nm, nm), lax.rem(above, nm)
        src = slot(d, ej)
        low, high = sa.at[ql, src], sa.at[qh, src]
        wait_in(low, a_r.at[ql, src], below >= 0)
        go = (below >= 0) & (m + 1 < nm)
        send_if(go, low, low, up_s.at[ql, ej], a_r.at[ql, src], dev(mm=lax.rem(m + 1, nm)))
        to_partner(ql, src, ej, below >= 0)
        wait_in(high, a_r.at[qh, src], above < nm)
        go = (above < nm) & (m > 0)
        send_if(go, high, high, dn_s.at[qh, ej], a_r.at[qh, src], dev(mm=lax.rem(m + nm - 1, nm)))
        to_partner(qh, src, ej, above < nm)

    spread(e)
    pack_second = picker(tok_pos[2:3, :], tok_weight[2:3, :])
    sas[...] = pack_second(cot_ref[:, :ca])
    send(sas, sa.at[m, me], xa_s.at[0], a_r.at[m, me], dev(ee=second))

    slot_flat = lax.broadcasted_iota(jnp.int32, (most, 2 * toks), 0)
    gap = lax.broadcasted_iota(jnp.int32, (toks, 2 * toks), 1) - 2 * lax.broadcasted_iota(
        jnp.int32, (toks, 2 * toks), 0
    )
    flat_pos = -1.0
    for k, hit in enumerate((hit0, hit1)):
        place_k = jnp.where(gap == k, 1.0, 0.0).astype(jnp.bfloat16)
        value = jnp.where(hit, tok_rank + 1.0, 0.0)
        high = jnp.floor(value * (1.0 / 16.0))
        for part, unit in ((high, 16.0), (value - 16.0 * high, 1.0)):
            flat_pos += unit * jnp.dot(part.astype(jnp.bfloat16), place_k, preferred_element_type=jnp.float32)
    flat_pos = flat_pos.astype(jnp.int32)
    loads[-1].wait()
    flat = (2 * toks, half)
    h_rows = [h_in[:, :, c * half : (c + 1) * half].reshape(flat) for c in range(nd)]

    def pack_h(j):
        pick = jnp.where(slot_flat == flat_pos[j : j + 1, :], 1.0, 0.0).astype(jnp.bfloat16)
        for c in range(nd):
            hs[j, c] = jnp.dot(pick, h_rows[c], preferred_element_type=jnp.float32).astype(jnp.bfloat16)

    whole = most // 256 * 256
    main, rest = pl.ds(0, whole), pl.ds(whole, most - whole)
    pack_h(3)
    for c in range(nd):
        send(hs.at[3, c], relay_h.at[c], h_s.at[3, c], rh_r.at[c], dev(ee=first))
    pack_h(2)
    wait_in(meta_in, rw_r.at[1])
    wait_in(raw_a, rw_r.at[0])
    from_first = slot(d, first)
    pack_relay = picker(meta_in[3:4, :].astype(jnp.int32), meta_in[ne + 3 : ne + 4, :])
    relay_a[...] = pack_relay(raw_a[...])
    send(relay_a, sa.at[m, from_first], ra_s.at[0], a_r.at[m, from_first], dev(ee=second))
    send(hs.at[2, d, main], hr.at[me, main], h_s.at[2, 0], h_r.at[me], dev(dd=d, ee=second))
    pack_first = picker(meta_in[1:2, :].astype(jnp.int32), meta_in[ne + 1 : ne + 2, :])
    sa[m, from_first] = pack_first(raw_a[...])
    spread(first)
    wait_in(sa.at[m, slot(d, second)], a_r.at[m, slot(d, second)])
    spread(second)
    pack_h(0)
    send(hs.at[0, side], hr.at[me], h_s.at[0, 0], h_r.at[me], dev(dd=side))
    hr[me] = hs[0, d]
    pack_h(1)

    in_order = (routes_ref[0:1, :] == row_id) | (routes_ref[1:2, :] == row_id)
    counts = jnp.sum(jnp.where(in_order, live, 0.0), axis=1, keepdims=True)
    lanes8 = lax.broadcasted_iota(jnp.int32, (rows8, LANES), 1) == row_id
    lbuf[me] = jnp.broadcast_to(jnp.sum(jnp.where(lanes8, counts, 0.0), axis=0, keepdims=True), (rows8, LANES))

    for i in range(1, nm):
        q = lax.rem(m + i, nm)
        wait_in(cotb.at[q], cb_r.at[q])
    send(cotb, raw_b, rw_s.at[2], rw_r.at[2], dev(ee=first))
    dense = jnp.concatenate([cotb[q] for q in range(nm)], axis=1)
    sbs[...] = pack_second(dense)
    send(sbs, sb.at[me], xb_s.at[0], b_r.at[me], dev(ee=second))
    sb[me] = pack_own(dense)
    send(sb.at[me], sb.at[me], db_s.at[0], b_r.at[me], dev(dd=side))

    def share_b(ej, n):
        src = slot(d, ej)
        wait_in(sb.at[src], b_r.at[src])
        send(sb.at[src], sb.at[src], db_s.at[n], b_r.at[src], dev(dd=side))

    n = 0
    for i in range(nd):
        for j in range(ne):
            if i or j:
                to = dev(dd=lax.rem(d + i, nd), ee=lax.rem(e + j, ne))
                send(lbuf.at[me], lbuf.at[me], l_s.at[n], l_r.at[me], to)
                n += 1

    for c, k in ((d, 0), (side, 1)):
        send(hs.at[1, c], hr.at[me], h_s.at[1, k], h_r.at[me], dev(dd=c, ee=first))

    def nearest(r):
        near = jnp.minimum(m, nm - 1 - m)
        both = m + (r + 1) // 2 * (1 if r % 2 == 0 else -1)
        far = jnp.where(m < nm - 1 - m, m + r - near, m - r + near)
        return jnp.where(r <= 2 * near, both, far)

    def put(ref, index, value, fresh):
        if fresh:
            ref[index] = value
        else:
            ref[index] = ref[index] + value

    def unit(r, left, cut, fresh=False):
        if r < nm:
            q = nearest(r)
            put(acc_a, q, jnp.dot(left[...], cut(sa.at[q]), preferred_element_type=jnp.float32), fresh)
        else:
            put(acc_b, ..., jnp.dot(left[...], cut(sb), preferred_element_type=jnp.float32), fresh)

    def rows_of(s0, s1, at, rows):
        def cut(ref):
            return jnp.concatenate([ref[s0, at : at + rows], ref[s1, at : at + rows]], axis=0)

        return cut

    def turn(s0, s1, at, rows):
        return jnp.concatenate([hr[s0, at : at + rows], hr[s1, at : at + rows]], axis=0).T

    def partner_a(r, ej):
        q = nearest(r)
        src = slot(side, ej)
        wait_in(sa.at[q, src], a_r.at[q, src])

    def partner_b(ej):
        src = slot(side, ej)
        wait_in(sb.at[src], b_r.at[src])

    def wait_h(src):
        wait_in(hr.at[src], h_r.at[src])

    def wait_main(src):
        wait_in(hr.at[src, main], h_r.at[src])

    B = nm
    own = rows_of(slot(0, e), slot(1, e), 0, whole)
    diag = rows_of(slot(0, eg), slot(1, eg), 0, whole)
    same = rows_of(slot(d, ex), slot(d, ey), 0, whole)

    pass_on(1, e)
    wait_in(sa.at[m, slot(d, eg)], a_r.at[m, slot(d, eg)])
    spread(eg)
    pass_on(1, first)
    pass_on(1, second)
    wait_h(slot(side, e))
    ht[0] = turn(slot(0, e), slot(1, e), 0, whole)
    partner_a(0, e)
    unit(0, ht.at[0], own, True)
    wait_in(relay_h.at[0], rh_r.at[0])
    send(relay_h.at[0, main], hr.at[from_first, main], rh_s.at[0], h_r.at[from_first], dev(dd=0, ee=second))
    partner_b(e)
    unit(B, ht.at[0], own, True)
    pass_on(1, eg)
    share_b(second, 1)
    partner_a(1, e)
    unit(1, ht.at[0], own, True)
    pass_on(2, e)
    wait_in(relay_h.at[1], rh_r.at[1])
    send(relay_h.at[1, main], hr.at[from_first, main], rh_s.at[1], h_r.at[from_first], dev(dd=1, ee=second))
    pass_on(2, first)
    wait_in(raw_b, rw_r.at[2])
    dense = jnp.concatenate([raw_b[q] for q in range(nm)], axis=1)
    relay_b[...] = pack_relay(dense)
    send(relay_b, sb.at[from_first], rb_s.at[0], b_r.at[from_first], dev(ee=second))
    send(hs.at[2, side, main], hr.at[me, main], h_s.at[2, 1], h_r.at[me], dev(dd=side, ee=second))
    for c, k in ((d, 0), (side, 1)):
        send(hs.at[2, c, rest], hr.at[me, rest], he_s.at[k], he_r.at[me], dev(dd=c, ee=second))
    for c in range(nd):
        send(relay_h.at[c, rest], hr.at[from_first, rest], re_s.at[c], he_r.at[from_first], dev(dd=c, ee=second))
    sb[from_first] = pack_first(dense)
    send(sb.at[from_first], sb.at[from_first], db_s.at[2], b_r.at[from_first], dev(dd=side))
    pass_on(2, second)
    pass_on(2, eg)
    partner_a(2, e)
    unit(2, ht.at[0], own, True)
    pass_on(3, e)
    partner_a(3, e)
    unit(3, ht.at[0], own, True)
    wait_h(slot(d, first))
    wait_main(slot(d, second))
    ht[2] = turn(slot(d, ex), slot(d, ey), 0, whole)
    for r in range(nm - 1):
        unit(r, ht.at[2], same)
    unit(B, ht.at[2], same)
    wait_main(slot(0, eg))
    wait_main(slot(1, eg))
    ht[1] = turn(slot(0, eg), slot(1, eg), 0, whole)
    for r in range(nm - 2):
        partner_a(r, eg)
        unit(r, ht.at[1], diag)
    pass_on(3, first)
    partner_a(nm - 2, eg)
    unit(nm - 2, ht.at[1], diag)
    share_b(eg, 3)
    pass_on(3, second)
    unit(nm - 1, ht.at[2], same)
    partner_b(eg)
    unit(B, ht.at[1], diag)

    def far(src, wait, ej):
        wait(src)
        ht_far[...] = hr[src, :whole].T
        for r in range(nm):
            partner_a(r, ej)
            unit(r, ht_far, lambda ref: ref[src, :whole])
        partner_b(ej)
        unit(B, ht_far, lambda ref: ref[src, :whole])

    far(slot(side, second), wait_h, second)
    pass_on(3, eg)
    far(slot(side, first), wait_main, first)
    partner_a(nm - 1, eg)
    unit(nm - 1, ht.at[1], diag)
    depth = nd * ne * (most - whole)
    for q in range(nm):
        end_a[q] = sa[q, :, whole:, :].reshape(depth, ca)
    end_b[...] = sb[:, whole:, :].reshape(depth, nm * cb)
    for src in (slot(d, second), slot(side, first), slot(0, eg), slot(1, eg)):
        wait_in(hr.at[src, rest], he_r.at[src])
    ht_end[...] = hr[:, whole:, :].reshape(depth, half).T

    for i in range(nd):
        for j in range(ne):
            if i or j:
                src = slot(lax.rem(d + i, nd), lax.rem(e + j, ne))
                wait_in(lbuf.at[src], l_r.at[src])
    total = lbuf[0]
    for k in range(1, nd * ne):
        total = total + lbuf[k]
    load_ref[...] = total

    for c in sends:
        c.wait_send()
    for go, c in guarded:
        pl.when(go)(c.wait_send)


def finish_kernel(
    nm, a_ref, b_ref, ht_ref, end_a, end_b, load_ref, out_ref, total_ref, stage_a, stage_b, sem
):
    ca, cb = a_ref.shape[2], b_ref.shape[1] // nm
    width = ca + cb
    copies = []

    def write(src, at, cols):
        copy = pltpu.make_async_copy(src, out_ref.at[0, :, pl.ds(at, cols)], sem.at[len(copies)])
        copy.start()
        copies.append(copy)

    stage_b[...] = b_ref[...] + jnp.dot(ht_ref[...], end_b[...], preferred_element_type=jnp.float32)
    for q in range(nm):
        write(stage_b.at[:, pl.ds(q * cb, cb)], q * width + ca, cb)
    for q in range(nm):
        stage_a[q] = a_ref[q] + jnp.dot(ht_ref[...], end_a[q], preferred_element_type=jnp.float32)
        write(stage_a.at[q], q * width, ca)
    total_ref[...] = load_ref[0:1, : total_ref.shape[1]]
    for copy in copies:
        copy.wait()


def fast_body(hidden, cotangent, routes, combine, block_pair, lengths, log_ratio):
    nd, ne, nm = lax.axis_size("dp"), lax.axis_size("expert"), lax.axis_size("mp")
    toks, top, ff = hidden.shape
    width = cotangent.shape[1]
    most = 3 * toks // 4
    cb = width // 4 // LANES * LANES
    ca = width - cb
    half = ff // nd
    srcs = nd * ne
    rows8 = -(-ne // 8) * 8
    whole = most // 256 * 256
    dims = (nd, ne, nm, most, ca, cb)
    bf16, f32 = jnp.bfloat16, jnp.float32
    vmem = pl.BlockSpec(memory_space=pltpu.VMEM)
    hbm = pl.BlockSpec(memory_space=pltpu.HBM)
    dma = pltpu.SemaphoreType.DMA
    depth = srcs * (most - whole)
    results = pl.pallas_call(
        functools.partial(exchange_kernel, dims),
        out_shape=(
            pltpu.VMEM((nm, half, ca), f32),
            pltpu.VMEM((half, nm * cb), f32),
            pltpu.VMEM((half, depth), bf16),
            pltpu.VMEM((nm, depth, ca), bf16),
            pltpu.VMEM((depth, nm * cb), bf16),
            pltpu.VMEM((rows8, LANES), f32),
        ),
        in_specs=[hbm] * 7,
        out_specs=(vmem,) * 6,
        scratch_shapes=[
            pltpu.VMEM((toks, top, ff), bf16),
            pltpu.VMEM(cotangent.shape, bf16),
            pltpu.VMEM((top, toks), jnp.int32),
            pltpu.VMEM((top, toks), f32),
            pltpu.VMEM(block_pair.shape, jnp.int32),
            pltpu.VMEM(lengths.shape, jnp.int32),
            pltpu.VMEM(log_ratio.shape, f32),
            pltpu.VMEM((srcs, most, half), bf16),
            pltpu.VMEM((nm, srcs, most, ca), bf16),
            pltpu.VMEM((srcs, most, nm * cb), bf16),
            pltpu.VMEM((ne, nd, most, half), bf16),
            pltpu.VMEM((most, ca), bf16),
            pltpu.VMEM((most, nm * cb), bf16),
            pltpu.VMEM((nm, toks, cb), bf16),
            pltpu.VMEM((srcs, rows8, LANES), f32),
            pltpu.VMEM((nd, most, half), bf16),
            pltpu.VMEM((most, ca), bf16),
            pltpu.VMEM((most, nm * cb), bf16),
            pltpu.VMEM((toks, ca), bf16),
            pltpu.VMEM((nm, toks, cb), bf16),
            pltpu.VMEM((2 * ne, toks), f32),
            pltpu.VMEM((2 * ne, toks), f32),
            pltpu.VMEM((3, half, 2 * whole), bf16),
            pltpu.VMEM((half, whole), bf16),
            dma((7,)),
            dma((1,)),
            dma((nm, srcs)),
            dma((1,)),
            dma((3,)),
            dma((3,)),
            dma((nm, ne)),
            dma((nm, ne)),
            dma((nm, ne)),
            dma((nm,)),
            dma((nm,)),
            dma((1,)),
            dma((srcs,)),
            dma((1,)),
            dma((ne,)),
            dma((ne, nd)),
            dma((srcs,)),
            dma((nd,)),
            dma((srcs,)),
            dma((nd,)),
            dma((nd,)),
            dma((nd,)),
            dma((srcs,)),
            dma((srcs,)),
        ],
        compiler_params=pltpu.CompilerParams(
            collective_id=0, has_side_effects=True, vmem_limit_bytes=VMEM_MOST - 12 * 1024 * 1024
        ),
    )(hidden, cotangent, routes.T, combine.T, block_pair, lengths, log_ratio)
    grad_down, total = pl.pallas_call(
        functools.partial(finish_kernel, nm),
        out_shape=(jax.ShapeDtypeStruct((1, half, nm * width), f32), jax.ShapeDtypeStruct((1, ne), f32)),
        in_specs=[vmem] * 6,
        out_specs=(hbm, vmem),
        scratch_shapes=[pltpu.VMEM((nm, half, ca), f32), pltpu.VMEM((half, nm * cb), f32), dma((2 * nm,))],
        compiler_params=pltpu.CompilerParams(vmem_limit_bytes=VMEM_MOST // 4),
    )(*results)
    return grad_down, total.reshape(ne)


def plain_body(hidden, cotangent, routes, combine, block_pair, lengths, log_ratio):
    per_token, within = token_factors(block_pair, lengths, log_ratio, LEN)
    weight = combine * per_token[:, None]
    tok_rows = routes.shape[0]
    route_top = routes.shape[1]
    ff_local = hidden.shape[2]
    groups = lax.axis_size("expert")
    experts = groups * EXP_DEV
    most_rows = 3 * tok_rows // 4
    labels = jnp.arange(experts, dtype=jnp.int32)
    routed = routes[:, :, None] == labels[None, None, :]
    local_load = jnp.sum(jnp.where(routed & within[:, None, None], 1.0, 0.0), axis=(0, 1)).astype(
        jnp.float32
    )
    flat_rows = tok_rows * route_top
    flat_hits = routed.reshape(flat_rows, experts).astype(jnp.int32)
    rank_of = jnp.sum((jnp.cumsum(flat_hits, axis=0) - 1) * flat_hits, axis=1)
    slot_of = routes.reshape(flat_rows) * most_rows + rank_of
    source = (
        jnp.zeros((experts * most_rows,), jnp.int32)
        .at[slot_of]
        .set(jnp.arange(flat_rows, dtype=jnp.int32))
    )
    filled = jnp.zeros((experts * most_rows,), jnp.float32).at[slot_of].set(1.0)
    token_of = source // route_top
    slot_weight = jnp.take(weight.reshape(flat_rows), source) * filled
    packed_h = jnp.take(hidden.reshape(flat_rows, ff_local), source, axis=0).reshape(
        groups, EXP_DEV * most_rows, ff_local
    )
    narrow_s = (
        slot_weight[:, None] * jnp.take(cotangent, token_of, axis=0).astype(jnp.float32)
    ).astype(jnp.bfloat16)
    moved_h, narrow = (
        lax.all_to_all(packed_h, "expert", split_axis=0, concat_axis=0, tiled=True),
        lax.all_to_all(
            narrow_s.reshape(groups, EXP_DEV * most_rows, cotangent.shape[1]),
            "expert",
            split_axis=0,
            concat_axis=0,
            tiled=True,
        ),
    )
    moved_s = lax.all_gather(narrow, "mp", axis=2, tiled=True)
    moved_h = moved_h.reshape(groups, EXP_DEV, most_rows, ff_local)
    moved_s = moved_s.reshape(groups, EXP_DEV, most_rows, moved_s.shape[2])
    products = [
        lax.dot_general(
            moved_h[:, 0],
            moved_s[:, 0],
            (((0, 1), (0, 1)), ((), ())),
            preferred_element_type=jnp.float32,
        )
    ]
    owned = lax.psum_scatter(jnp.stack(products, axis=1), "dp", scatter_dimension=0, tiled=True)
    grad_down = jnp.transpose(owned, (1, 0, 2))
    expert_load = lax.psum(local_load, ("dp", "expert"))
    return (grad_down, expert_load)


def solution(mesh):
    in_specs = (
        P(("dp", "expert"), None, "mp"),
        P(("dp", "expert"), "mp"),
        P(("dp", "expert"), None),
        P(("dp", "expert"), None),
        P(("dp", "expert"), None),
        P(("dp", "expert"), None),
        P(("dp", "expert"), None),
    )
    out_specs = (P("expert", ("mp", "dp"), None), P())

    def body(hidden, cotangent, *rest):
        rows = mesh.shape["dp"] * mesh.shape["expert"] * (3 * hidden.shape[0] // 4)
        bytes_in = 2 * rows * (cotangent.shape[1] * mesh.shape["mp"] + hidden.shape[2])
        most = 3 * hidden.shape[0] // 4
        whole = most // 256 * 256
        square = mesh.shape["dp"] == 2 and mesh.shape["expert"] == 4 and mesh.shape["mp"] == 4
        fits = square and whole and 8 * (most - whole) == whole
        run = fast_body if fits and 2 * bytes_in < VMEM_ROOM else plain_body
        return run(hidden, cotangent, *rest)

    return jax.shard_map(body, mesh=mesh, in_specs=in_specs, out_specs=out_specs, check_vma=False)
```

```python
import functools

import jax
import jax.numpy as jnp
from jax import lax
from jax.experimental import pallas as pl
from jax.experimental.pallas import tpu as pltpu
from jax.sharding import PartitionSpec as P

EXP_DEV = 1
LEN = 32
LANES = 128
VMEM_ROOM = 48 * 1024 * 1024
VMEM_MOST = 67043328
MESH = pl.DeviceIdType.MESH


beta_scale = 0.1


def token_factors(block_pair, lengths, log_ratio, block_len):
    blocks = block_pair.shape[1]
    labels = jnp.arange(blocks, dtype=jnp.int32)
    matches = block_pair[:, :, None] == labels[None, None, :]
    by_label = jnp.sum(jnp.where(matches, log_ratio[:, :, None], 0.0), axis=1)
    margin = by_label[:, 0::2] - by_label[:, 1::2]
    pair_coef = beta_scale * jax.nn.sigmoid(-beta_scale * margin)
    owners = block_pair // 2
    pair_ids = jnp.arange(blocks // 2, dtype=jnp.int32)
    picked = owners[:, :, None] == pair_ids[None, None, :]
    block_coef = jnp.sum(jnp.where(picked, pair_coef[:, None, :], 0.0), axis=2)
    block_weight = jnp.where(block_pair % 2 == 0, -block_coef, block_coef)
    position = jnp.arange(block_len, dtype=jnp.int32)
    within = position[None, None, :] < lengths[:, :, None]
    per_token = jnp.where(within, block_weight[:, :, None], 0.0).reshape(-1)
    return per_token, within.reshape(-1)


def exchange_kernel(
    dims, h_hbm, cot_hbm, routes_hbm, combine_hbm, pair_hbm, len_hbm, ratio_hbm,
    acc_a, acc_b, ht_end, end_a, end_b, load_ref,
    h_in, cot_ref, routes_ref, combine_ref, pair_ref, len_ref, ratio_ref,
    hr, sa, sb, hs, sas, sbs, cotb, lbuf, relay_h, relay_a, relay_b, raw_a, raw_b, meta_out, meta_in, ht, ht_far,
    in_sem, s_s, up_s, dn_s, cu_s, cd_s, a_r, rw_r, cb_r, b_r, h_r, he_r, rh_r, l_r,
):
    nd, ne, nm, most, ca, cb = dims
    d, e, m = lax.axis_index("dp"), lax.axis_index("expert"), lax.axis_index("mp")
    toks, top, ff = h_in.shape
    half = ff // nd
    side = 1 - d
    ex, ey, eg = e + 1 - 2 * lax.rem(e, 2), lax.rem(e + 2, ne), ne - 1 - e
    first, second = ex + d * (ey - ex), ey + d * (ex - ey)
    dests = (e, first, second, eg)

    def slot(dd, ee):
        return ee * nd + dd

    me = slot(d, e)

    def dev(dd=None, ee=None, mm=None):
        return {"dp": d if dd is None else dd, "expert": e if ee is None else ee, "mp": m if mm is None else mm}

    S_RAW_A, S_META, S_RAW_B, S_A, S_B, S_RELAY_A, S_RELAY_B, S_SIDE_A, S_SIDE_B, S_H, S_MAIN, S_REST, S_LOAD = range(13)
    H_OWN, H_FIRST, H_SECOND, H_FAR_FIRST, H_FAR_SECOND, H_DIAG = range(6)

    def remote(src, dst, ssem, rsem, where):
        return pltpu.make_async_remote_copy(
            src_ref=src, dst_ref=dst, send_sem=ssem, recv_sem=rsem, device_id=where, device_id_type=MESH
        )

    def send(src, dst, ssem, rsem, where, go=None):
        copy = remote(src, dst, s_s.at[ssem] if isinstance(ssem, int) else ssem, rsem, where)
        if go is None:
            copy.start()
        else:
            pl.when(go)(copy.start)

    def wait_in(buf, sem, guard=None):
        c = pltpu.make_async_copy(buf, buf, sem)
        if guard is None:
            c.wait()
        else:
            pl.when(guard)(c.wait)

    loads = [
        pltpu.make_async_copy(src, dst, in_sem.at[i])
        for i, (src, dst) in enumerate((
            (routes_hbm, routes_ref), (cot_hbm, cot_ref), (pair_hbm, pair_ref), (len_hbm, len_ref),
            (ratio_hbm, ratio_ref), (combine_hbm, combine_ref), (h_hbm, h_in),
        ))
    ]
    for load in loads:
        load.start()
    barrier = pltpu.get_barrier_semaphore()
    peers = [
        dev(dd=lax.rem(d + i, nd), ee=lax.rem(e + j, ne)) for i in range(nd) for j in range(ne) if i or j
    ]
    for peer in peers:
        pl.semaphore_signal(barrier, inc=1, device_id=peer, device_id_type=MESH)
    has_up, has_down = m + 1 < nm, m > 0
    up, down = dev(mm=lax.rem(m + 1, nm)), dev(mm=lax.rem(m + nm - 1, nm))
    for go, peer in ((has_up, up), (has_down, down)):
        pl.when(go)(
            functools.partial(pl.semaphore_signal, barrier, inc=1, device_id=peer, device_id_type=MESH)
        )
    n_peers = len(peers) + jnp.where(has_up, 1, 0) + jnp.where(has_down, 1, 0)

    loads[0].wait()
    rows8 = -(-ne // 8) * 8
    row_id = lax.broadcasted_iota(jnp.int32, (rows8, 1), 0)
    owner = jnp.full((rows8, 1), -1, jnp.int32)
    for j, to in enumerate(dests):
        owner = jnp.where(row_id == j, to, owner)
    hit0 = routes_ref[0:1, :] == owner
    hit1 = routes_ref[1:2, :] == owner
    named = hit0 | hit1
    before = lax.broadcasted_iota(jnp.int32, (toks, toks), 0) < lax.broadcasted_iota(jnp.int32, (toks, toks), 1)
    tok_rank = jnp.dot(
        jnp.where(named, 1.0, 0.0).astype(jnp.bfloat16),
        jnp.where(before, 1.0, 0.0).astype(jnp.bfloat16),
        preferred_element_type=jnp.float32,
    )
    tok_rank = jnp.where(named, tok_rank, -1.0)
    tok_pos = tok_rank.astype(jnp.int32)

    for load in loads[2:-1]:
        load.wait()

    blocks = pair_ref.shape[1]
    block_len = toks // blocks
    square = (blocks, blocks)
    diagonal = lax.broadcasted_iota(jnp.int32, square, 0) == lax.broadcasted_iota(jnp.int32, square, 1)

    def column(row):
        return jnp.sum(jnp.where(diagonal, row, 0.0), axis=1, keepdims=True)

    pair, ratio = pair_ref[...], ratio_ref[...]
    chosen = lax.rem(pair, 2) == 0
    other_side = jnp.where(chosen, pair + 1, pair - 1)
    is_other = column(pair.astype(jnp.float32)) == other_side.astype(jnp.float32)
    other_ratio = jnp.sum(jnp.where(is_other, column(ratio), 0.0), axis=0, keepdims=True)
    margin = jnp.where(chosen, ratio - other_ratio, other_ratio - ratio)
    coef = beta_scale * (1.0 / (1.0 + jnp.exp(beta_scale * margin)))
    block_weight = column(jnp.where(chosen, -coef, coef))
    token_id = lax.broadcasted_iota(jnp.int32, (blocks, toks), 1)
    place = token_id - block_len * lax.broadcasted_iota(jnp.int32, (blocks, toks), 0)
    inside = (place >= 0) & (place < block_len)
    alive = inside & (place.astype(jnp.float32) < column(len_ref[...].astype(jnp.float32)))
    live = jnp.sum(jnp.where(alive, 1.0, 0.0), axis=0, keepdims=True)
    per_token = jnp.sum(jnp.where(alive, block_weight, 0.0), axis=0, keepdims=True)
    weight = combine_ref[...] * per_token
    tok_weight = jnp.where(hit0, weight[0:1, :], 0.0) + jnp.where(hit1, weight[1:2, :], 0.0)

    loads[1].wait()
    cotb[m] = cot_ref[:, ca:]
    meta_out[...] = jnp.concatenate([tok_rank[:ne], tok_weight[:ne]], axis=0)
    slot_tok = lax.broadcasted_iota(jnp.int32, (most, toks), 0)
    pl.semaphore_wait(barrier, n_peers)
    send(cot_ref.at[:, pl.ds(0, ca)], raw_a, S_RAW_A, rw_r.at[0], dev(ee=first))
    own_cols = cot_ref.at[:, pl.ds(ca, cb)]
    send(own_cols, cotb.at[m], cu_s.at[0], cb_r.at[m], up, has_up)
    send(own_cols, cotb.at[m], cd_s.at[0], cb_r.at[m], down, has_down)
    send(meta_out, meta_in, S_META, rw_r.at[1], dev(ee=first))

    def chain(k):
        return (m - k, lax.rem(m - k + nm, nm), m - k >= 0), (m + k, lax.rem(m + k, nm), m + k < nm)

    def pass_cot(k):
        (_, ql, low_here), (_, qh, high_here) = chain(k)
        for q, here, sem, to, more in ((ql, low_here, cu_s, up, has_up), (qh, high_here, cd_s, down, has_down)):
            wait_in(cotb.at[q], cb_r.at[q], here)
            if k + 1 < nm:
                send(cotb.at[q], cotb.at[q], sem.at[k], cb_r.at[q], to, here & more)

    def picker(position, factor):
        hit = slot_tok == position
        pick = jnp.where(hit, 1.0, 0.0).astype(jnp.bfloat16)
        scale = jnp.sum(jnp.where(hit, factor, 0.0), axis=1, keepdims=True)

        def pack(rows):
            rows = jnp.dot(pick, rows, preferred_element_type=jnp.float32)
            return (scale * rows).astype(jnp.bfloat16)

        return pack

    pack_own = picker(tok_pos[0:1, :], tok_weight[0:1, :])
    sa[m, me] = pack_own(cot_ref[:, :ca])

    def to_partner(q, src, guard=None):
        send(sa.at[q, src], sa.at[q, src], S_SIDE_A, a_r.at[q, src], dev(dd=side), guard)

    def spread(ej):
        src = slot(d, ej)
        block = sa.at[m, src]
        send(block, block, up_s.at[0], a_r.at[m, src], up, has_up)
        send(block, block, dn_s.at[0], a_r.at[m, src], down, has_down)
        to_partner(m, src)

    def pass_on(k, ej):
        (_, ql, low_here), (_, qh, high_here) = chain(k)
        src = slot(d, ej)
        for q, here, sem, to, more in ((ql, low_here, up_s, up, has_up), (qh, high_here, dn_s, down, has_down)):
            block = sa.at[q, src]
            wait_in(block, a_r.at[q, src], here)
            if k + 1 < nm:
                send(block, block, sem.at[k], a_r.at[q, src], to, here & more)
            to_partner(q, src, here)

    spread(e)
    pack_second = picker(tok_pos[2:3, :], tok_weight[2:3, :])
    sas[...] = pack_second(cot_ref[:, :ca])
    send(sas, sa.at[m, me], S_A, a_r.at[m, me], dev(ee=second))

    slot_flat = lax.broadcasted_iota(jnp.int32, (most, 2 * toks), 0)
    gap = lax.broadcasted_iota(jnp.int32, (toks, 2 * toks), 1) - 2 * lax.broadcasted_iota(
        jnp.int32, (toks, 2 * toks), 0
    )
    flat_pos = -1.0
    for k, hit in enumerate((hit0, hit1)):
        place_k = jnp.where(gap == k, 1.0, 0.0).astype(jnp.bfloat16)
        value = jnp.where(hit, tok_rank + 1.0, 0.0)
        high = jnp.floor(value * (1.0 / 16.0))
        for part, unit in ((high, 16.0), (value - 16.0 * high, 1.0)):
            flat_pos += unit * jnp.dot(part.astype(jnp.bfloat16), place_k, preferred_element_type=jnp.float32)
    flat_pos = flat_pos.astype(jnp.int32)
    loads[-1].wait()
    flat = (2 * toks, half)
    h_rows = [h_in[:, :, c * half : (c + 1) * half].reshape(flat) for c in range(nd)]

    def pack_h(j):
        pick = jnp.where(slot_flat == flat_pos[j : j + 1, :], 1.0, 0.0).astype(jnp.bfloat16)
        for c in range(nd):
            hs[j, c] = jnp.dot(pick, h_rows[c], preferred_element_type=jnp.float32).astype(jnp.bfloat16)

    whole = most // 256 * 256
    main, rest = pl.ds(0, whole), pl.ds(whole, most - whole)
    pack_h(3)
    for c in range(nd):
        send(hs.at[3, c], relay_h.at[c], S_H, rh_r.at[c], dev(ee=first))
    pass_cot(1)
    pack_h(2)
    wait_in(meta_in, rw_r.at[1])
    wait_in(raw_a, rw_r.at[0])
    from_first = slot(d, first)
    pack_relay = picker(meta_in[3:4, :].astype(jnp.int32), meta_in[ne + 3 : ne + 4, :])
    relay_a[...] = pack_relay(raw_a[...])
    send(relay_a, sa.at[m, from_first], S_RELAY_A, a_r.at[m, from_first], dev(ee=second))
    send(hs.at[2, d, main], hr.at[me, main], S_MAIN, h_r.at[H_SECOND], dev(dd=d, ee=second))
    pack_first = picker(meta_in[1:2, :].astype(jnp.int32), meta_in[ne + 1 : ne + 2, :])
    sa[m, from_first] = pack_first(raw_a[...])
    spread(first)
    pass_cot(2)
    wait_in(sa.at[m, slot(d, second)], a_r.at[m, slot(d, second)])
    spread(second)
    pack_h(0)
    send(hs.at[0, side], hr.at[me], S_H, h_r.at[H_OWN], dev(dd=side))
    hr[me] = hs[0, d]
    pack_h(1)

    in_order = (routes_ref[0:1, :] == row_id) | (routes_ref[1:2, :] == row_id)
    counts = jnp.sum(jnp.where(in_order, live, 0.0), axis=1, keepdims=True)
    lanes8 = lax.broadcasted_iota(jnp.int32, (rows8, LANES), 1) == row_id
    lbuf[me] = jnp.broadcast_to(jnp.sum(jnp.where(lanes8, counts, 0.0), axis=0, keepdims=True), (rows8, LANES))

    pass_cot(3)
    send(cotb, raw_b, S_RAW_B, rw_r.at[2], dev(ee=first))
    dense = jnp.concatenate([cotb[q] for q in range(nm)], axis=1)
    sbs[...] = pack_second(dense)
    send(sbs, sb.at[me], S_B, b_r.at[me], dev(ee=second))
    sb[me] = pack_own(dense)
    send(sb.at[me], sb.at[me], S_SIDE_B, b_r.at[me], dev(dd=side))

    def share_b(ej):
        src = slot(d, ej)
        wait_in(sb.at[src], b_r.at[src])
        send(sb.at[src], sb.at[src], S_SIDE_B, b_r.at[src], dev(dd=side))

    for i in range(nd):
        for j in range(ne):
            if i or j:
                to = dev(dd=lax.rem(d + i, nd), ee=lax.rem(e + j, ne))
                send(lbuf.at[me], lbuf.at[me], S_LOAD, l_r.at[0], to)

    for c, role in ((d, H_FIRST), (side, H_FAR_FIRST)):
        send(hs.at[1, c], hr.at[me], S_H, h_r.at[role], dev(dd=c, ee=first))

    def nearest(r):
        near = jnp.minimum(m, nm - 1 - m)
        both = m + (r + 1) // 2 * (1 if r % 2 == 0 else -1)
        far = jnp.where(m < nm - 1 - m, m + r - near, m - r + near)
        return jnp.where(r <= 2 * near, both, far)

    def put(ref, index, value, fresh):
        if fresh:
            ref[index] = value
        else:
            ref[index] = ref[index] + value

    def unit(r, left, cut, fresh=False):
        if r < nm:
            q = nearest(r)
            put(acc_a, q, jnp.dot(left[...], cut(sa.at[q]), preferred_element_type=jnp.float32), fresh)
        else:
            put(acc_b, ..., jnp.dot(left[...], cut(sb), preferred_element_type=jnp.float32), fresh)

    def rows_of(s0, s1, at, rows):
        def cut(ref):
            return jnp.concatenate([ref[s0, at : at + rows], ref[s1, at : at + rows]], axis=0)

        return cut

    def turn(s0, s1, at, rows):
        return jnp.concatenate([hr[s0, at : at + rows], hr[s1, at : at + rows]], axis=0).T

    def partner_a(r, ej):
        q = nearest(r)
        src = slot(side, ej)
        wait_in(sa.at[q, src], a_r.at[q, src])

    def partner_b(ej):
        src = slot(side, ej)
        wait_in(sb.at[src], b_r.at[src])

    def wait_h(src, role):
        wait_in(hr.at[src], h_r.at[role])

    def wait_main(src, role):
        wait_in(hr.at[src, main], h_r.at[role])

    B = nm
    own = rows_of(slot(0, e), slot(1, e), 0, whole)
    diag = rows_of(slot(0, eg), slot(1, eg), 0, whole)
    same = rows_of(slot(d, ex), slot(d, ey), 0, whole)

    pass_on(1, e)
    wait_in(sa.at[m, slot(d, eg)], a_r.at[m, slot(d, eg)])
    spread(eg)
    pass_on(1, first)
    pass_on(1, second)
    wait_h(slot(side, e), H_OWN)
    ht[0] = turn(slot(0, e), slot(1, e), 0, whole)
    partner_a(0, e)
    unit(0, ht.at[0], own, True)
    wait_in(relay_h.at[0], rh_r.at[0])
    send(relay_h.at[0, main], hr.at[from_first, main], S_MAIN, h_r.at[H_DIAG], dev(dd=0, ee=second))
    partner_b(e)
    unit(B, ht.at[0], own, True)
    pass_on(1, eg)
    share_b(second)
    partner_a(1, e)
    unit(1, ht.at[0], own, True)
    pass_on(2, e)
    wait_in(relay_h.at[1], rh_r.at[1])
    send(relay_h.at[1, main], hr.at[from_first, main], S_MAIN, h_r.at[H_DIAG], dev(dd=1, ee=second))
    pass_on(2, first)
    wait_in(raw_b, rw_r.at[2])
    dense = jnp.concatenate([raw_b[q] for q in range(nm)], axis=1)
    relay_b[...] = pack_relay(dense)
    send(relay_b, sb.at[from_first], S_RELAY_B, b_r.at[from_first], dev(ee=second))
    send(hs.at[2, side, main], hr.at[me, main], S_MAIN, h_r.at[H_FAR_SECOND], dev(dd=side, ee=second))
    for c in range(nd):
        send(hs.at[2, c, rest], hr.at[me, rest], S_REST, he_r.at[0], dev(dd=c, ee=second))
    for c in range(nd):
        send(relay_h.at[c, rest], hr.at[from_first, rest], S_REST, he_r.at[0], dev(dd=c, ee=second))
    sb[from_first] = pack_first(dense)
    send(sb.at[from_first], sb.at[from_first], S_SIDE_B, b_r.at[from_first], dev(dd=side))
    pass_on(2, second)
    pass_on(2, eg)
    partner_a(2, e)
    unit(2, ht.at[0], own, True)
    pass_on(3, e)
    partner_a(3, e)
    unit(3, ht.at[0], own, True)
    wait_h(slot(d, first), H_FIRST)
    wait_main(slot(d, second), H_SECOND)
    ht[2] = turn(slot(d, ex), slot(d, ey), 0, whole)
    for r in range(nm - 1):
        unit(r, ht.at[2], same)
    unit(B, ht.at[2], same)
    pairs = hr.at[pl.ds(slot(0, eg), nd), main]
    wait_in(pairs, h_r.at[H_DIAG])
    ht[1] = turn(slot(0, eg), slot(1, eg), 0, whole)
    for r in range(nm - 1):
        partner_a(r, eg)
        unit(r, ht.at[1], diag)
    share_b(eg)
    partner_b(eg)
    unit(B, ht.at[1], diag)
    ends = (slot(side, second), second), (slot(side, first), first)

    def far(n, r):
        src, ej = ends[n]
        if r < nm:
            partner_a(r, ej)
        else:
            partner_b(ej)
        unit(r, ht_far.at[n], lambda ref: ref[src, :whole])

    wait_h(ends[0][0], H_FAR_FIRST)
    ht_far[0] = hr[ends[0][0], :whole].T
    for r in (0, 1, 2, B):
        far(0, r)
    pass_on(3, first)
    pass_on(3, second)
    unit(nm - 1, ht.at[2], same)
    far(0, nm - 1)
    wait_main(ends[1][0], H_FAR_SECOND)
    ht_far[1] = hr[ends[1][0], :whole].T
    for r in (0, 1, 2, B, 3):
        far(1, r)
    pass_on(3, eg)
    partner_a(nm - 1, eg)
    unit(nm - 1, ht.at[1], diag)
    depth = nd * ne * (most - whole)
    for q in range(nm):
        end_a[q] = sa[q, :, whole:, :].reshape(depth, ca)
    end_b[...] = sb[:, whole:, :].reshape(depth, nm * cb)
    wait_in(hr.at[pl.ds(0, 2 * nd), rest], he_r.at[0])
    ht_end[...] = hr[:, whole:, :].reshape(depth, half).T

    others = nd * ne - 1
    wait_in(lbuf.at[pl.ds(0, others)], l_r.at[0])
    total = lbuf[0]
    for k in range(1, nd * ne):
        total = total + lbuf[k]
    load_ref[...] = total

    for ref, sem in (
        (cot_ref.at[:, pl.ds(0, ca)], S_RAW_A), (meta_out, S_META), (cotb, S_RAW_B), (sas, S_A), (sbs, S_B),
        (relay_a, S_RELAY_A), (relay_b, S_RELAY_B), (sa.at[:, pl.ds(0, ne)], S_SIDE_A), (sb.at[pl.ds(0, ne)], S_SIDE_B),
        (hr.at[pl.ds(0, 2 * nd + 1)], S_H), (hr.at[pl.ds(0, 2 * nd), main], S_MAIN),
        (hr.at[pl.ds(0, 2 * nd), rest], S_REST), (lbuf.at[pl.ds(0, others)], S_LOAD),
    ):
        wait_in(ref, s_s.at[sem])
    blocks_a = sa.at[0, pl.ds(0, ne)]
    for k in range(nm - 1):
        for go, sems, ref in (
            ((m - k >= 0) & has_up, (up_s, cu_s), cotb.at[0]), ((m + k < nm) & has_down, (dn_s, cd_s), cotb.at[0])
        ):
            wait_in(blocks_a, sems[0].at[k], go)
            wait_in(ref, sems[1].at[k], go)


def finish_kernel(
    nm, a_ref, b_ref, ht_ref, end_a, end_b, load_ref, out_ref, total_ref, stage_a, stage_b, sem
):
    ca, cb = a_ref.shape[2], b_ref.shape[1] // nm
    width = ca + cb
    copies = []

    def write(src, at, cols):
        copy = pltpu.make_async_copy(src, out_ref.at[0, :, pl.ds(at, cols)], sem.at[len(copies)])
        copy.start()
        copies.append(copy)

    stage_b[...] = b_ref[...] + jnp.dot(ht_ref[...], end_b[...], preferred_element_type=jnp.float32)
    for q in range(nm):
        write(stage_b.at[:, pl.ds(q * cb, cb)], q * width + ca, cb)
    for q in range(nm):
        stage_a[q] = a_ref[q] + jnp.dot(ht_ref[...], end_a[q], preferred_element_type=jnp.float32)
        write(stage_a.at[q], q * width, ca)
    total_ref[...] = load_ref[0:1, : total_ref.shape[1]]
    for copy in copies:
        copy.wait()


def fast_body(hidden, cotangent, routes, combine, block_pair, lengths, log_ratio):
    nd, ne, nm = lax.axis_size("dp"), lax.axis_size("expert"), lax.axis_size("mp")
    toks, top, ff = hidden.shape
    width = cotangent.shape[1]
    most = 3 * toks // 4
    cb = width // 4 // LANES * LANES
    ca = width - cb
    half = ff // nd
    srcs = nd * ne
    rows8 = -(-ne // 8) * 8
    whole = most // 256 * 256
    dims = (nd, ne, nm, most, ca, cb)
    bf16, f32 = jnp.bfloat16, jnp.float32
    vmem = pl.BlockSpec(memory_space=pltpu.VMEM)
    hbm = pl.BlockSpec(memory_space=pltpu.HBM)
    dma = pltpu.SemaphoreType.DMA
    depth = srcs * (most - whole)
    results = pl.pallas_call(
        functools.partial(exchange_kernel, dims),
        out_shape=(
            pltpu.VMEM((nm, half, ca), f32),
            pltpu.VMEM((half, nm * cb), f32),
            pltpu.VMEM((half, depth), bf16),
            pltpu.VMEM((nm, depth, ca), bf16),
            pltpu.VMEM((depth, nm * cb), bf16),
            pltpu.VMEM((rows8, LANES), f32),
        ),
        in_specs=[hbm] * 7,
        out_specs=(vmem,) * 6,
        scratch_shapes=[
            pltpu.VMEM((toks, top, ff), bf16),
            pltpu.VMEM(cotangent.shape, bf16),
            pltpu.VMEM((top, toks), jnp.int32),
            pltpu.VMEM((top, toks), f32),
            pltpu.VMEM(block_pair.shape, jnp.int32),
            pltpu.VMEM(lengths.shape, jnp.int32),
            pltpu.VMEM(log_ratio.shape, f32),
            pltpu.VMEM((srcs, most, half), bf16),
            pltpu.VMEM((nm, srcs, most, ca), bf16),
            pltpu.VMEM((srcs, most, nm * cb), bf16),
            pltpu.VMEM((ne, nd, most, half), bf16),
            pltpu.VMEM((most, ca), bf16),
            pltpu.VMEM((most, nm * cb), bf16),
            pltpu.VMEM((nm, toks, cb), bf16),
            pltpu.VMEM((srcs, rows8, LANES), f32),
            pltpu.VMEM((nd, most, half), bf16),
            pltpu.VMEM((most, ca), bf16),
            pltpu.VMEM((most, nm * cb), bf16),
            pltpu.VMEM((toks, ca), bf16),
            pltpu.VMEM((nm, toks, cb), bf16),
            pltpu.VMEM((2 * ne, toks), f32),
            pltpu.VMEM((2 * ne, toks), f32),
            pltpu.VMEM((3, half, 2 * whole), bf16),
            pltpu.VMEM((2, half, whole), bf16),
            dma((7,)),
            dma((13,)),
            dma((nm - 1,)),
            dma((nm - 1,)),
            dma((nm - 1,)),
            dma((nm - 1,)),
            dma((nm, srcs)),
            dma((3,)),
            dma((nm,)),
            dma((srcs,)),
            dma((6,)),
            dma((1,)),
            dma((nd,)),
            dma((1,)),
        ],
        compiler_params=pltpu.CompilerParams(
            collective_id=0, has_side_effects=True, vmem_limit_bytes=VMEM_MOST - 12 * 1024 * 1024
        ),
    )(hidden, cotangent, routes.T, combine.T, block_pair, lengths, log_ratio)
    grad_down, total = pl.pallas_call(
        functools.partial(finish_kernel, nm),
        out_shape=(jax.ShapeDtypeStruct((1, half, nm * width), f32), jax.ShapeDtypeStruct((1, ne), f32)),
        in_specs=[vmem] * 6,
        out_specs=(hbm, vmem),
        scratch_shapes=[pltpu.VMEM((nm, half, ca), f32), pltpu.VMEM((half, nm * cb), f32), dma((2 * nm,))],
        compiler_params=pltpu.CompilerParams(vmem_limit_bytes=VMEM_MOST // 4),
    )(*results)
    return grad_down, total.reshape(ne)


def plain_body(hidden, cotangent, routes, combine, block_pair, lengths, log_ratio):
    per_token, within = token_factors(block_pair, lengths, log_ratio, LEN)
    weight = combine * per_token[:, None]
    tok_rows = routes.shape[0]
    route_top = routes.shape[1]
    ff_local = hidden.shape[2]
    groups = lax.axis_size("expert")
    experts = groups * EXP_DEV
    most_rows = 3 * tok_rows // 4
    labels = jnp.arange(experts, dtype=jnp.int32)
    routed = routes[:, :, None] == labels[None, None, :]
    local_load = jnp.sum(jnp.where(routed & within[:, None, None], 1.0, 0.0), axis=(0, 1)).astype(
        jnp.float32
    )
    flat_rows = tok_rows * route_top
    flat_hits = routed.reshape(flat_rows, experts).astype(jnp.int32)
    rank_of = jnp.sum((jnp.cumsum(flat_hits, axis=0) - 1) * flat_hits, axis=1)
    slot_of = routes.reshape(flat_rows) * most_rows + rank_of
    source = (
        jnp.zeros((experts * most_rows,), jnp.int32)
        .at[slot_of]
        .set(jnp.arange(flat_rows, dtype=jnp.int32))
    )
    filled = jnp.zeros((experts * most_rows,), jnp.float32).at[slot_of].set(1.0)
    token_of = source // route_top
    slot_weight = jnp.take(weight.reshape(flat_rows), source) * filled
    packed_h = jnp.take(hidden.reshape(flat_rows, ff_local), source, axis=0).reshape(
        groups, EXP_DEV * most_rows, ff_local
    )
    narrow_s = (
        slot_weight[:, None] * jnp.take(cotangent, token_of, axis=0).astype(jnp.float32)
    ).astype(jnp.bfloat16)
    moved_h, narrow = (
        lax.all_to_all(packed_h, "expert", split_axis=0, concat_axis=0, tiled=True),
        lax.all_to_all(
            narrow_s.reshape(groups, EXP_DEV * most_rows, cotangent.shape[1]),
            "expert",
            split_axis=0,
            concat_axis=0,
            tiled=True,
        ),
    )
    moved_s = lax.all_gather(narrow, "mp", axis=2, tiled=True)
    moved_h = moved_h.reshape(groups, EXP_DEV, most_rows, ff_local)
    moved_s = moved_s.reshape(groups, EXP_DEV, most_rows, moved_s.shape[2])
    products = [
        lax.dot_general(
            moved_h[:, 0],
            moved_s[:, 0],
            (((0, 1), (0, 1)), ((), ())),
            preferred_element_type=jnp.float32,
        )
    ]
    owned = lax.psum_scatter(jnp.stack(products, axis=1), "dp", scatter_dimension=0, tiled=True)
    grad_down = jnp.transpose(owned, (1, 0, 2))
    expert_load = lax.psum(local_load, ("dp", "expert"))
    return (grad_down, expert_load)


def solution(mesh):
    in_specs = (
        P(("dp", "expert"), None, "mp"),
        P(("dp", "expert"), "mp"),
        P(("dp", "expert"), None),
        P(("dp", "expert"), None),
        P(("dp", "expert"), None),
        P(("dp", "expert"), None),
        P(("dp", "expert"), None),
    )
    out_specs = (P("expert", ("mp", "dp"), None), P())

    def body(hidden, cotangent, *rest):
        rows = mesh.shape["dp"] * mesh.shape["expert"] * (3 * hidden.shape[0] // 4)
        bytes_in = 2 * rows * (cotangent.shape[1] * mesh.shape["mp"] + hidden.shape[2])
        most = 3 * hidden.shape[0] // 4
        whole = most // 256 * 256
        square = mesh.shape["dp"] == 2 and mesh.shape["expert"] == 4 and mesh.shape["mp"] == 4
        fits = square and whole and 8 * (most - whole) == whole
        run = fast_body if fits and 2 * bytes_in < VMEM_ROOM else plain_body
        return run(hidden, cotangent, *rest)

    return jax.shard_map(body, mesh=mesh, in_specs=in_specs, out_specs=out_specs, check_vma=False)
```

```python
import functools

import jax
import jax.numpy as jnp
from jax import lax
from jax.experimental import pallas as pl
from jax.experimental.pallas import tpu as pltpu
from jax.sharding import PartitionSpec as P

EXP_DEV = 1
LEN = 32
LANES = 128
VMEM_ROOM = 48 * 1024 * 1024
VMEM_MOST = 67043328
MESH = pl.DeviceIdType.MESH


beta_scale = 0.1


def token_factors(block_pair, lengths, log_ratio, block_len):
    blocks = block_pair.shape[1]
    labels = jnp.arange(blocks, dtype=jnp.int32)
    matches = block_pair[:, :, None] == labels[None, None, :]
    by_label = jnp.sum(jnp.where(matches, log_ratio[:, :, None], 0.0), axis=1)
    margin = by_label[:, 0::2] - by_label[:, 1::2]
    pair_coef = beta_scale * jax.nn.sigmoid(-beta_scale * margin)
    owners = block_pair // 2
    pair_ids = jnp.arange(blocks // 2, dtype=jnp.int32)
    picked = owners[:, :, None] == pair_ids[None, None, :]
    block_coef = jnp.sum(jnp.where(picked, pair_coef[:, None, :], 0.0), axis=2)
    block_weight = jnp.where(block_pair % 2 == 0, -block_coef, block_coef)
    position = jnp.arange(block_len, dtype=jnp.int32)
    within = position[None, None, :] < lengths[:, :, None]
    per_token = jnp.where(within, block_weight[:, :, None], 0.0).reshape(-1)
    return per_token, within.reshape(-1)


def exchange_kernel(
    dims, h_hbm, cot_hbm, routes_hbm, combine_hbm, pair_hbm, len_hbm, ratio_hbm,
    acc_a, acc_b, ht_end, end_a, end_b, load_ref,
    h_in, cot_ref, routes_ref, combine_ref, pair_ref, len_ref, ratio_ref,
    hr, sa, sb, hs, sas, sbs, cotb, lbuf, relay_h, relay_a, relay_b, raw_a, raw_b, meta_out, meta_in, ht, ht_far,
    in_sem, s_s, up_s, dn_s, cu_s, cd_s, a_r, rw_r, cb_r, b_r, h_r, he_r, rh_r, l_r,
):
    nd, ne, nm, most, ca, cb = dims
    d, e, m = lax.axis_index("dp"), lax.axis_index("expert"), lax.axis_index("mp")
    toks, top, ff = h_in.shape
    half = ff // nd
    side = 1 - d
    ex, ey, eg = e + 1 - 2 * lax.rem(e, 2), lax.rem(e + 2, ne), ne - 1 - e
    first, second = ex + d * (ey - ex), ey + d * (ex - ey)
    dests = (e, first, second, eg)

    def slot(dd, ee):
        return ee * nd + dd

    me = slot(d, e)

    def dev(dd=None, ee=None, mm=None):
        return {"dp": d if dd is None else dd, "expert": e if ee is None else ee, "mp": m if mm is None else mm}

    S_RAW_A, S_META, S_RAW_B, S_A, S_B, S_RELAY_A, S_RELAY_B, S_SIDE_A, S_SIDE_B, S_H, S_MAIN, S_REST, S_LOAD = range(13)
    H_OWN, H_FIRST, H_SECOND, H_FAR_FIRST, H_FAR_SECOND, H_DIAG = range(6)

    def remote(src, dst, ssem, rsem, where):
        return pltpu.make_async_remote_copy(
            src_ref=src, dst_ref=dst, send_sem=ssem, recv_sem=rsem, device_id=where, device_id_type=MESH
        )

    def send(src, dst, ssem, rsem, where, go=None):
        copy = remote(src, dst, s_s.at[ssem] if isinstance(ssem, int) else ssem, rsem, where)
        if go is None:
            copy.start()
        else:
            pl.when(go)(copy.start)

    def wait_in(buf, sem, guard=None):
        c = pltpu.make_async_copy(buf, buf, sem)
        if guard is None:
            c.wait()
        else:
            pl.when(guard)(c.wait)

    loads = [
        pltpu.make_async_copy(src, dst, in_sem.at[i])
        for i, (src, dst) in enumerate((
            (routes_hbm, routes_ref), (cot_hbm, cot_ref), (pair_hbm, pair_ref), (len_hbm, len_ref),
            (ratio_hbm, ratio_ref), (combine_hbm, combine_ref), (h_hbm, h_in),
        ))
    ]
    for load in loads:
        load.start()
    barrier = pltpu.get_barrier_semaphore()
    peers = [
        dev(dd=lax.rem(d + i, nd), ee=lax.rem(e + j, ne)) for i in range(nd) for j in range(ne) if i or j
    ]
    for peer in peers:
        pl.semaphore_signal(barrier, inc=1, device_id=peer, device_id_type=MESH)
    has_up, has_down = m + 1 < nm, m > 0
    up, down = dev(mm=lax.rem(m + 1, nm)), dev(mm=lax.rem(m + nm - 1, nm))
    for go, peer in ((has_up, up), (has_down, down)):
        pl.when(go)(
            functools.partial(pl.semaphore_signal, barrier, inc=1, device_id=peer, device_id_type=MESH)
        )
    n_peers = len(peers) + jnp.where(has_up, 1, 0) + jnp.where(has_down, 1, 0)

    loads[0].wait()
    rows8 = -(-ne // 8) * 8
    row_id = lax.broadcasted_iota(jnp.int32, (rows8, 1), 0)
    owner = jnp.full((rows8, 1), -1, jnp.int32)
    for j, to in enumerate(dests):
        owner = jnp.where(row_id == j, to, owner)
    hit0 = routes_ref[0:1, :] == owner
    hit1 = routes_ref[1:2, :] == owner
    named = hit0 | hit1
    before = lax.broadcasted_iota(jnp.int32, (toks, toks), 0) < lax.broadcasted_iota(jnp.int32, (toks, toks), 1)
    tok_rank = jnp.dot(
        jnp.where(named, 1.0, 0.0).astype(jnp.bfloat16),
        jnp.where(before, 1.0, 0.0).astype(jnp.bfloat16),
        preferred_element_type=jnp.float32,
    )
    tok_rank = jnp.where(named, tok_rank, -1.0)
    tok_pos = tok_rank.astype(jnp.int32)

    for load in loads[2:-1]:
        load.wait()

    blocks = pair_ref.shape[1]
    block_len = toks // blocks
    square = (blocks, blocks)
    diagonal = lax.broadcasted_iota(jnp.int32, square, 0) == lax.broadcasted_iota(jnp.int32, square, 1)

    def column(row):
        return jnp.sum(jnp.where(diagonal, row, 0.0), axis=1, keepdims=True)

    pair, ratio = pair_ref[...], ratio_ref[...]
    chosen = lax.rem(pair, 2) == 0
    other_side = jnp.where(chosen, pair + 1, pair - 1)
    is_other = column(pair.astype(jnp.float32)) == other_side.astype(jnp.float32)
    other_ratio = jnp.sum(jnp.where(is_other, column(ratio), 0.0), axis=0, keepdims=True)
    margin = jnp.where(chosen, ratio - other_ratio, other_ratio - ratio)
    coef = beta_scale * (1.0 / (1.0 + jnp.exp(beta_scale * margin)))
    block_weight = column(jnp.where(chosen, -coef, coef))
    token_id = lax.broadcasted_iota(jnp.int32, (blocks, toks), 1)
    place = token_id - block_len * lax.broadcasted_iota(jnp.int32, (blocks, toks), 0)
    inside = (place >= 0) & (place < block_len)
    alive = inside & (place.astype(jnp.float32) < column(len_ref[...].astype(jnp.float32)))
    live = jnp.sum(jnp.where(alive, 1.0, 0.0), axis=0, keepdims=True)
    per_token = jnp.sum(jnp.where(alive, block_weight, 0.0), axis=0, keepdims=True)
    weight = combine_ref[...] * per_token
    tok_weight = jnp.where(hit0, weight[0:1, :], 0.0) + jnp.where(hit1, weight[1:2, :], 0.0)

    loads[1].wait()
    cotb[m] = cot_ref[:, ca:]
    meta_out[...] = jnp.concatenate([tok_rank[:ne], tok_weight[:ne]], axis=0)
    slot_tok = lax.broadcasted_iota(jnp.int32, (most, toks), 0)
    pl.semaphore_wait(barrier, n_peers)
    send(cot_ref.at[:, pl.ds(0, ca)], raw_a, S_RAW_A, rw_r.at[0], dev(ee=first))
    own_cols = cot_ref.at[:, pl.ds(ca, cb)]
    send(own_cols, cotb.at[m], cu_s.at[0], cb_r.at[m], up, has_up)
    send(own_cols, cotb.at[m], cd_s.at[0], cb_r.at[m], down, has_down)
    send(meta_out, meta_in, S_META, rw_r.at[1], dev(ee=first))

    def chain(k):
        return (m - k, lax.rem(m - k + nm, nm), m - k >= 0), (m + k, lax.rem(m + k, nm), m + k < nm)

    def pass_cot(k):
        (_, ql, low_here), (_, qh, high_here) = chain(k)
        for q, here, sem, to, more in ((ql, low_here, cu_s, up, has_up), (qh, high_here, cd_s, down, has_down)):
            wait_in(cotb.at[q], cb_r.at[q], here)
            if k + 1 < nm:
                send(cotb.at[q], cotb.at[q], sem.at[k], cb_r.at[q], to, here & more)

    def picker(position, factor):
        hit = slot_tok == position
        pick = jnp.where(hit, 1.0, 0.0).astype(jnp.bfloat16)
        scale = jnp.sum(jnp.where(hit, factor, 0.0), axis=1, keepdims=True)

        def pack(rows):
            rows = jnp.dot(pick, rows, preferred_element_type=jnp.float32)
            return (scale * rows).astype(jnp.bfloat16)

        return pack

    pack_own = picker(tok_pos[0:1, :], tok_weight[0:1, :])
    sa[m, me] = pack_own(cot_ref[:, :ca])

    def to_partner(q, src, guard=None):
        send(sa.at[q, src], sa.at[q, src], S_SIDE_A, a_r.at[q, src], dev(dd=side), guard)

    def spread(ej):
        src = slot(d, ej)
        block = sa.at[m, src]
        send(block, block, up_s.at[0], a_r.at[m, src], up, has_up)
        send(block, block, dn_s.at[0], a_r.at[m, src], down, has_down)
        to_partner(m, src)

    def pass_on(k, ej):
        (_, ql, low_here), (_, qh, high_here) = chain(k)
        src = slot(d, ej)
        for q, here, sem, to, more in ((ql, low_here, up_s, up, has_up), (qh, high_here, dn_s, down, has_down)):
            block = sa.at[q, src]
            wait_in(block, a_r.at[q, src], here)
            if k + 1 < nm:
                send(block, block, sem.at[k], a_r.at[q, src], to, here & more)
            to_partner(q, src, here)

    spread(e)
    pack_second = picker(tok_pos[2:3, :], tok_weight[2:3, :])
    sas[...] = pack_second(cot_ref[:, :ca])
    send(sas, sa.at[m, me], S_A, a_r.at[m, me], dev(ee=second))

    slot_flat = lax.broadcasted_iota(jnp.int32, (most, 2 * toks), 0)
    gap = lax.broadcasted_iota(jnp.int32, (toks, 2 * toks), 1) - 2 * lax.broadcasted_iota(
        jnp.int32, (toks, 2 * toks), 0
    )
    flat_pos = -1.0
    for k, hit in enumerate((hit0, hit1)):
        place_k = jnp.where(gap == k, 1.0, 0.0).astype(jnp.bfloat16)
        value = jnp.where(hit, tok_rank + 1.0, 0.0)
        high = jnp.floor(value * (1.0 / 16.0))
        for part, unit in ((high, 16.0), (value - 16.0 * high, 1.0)):
            flat_pos += unit * jnp.dot(part.astype(jnp.bfloat16), place_k, preferred_element_type=jnp.float32)
    flat_pos = flat_pos.astype(jnp.int32)
    loads[-1].wait()
    flat = (2 * toks, half)
    h_rows = [h_in[:, :, c * half : (c + 1) * half].reshape(flat) for c in range(nd)]

    def pack_h(j):
        pick = jnp.where(slot_flat == flat_pos[j : j + 1, :], 1.0, 0.0).astype(jnp.bfloat16)
        for c in range(nd):
            hs[j, c] = jnp.dot(pick, h_rows[c], preferred_element_type=jnp.float32).astype(jnp.bfloat16)

    whole = most // 256 * 256
    main, rest = pl.ds(0, whole), pl.ds(whole, most - whole)
    pack_h(3)
    for c in range(nd):
        send(hs.at[3, c], relay_h.at[c], S_H, rh_r.at[c], dev(ee=first))
    pass_cot(1)
    pack_h(2)
    wait_in(meta_in, rw_r.at[1])
    wait_in(raw_a, rw_r.at[0])
    from_first = slot(d, first)
    pack_relay = picker(meta_in[3:4, :].astype(jnp.int32), meta_in[ne + 3 : ne + 4, :])
    relay_a[...] = pack_relay(raw_a[...])
    send(relay_a, sa.at[m, from_first], S_RELAY_A, a_r.at[m, from_first], dev(ee=second))
    send(hs.at[2, d, main], hr.at[me, main], S_MAIN, h_r.at[H_SECOND], dev(dd=d, ee=second))
    pack_first = picker(meta_in[1:2, :].astype(jnp.int32), meta_in[ne + 1 : ne + 2, :])
    sa[m, from_first] = pack_first(raw_a[...])
    spread(first)
    pass_cot(2)
    wait_in(sa.at[m, slot(d, second)], a_r.at[m, slot(d, second)])
    spread(second)
    pack_h(0)
    send(hs.at[0, side], hr.at[me], S_H, h_r.at[H_OWN], dev(dd=side))
    hr[me] = hs[0, d]
    pack_h(1)

    in_order = (routes_ref[0:1, :] == row_id) | (routes_ref[1:2, :] == row_id)
    counts = jnp.sum(jnp.where(in_order, live, 0.0), axis=1, keepdims=True)
    lanes8 = lax.broadcasted_iota(jnp.int32, (rows8, LANES), 1) == row_id
    lbuf[me] = jnp.broadcast_to(jnp.sum(jnp.where(lanes8, counts, 0.0), axis=0, keepdims=True), (rows8, LANES))

    pass_cot(3)
    send(cotb, raw_b, S_RAW_B, rw_r.at[2], dev(ee=first))
    dense = jnp.concatenate([cotb[q] for q in range(nm)], axis=1)
    sbs[...] = pack_second(dense)
    send(sbs, sb.at[me], S_B, b_r.at[me], dev(ee=second))
    sb[me] = pack_own(dense)
    send(sb.at[me], sb.at[me], S_SIDE_B, b_r.at[me], dev(dd=side))

    def share_b(ej):
        src = slot(d, ej)
        wait_in(sb.at[src], b_r.at[src])
        send(sb.at[src], sb.at[src], S_SIDE_B, b_r.at[src], dev(dd=side))

    for i in range(nd):
        for j in range(ne):
            if i or j:
                to = dev(dd=lax.rem(d + i, nd), ee=lax.rem(e + j, ne))
                send(lbuf.at[me], lbuf.at[me], S_LOAD, l_r.at[0], to)

    for c, role in ((d, H_FIRST), (side, H_FAR_FIRST)):
        send(hs.at[1, c], hr.at[me], S_H, h_r.at[role], dev(dd=c, ee=first))

    def nearest(r):
        near = jnp.minimum(m, nm - 1 - m)
        both = m + (r + 1) // 2 * (1 if r % 2 == 0 else -1)
        far = jnp.where(m < nm - 1 - m, m + r - near, m - r + near)
        return jnp.where(r <= 2 * near, both, far)

    def put(ref, index, value, fresh):
        if fresh:
            ref[index] = value
        else:
            ref[index] = ref[index] + value

    def unit(r, left, cut, fresh=False):
        if r < nm:
            q = nearest(r)
            put(acc_a, q, jnp.dot(left[...], cut(sa.at[q]), preferred_element_type=jnp.float32), fresh)
        else:
            put(acc_b, ..., jnp.dot(left[...], cut(sb), preferred_element_type=jnp.float32), fresh)

    def rows_of(s0, s1, at, rows):
        def cut(ref):
            return jnp.concatenate([ref[s0, at : at + rows], ref[s1, at : at + rows]], axis=0)

        return cut

    def turn(s0, s1, at, rows):
        return jnp.concatenate([hr[s0, at : at + rows], hr[s1, at : at + rows]], axis=0).T

    def partner_a(r, ej):
        q = nearest(r)
        src = slot(side, ej)
        wait_in(sa.at[q, src], a_r.at[q, src])

    def partner_b(ej):
        src = slot(side, ej)
        wait_in(sb.at[src], b_r.at[src])

    def wait_h(src, role):
        wait_in(hr.at[src], h_r.at[role])

    def wait_main(src, role):
        wait_in(hr.at[src, main], h_r.at[role])

    B = nm
    own = rows_of(slot(0, e), slot(1, e), 0, whole)
    diag = rows_of(slot(0, eg), slot(1, eg), 0, whole)
    same = rows_of(slot(d, ex), slot(d, ey), 0, whole)

    pass_on(1, e)
    wait_in(sa.at[m, slot(d, eg)], a_r.at[m, slot(d, eg)])
    spread(eg)
    pass_on(1, first)
    pass_on(1, second)
    wait_h(slot(side, e), H_OWN)
    ht[0] = turn(slot(0, e), slot(1, e), 0, whole)
    partner_a(0, e)
    unit(0, ht.at[0], own, True)
    wait_in(relay_h.at[0], rh_r.at[0])
    send(relay_h.at[0, main], hr.at[from_first, main], S_MAIN, h_r.at[H_DIAG], dev(dd=0, ee=second))
    partner_b(e)
    unit(B, ht.at[0], own, True)
    pass_on(1, eg)
    share_b(second)
    partner_a(1, e)
    unit(1, ht.at[0], own, True)
    pass_on(2, e)
    wait_in(relay_h.at[1], rh_r.at[1])
    send(relay_h.at[1, main], hr.at[from_first, main], S_MAIN, h_r.at[H_DIAG], dev(dd=1, ee=second))
    pass_on(2, first)
    wait_in(raw_b, rw_r.at[2])
    dense = jnp.concatenate([raw_b[q] for q in range(nm)], axis=1)
    relay_b[...] = pack_relay(dense)
    send(relay_b, sb.at[from_first], S_RELAY_B, b_r.at[from_first], dev(ee=second))
    send(hs.at[2, side, main], hr.at[me, main], S_MAIN, h_r.at[H_FAR_SECOND], dev(dd=side, ee=second))
    for c in range(nd):
        send(hs.at[2, c, rest], hr.at[me, rest], S_REST, he_r.at[0], dev(dd=c, ee=second))
    for c in range(nd):
        send(relay_h.at[c, rest], hr.at[from_first, rest], S_REST, he_r.at[0], dev(dd=c, ee=second))
    sb[from_first] = pack_first(dense)
    send(sb.at[from_first], sb.at[from_first], S_SIDE_B, b_r.at[from_first], dev(dd=side))
    pass_on(2, second)
    pass_on(2, eg)
    partner_a(2, e)
    unit(2, ht.at[0], own, True)
    pass_on(3, e)
    partner_a(3, e)
    unit(3, ht.at[0], own, True)
    wait_h(slot(d, first), H_FIRST)
    wait_main(slot(d, second), H_SECOND)
    ht[2] = turn(slot(d, ex), slot(d, ey), 0, whole)
    for r in range(nm - 1):
        unit(r, ht.at[2], same)
    unit(B, ht.at[2], same)
    pairs = hr.at[pl.ds(slot(0, eg), nd), main]
    wait_in(pairs, h_r.at[H_DIAG])
    ht[1] = turn(slot(0, eg), slot(1, eg), 0, whole)
    for r in range(nm - 1):
        partner_a(r, eg)
        unit(r, ht.at[1], diag)
    share_b(eg)
    partner_b(eg)
    unit(B, ht.at[1], diag)
    ends = (slot(side, second), second), (slot(side, first), first)

    def far(n, r):
        src, ej = ends[n]
        if n == 0 and r == B:
            partner_b(ej)
        elif n == 0 or r == nm - 1:
            partner_a(r, ej)
        unit(r, ht_far.at[n], lambda ref: ref[src, :whole])

    wait_h(ends[0][0], H_FAR_FIRST)
    ht_far[0] = hr[ends[0][0], :whole].T
    for r in (0, 1, 2, B):
        far(0, r)
    pass_on(3, first)
    pass_on(3, second)
    unit(nm - 1, ht.at[2], same)
    far(0, nm - 1)
    depth = nd * ne * (most - whole)

    def keep_end(r):
        q = nearest(r)
        end_a[q] = sa[q, :, whole:, :].reshape(depth, ca)

    for r in range(nm - 1):
        partner_a(r, first)
        keep_end(r)
    partner_b(first)
    end_b[...] = sb[:, whole:, :].reshape(depth, nm * cb)

    def last_unit():
        partner_a(nm - 1, eg)
        unit(nm - 1, ht.at[1], diag)

    middle = has_up & has_down
    pl.when(middle)(last_unit)
    wait_main(ends[1][0], H_FAR_SECOND)
    ht_far[1] = hr[ends[1][0], :whole].T
    far(1, 0)
    pass_on(3, eg)
    for r in (1, 2, B, 3):
        far(1, r)
    pl.when(jnp.logical_not(middle))(last_unit)
    keep_end(nm - 1)
    wait_in(hr.at[pl.ds(0, 2 * nd), rest], he_r.at[0])
    ht_end[...] = hr[:, whole:, :].reshape(depth, half).T

    others = nd * ne - 1
    wait_in(lbuf.at[pl.ds(0, others)], l_r.at[0])
    total = lbuf[0]
    for k in range(1, nd * ne):
        total = total + lbuf[k]
    load_ref[...] = total

    for ref, sem in (
        (cot_ref.at[:, pl.ds(0, ca)], S_RAW_A), (meta_out, S_META), (cotb, S_RAW_B), (sas, S_A), (sbs, S_B),
        (relay_a, S_RELAY_A), (relay_b, S_RELAY_B), (sa.at[:, pl.ds(0, ne)], S_SIDE_A), (sb.at[pl.ds(0, ne)], S_SIDE_B),
        (hr.at[pl.ds(0, 2 * nd + 1)], S_H), (hr.at[pl.ds(0, 2 * nd), main], S_MAIN),
        (hr.at[pl.ds(0, 2 * nd), rest], S_REST), (lbuf.at[pl.ds(0, others)], S_LOAD),
    ):
        wait_in(ref, s_s.at[sem])
    blocks_a = sa.at[0, pl.ds(0, ne)]
    for k in range(nm - 1):
        for go, sems, ref in (
            ((m - k >= 0) & has_up, (up_s, cu_s), cotb.at[0]), ((m + k < nm) & has_down, (dn_s, cd_s), cotb.at[0])
        ):
            wait_in(blocks_a, sems[0].at[k], go)
            wait_in(ref, sems[1].at[k], go)


def finish_kernel(
    nm, a_ref, b_ref, ht_ref, end_a, end_b, load_ref, out_ref, total_ref, stage_a, stage_b, sem
):
    ca, cb = a_ref.shape[2], b_ref.shape[1] // nm
    width = ca + cb
    copies = []

    def write(src, rows, at, cols):
        copy = pltpu.make_async_copy(src, out_ref.at[0, rows, pl.ds(at, cols)], sem.at[len(copies)])
        copy.start()
        copies.append(copy)

    def rows_a(q, parts):
        rows = a_ref.shape[1] // parts
        for p in range(parts):
            cut = pl.ds(p * rows, rows)
            stage_a[q, cut] = a_ref[q, cut] + jnp.dot(ht_ref[cut, :], end_a[q], preferred_element_type=jnp.float32)
            write(stage_a.at[q, cut], cut, q * width, ca)

    half = pl.ds(0, b_ref.shape[0])
    rows_a(0, 2)
    stage_b[...] = b_ref[...] + jnp.dot(ht_ref[...], end_b[...], preferred_element_type=jnp.float32)
    for q in range(nm):
        write(stage_b.at[:, pl.ds(q * cb, cb)], half, q * width + ca, cb)
    for q in range(1, nm):
        rows_a(q, 2 if q == nm - 1 else 1)
    total_ref[...] = load_ref[0:1, : total_ref.shape[1]]
    for copy in copies:
        copy.wait()


def fast_body(hidden, cotangent, routes, combine, block_pair, lengths, log_ratio):
    nd, ne, nm = lax.axis_size("dp"), lax.axis_size("expert"), lax.axis_size("mp")
    toks, top, ff = hidden.shape
    width = cotangent.shape[1]
    most = 3 * toks // 4
    cb = width // 4 // LANES * LANES
    ca = width - cb
    half = ff // nd
    srcs = nd * ne
    rows8 = -(-ne // 8) * 8
    whole = most // 256 * 256
    dims = (nd, ne, nm, most, ca, cb)
    bf16, f32 = jnp.bfloat16, jnp.float32
    vmem = pl.BlockSpec(memory_space=pltpu.VMEM)
    hbm = pl.BlockSpec(memory_space=pltpu.HBM)
    dma = pltpu.SemaphoreType.DMA
    depth = srcs * (most - whole)
    results = pl.pallas_call(
        functools.partial(exchange_kernel, dims),
        out_shape=(
            pltpu.VMEM((nm, half, ca), f32),
            pltpu.VMEM((half, nm * cb), f32),
            pltpu.VMEM((half, depth), bf16),
            pltpu.VMEM((nm, depth, ca), bf16),
            pltpu.VMEM((depth, nm * cb), bf16),
            pltpu.VMEM((rows8, LANES), f32),
        ),
        in_specs=[hbm] * 7,
        out_specs=(vmem,) * 6,
        scratch_shapes=[
            pltpu.VMEM((toks, top, ff), bf16),
            pltpu.VMEM(cotangent.shape, bf16),
            pltpu.VMEM((top, toks), jnp.int32),
            pltpu.VMEM((top, toks), f32),
            pltpu.VMEM(block_pair.shape, jnp.int32),
            pltpu.VMEM(lengths.shape, jnp.int32),
            pltpu.VMEM(log_ratio.shape, f32),
            pltpu.VMEM((srcs, most, half), bf16),
            pltpu.VMEM((nm, srcs, most, ca), bf16),
            pltpu.VMEM((srcs, most, nm * cb), bf16),
            pltpu.VMEM((ne, nd, most, half), bf16),
            pltpu.VMEM((most, ca), bf16),
            pltpu.VMEM((most, nm * cb), bf16),
            pltpu.VMEM((nm, toks, cb), bf16),
            pltpu.VMEM((srcs, rows8, LANES), f32),
            pltpu.VMEM((nd, most, half), bf16),
            pltpu.VMEM((most, ca), bf16),
            pltpu.VMEM((most, nm * cb), bf16),
            pltpu.VMEM((toks, ca), bf16),
            pltpu.VMEM((nm, toks, cb), bf16),
            pltpu.VMEM((2 * ne, toks), f32),
            pltpu.VMEM((2 * ne, toks), f32),
            pltpu.VMEM((3, half, 2 * whole), bf16),
            pltpu.VMEM((2, half, whole), bf16),
            dma((7,)),
            dma((13,)),
            dma((nm - 1,)),
            dma((nm - 1,)),
            dma((nm - 1,)),
            dma((nm - 1,)),
            dma((nm, srcs)),
            dma((3,)),
            dma((nm,)),
            dma((srcs,)),
            dma((6,)),
            dma((1,)),
            dma((nd,)),
            dma((1,)),
        ],
        compiler_params=pltpu.CompilerParams(
            collective_id=0, has_side_effects=True, vmem_limit_bytes=VMEM_MOST - 12 * 1024 * 1024
        ),
    )(hidden, cotangent, routes.T, combine.T, block_pair, lengths, log_ratio)
    grad_down, total = pl.pallas_call(
        functools.partial(finish_kernel, nm),
        out_shape=(jax.ShapeDtypeStruct((1, half, nm * width), f32), jax.ShapeDtypeStruct((1, ne), f32)),
        in_specs=[vmem] * 6,
        out_specs=(hbm, vmem),
        scratch_shapes=[pltpu.VMEM((nm, half, ca), f32), pltpu.VMEM((half, nm * cb), f32), dma((2 * nm + 2,))],
        compiler_params=pltpu.CompilerParams(vmem_limit_bytes=VMEM_MOST // 4),
    )(*results)
    return grad_down, total.reshape(ne)


def plain_body(hidden, cotangent, routes, combine, block_pair, lengths, log_ratio):
    per_token, within = token_factors(block_pair, lengths, log_ratio, LEN)
    weight = combine * per_token[:, None]
    tok_rows = routes.shape[0]
    route_top = routes.shape[1]
    ff_local = hidden.shape[2]
    groups = lax.axis_size("expert")
    experts = groups * EXP_DEV
    most_rows = 3 * tok_rows // 4
    labels = jnp.arange(experts, dtype=jnp.int32)
    routed = routes[:, :, None] == labels[None, None, :]
    local_load = jnp.sum(jnp.where(routed & within[:, None, None], 1.0, 0.0), axis=(0, 1)).astype(
        jnp.float32
    )
    flat_rows = tok_rows * route_top
    flat_hits = routed.reshape(flat_rows, experts).astype(jnp.int32)
    rank_of = jnp.sum((jnp.cumsum(flat_hits, axis=0) - 1) * flat_hits, axis=1)
    slot_of = routes.reshape(flat_rows) * most_rows + rank_of
    source = (
        jnp.zeros((experts * most_rows,), jnp.int32)
        .at[slot_of]
        .set(jnp.arange(flat_rows, dtype=jnp.int32))
    )
    filled = jnp.zeros((experts * most_rows,), jnp.float32).at[slot_of].set(1.0)
    token_of = source // route_top
    slot_weight = jnp.take(weight.reshape(flat_rows), source) * filled
    packed_h = jnp.take(hidden.reshape(flat_rows, ff_local), source, axis=0).reshape(
        groups, EXP_DEV * most_rows, ff_local
    )
    narrow_s = (
        slot_weight[:, None] * jnp.take(cotangent, token_of, axis=0).astype(jnp.float32)
    ).astype(jnp.bfloat16)
    moved_h, narrow = (
        lax.all_to_all(packed_h, "expert", split_axis=0, concat_axis=0, tiled=True),
        lax.all_to_all(
            narrow_s.reshape(groups, EXP_DEV * most_rows, cotangent.shape[1]),
            "expert",
            split_axis=0,
            concat_axis=0,
            tiled=True,
        ),
    )
    moved_s = lax.all_gather(narrow, "mp", axis=2, tiled=True)
    moved_h = moved_h.reshape(groups, EXP_DEV, most_rows, ff_local)
    moved_s = moved_s.reshape(groups, EXP_DEV, most_rows, moved_s.shape[2])
    products = [
        lax.dot_general(
            moved_h[:, 0],
            moved_s[:, 0],
            (((0, 1), (0, 1)), ((), ())),
            preferred_element_type=jnp.float32,
        )
    ]
    owned = lax.psum_scatter(jnp.stack(products, axis=1), "dp", scatter_dimension=0, tiled=True)
    grad_down = jnp.transpose(owned, (1, 0, 2))
    expert_load = lax.psum(local_load, ("dp", "expert"))
    return (grad_down, expert_load)


def solution(mesh):
    in_specs = (
        P(("dp", "expert"), None, "mp"),
        P(("dp", "expert"), "mp"),
        P(("dp", "expert"), None),
        P(("dp", "expert"), None),
        P(("dp", "expert"), None),
        P(("dp", "expert"), None),
        P(("dp", "expert"), None),
    )
    out_specs = (P("expert", ("mp", "dp"), None), P())

    def body(hidden, cotangent, *rest):
        rows = mesh.shape["dp"] * mesh.shape["expert"] * (3 * hidden.shape[0] // 4)
        bytes_in = 2 * rows * (cotangent.shape[1] * mesh.shape["mp"] + hidden.shape[2])
        most = 3 * hidden.shape[0] // 4
        whole = most // 256 * 256
        square = mesh.shape["dp"] == 2 and mesh.shape["expert"] == 4 and mesh.shape["mp"] == 4
        fits = square and whole and 8 * (most - whole) == whole
        run = fast_body if fits and 2 * bytes_in < VMEM_ROOM else plain_body
        return run(hidden, cotangent, *rest)

    return jax.shard_map(body, mesh=mesh, in_specs=in_specs, out_specs=out_specs, check_vma=False)
```

```python
import functools

import jax
import jax.numpy as jnp
from jax import lax
from jax.experimental import pallas as pl
from jax.experimental.pallas import tpu as pltpu
from jax.sharding import PartitionSpec as P

EXP_DEV = 1
LEN = 32
LANES = 128
VMEM_ROOM = 48 * 1024 * 1024
VMEM_MOST = 67043328
MESH = pl.DeviceIdType.MESH


beta_scale = 0.1


def token_factors(block_pair, lengths, log_ratio, block_len):
    blocks = block_pair.shape[1]
    labels = jnp.arange(blocks, dtype=jnp.int32)
    matches = block_pair[:, :, None] == labels[None, None, :]
    by_label = jnp.sum(jnp.where(matches, log_ratio[:, :, None], 0.0), axis=1)
    margin = by_label[:, 0::2] - by_label[:, 1::2]
    pair_coef = beta_scale * jax.nn.sigmoid(-beta_scale * margin)
    owners = block_pair // 2
    pair_ids = jnp.arange(blocks // 2, dtype=jnp.int32)
    picked = owners[:, :, None] == pair_ids[None, None, :]
    block_coef = jnp.sum(jnp.where(picked, pair_coef[:, None, :], 0.0), axis=2)
    block_weight = jnp.where(block_pair % 2 == 0, -block_coef, block_coef)
    position = jnp.arange(block_len, dtype=jnp.int32)
    within = position[None, None, :] < lengths[:, :, None]
    per_token = jnp.where(within, block_weight[:, :, None], 0.0).reshape(-1)
    return per_token, within.reshape(-1)


def exchange_kernel(
    dims, h_hbm, cot_hbm, routes_hbm, combine_hbm, pair_hbm, len_hbm, ratio_hbm,
    acc_a, acc_b, ht_end, end_a, end_b, load_ref,
    h_in, cot_ref, routes_ref, combine_ref, pair_ref, len_ref, ratio_ref,
    hr, sa, sb, hs, sas, sbs, cotb, load_out, load_in, relay_h, relay_a, relay_b, raw_a, raw_b, meta_out, meta_in, ht, ht_far,
    in_sem, s_s, up_s, dn_s, cu_s, cd_s, a_r, rw_r, cb_r, b_r, h_r, he_r, rh_r, l_r,
):
    nd, ne, nm, most, ca, cb = dims
    d, e, m = lax.axis_index("dp"), lax.axis_index("expert"), lax.axis_index("mp")
    toks, top, ff = h_in.shape
    half = ff // nd
    side = 1 - d
    ex, ey, eg = e + 1 - 2 * lax.rem(e, 2), lax.rem(e + 2, ne), ne - 1 - e
    first, second = ex + d * (ey - ex), ey + d * (ex - ey)
    dests = (e, first, second, eg)

    def slot(dd, ee):
        return ee * nd + dd

    me = slot(d, e)

    def dev(dd=None, ee=None, mm=None):
        return {"dp": d if dd is None else dd, "expert": e if ee is None else ee, "mp": m if mm is None else mm}

    S_RAW_A, S_META, S_RAW_B, S_A, S_B, S_H, S_Q, S_LOAD = range(8)
    H_OWN, H_FIRST, H_SECOND, H_FAR_FIRST, H_FAR_SECOND, H_DIAG = range(6)

    def remote(src, dst, ssem, rsem, where):
        return pltpu.make_async_remote_copy(
            src_ref=src, dst_ref=dst, send_sem=ssem, recv_sem=rsem, device_id=where, device_id_type=MESH
        )

    def send(src, dst, ssem, rsem, where, go=None):
        copy = remote(src, dst, s_s.at[ssem] if isinstance(ssem, int) else ssem, rsem, where)
        if go is None:
            copy.start()
        else:
            pl.when(go)(copy.start)

    def wait_in(buf, sem, guard=None):
        c = pltpu.make_async_copy(buf, buf, sem)
        if guard is None:
            c.wait()
        else:
            pl.when(guard)(c.wait)

    loads = [
        pltpu.make_async_copy(src, dst, in_sem.at[i])
        for i, (src, dst) in enumerate((
            (routes_hbm, routes_ref), (cot_hbm, cot_ref), (pair_hbm, pair_ref), (len_hbm, len_ref),
            (ratio_hbm, ratio_ref), (combine_hbm, combine_ref), (h_hbm, h_in),
        ))
    ]
    for load in loads:
        load.start()
    barrier = pltpu.get_barrier_semaphore()
    peers = [dev(dd=side)] + [dev(dd=i, ee=to) for i in range(nd) for to in (first, second)]
    for peer in peers:
        pl.semaphore_signal(barrier, inc=1, device_id=peer, device_id_type=MESH)
    has_up, has_down = m + 1 < nm, m > 0
    up, down = dev(mm=lax.rem(m + 1, nm)), dev(mm=lax.rem(m + nm - 1, nm))
    for go, peer in ((has_up, up), (has_down, down)):
        pl.when(go)(
            functools.partial(pl.semaphore_signal, barrier, inc=1, device_id=peer, device_id_type=MESH)
        )
    n_peers = len(peers) + jnp.where(has_up, 1, 0) + jnp.where(has_down, 1, 0)

    loads[0].wait()
    rows8 = -(-ne // 8) * 8
    row_id = lax.broadcasted_iota(jnp.int32, (rows8, 1), 0)
    owner = jnp.full((rows8, 1), -1, jnp.int32)
    for j, to in enumerate(dests):
        owner = jnp.where(row_id == j, to, owner)
    hit0 = routes_ref[0:1, :] == owner
    hit1 = routes_ref[1:2, :] == owner
    named = hit0 | hit1
    before = lax.broadcasted_iota(jnp.int32, (toks, toks), 0) < lax.broadcasted_iota(jnp.int32, (toks, toks), 1)
    tok_rank = jnp.dot(
        jnp.where(named, 1.0, 0.0).astype(jnp.bfloat16),
        jnp.where(before, 1.0, 0.0).astype(jnp.bfloat16),
        preferred_element_type=jnp.float32,
    )
    tok_rank = jnp.where(named, tok_rank, -1.0)
    tok_pos = tok_rank.astype(jnp.int32)

    for load in loads[2:-1]:
        load.wait()

    blocks = pair_ref.shape[1]
    block_len = toks // blocks
    square = (blocks, blocks)
    diagonal = lax.broadcasted_iota(jnp.int32, square, 0) == lax.broadcasted_iota(jnp.int32, square, 1)

    def column(row):
        return jnp.sum(jnp.where(diagonal, row, 0.0), axis=1, keepdims=True)

    pair, ratio = pair_ref[...], ratio_ref[...]
    chosen = lax.rem(pair, 2) == 0
    other_side = jnp.where(chosen, pair + 1, pair - 1)
    is_other = column(pair.astype(jnp.float32)) == other_side.astype(jnp.float32)
    other_ratio = jnp.sum(jnp.where(is_other, column(ratio), 0.0), axis=0, keepdims=True)
    margin = jnp.where(chosen, ratio - other_ratio, other_ratio - ratio)
    coef = beta_scale * (1.0 / (1.0 + jnp.exp(beta_scale * margin)))
    block_weight = column(jnp.where(chosen, -coef, coef))
    token_id = lax.broadcasted_iota(jnp.int32, (blocks, toks), 1)
    place = token_id - block_len * lax.broadcasted_iota(jnp.int32, (blocks, toks), 0)
    inside = (place >= 0) & (place < block_len)
    alive = inside & (place.astype(jnp.float32) < column(len_ref[...].astype(jnp.float32)))
    live = jnp.sum(jnp.where(alive, 1.0, 0.0), axis=0, keepdims=True)
    per_token = jnp.sum(jnp.where(alive, block_weight, 0.0), axis=0, keepdims=True)
    weight = combine_ref[...] * per_token
    tok_weight = jnp.where(hit0, weight[0:1, :], 0.0) + jnp.where(hit1, weight[1:2, :], 0.0)

    loads[1].wait()
    cotb[m] = cot_ref[:, ca:]
    meta_out[...] = jnp.concatenate([tok_rank[:ne], tok_weight[:ne]], axis=0)
    slot_tok = lax.broadcasted_iota(jnp.int32, (most, toks), 0)
    pl.semaphore_wait(barrier, n_peers)
    send(cot_ref.at[:, pl.ds(0, ca)], raw_a, S_RAW_A, rw_r.at[0], dev(ee=first))
    own_cols = cot_ref.at[:, pl.ds(ca, cb)]
    send(own_cols, cotb.at[m], cu_s.at[0], cb_r.at[m], up, has_up)
    send(own_cols, cotb.at[m], cd_s.at[0], cb_r.at[m], down, has_down)
    send(meta_out, meta_in, S_META, rw_r.at[1], dev(ee=first))

    def chain(k):
        return (m - k, lax.rem(m - k + nm, nm), m - k >= 0), (m + k, lax.rem(m + k, nm), m + k < nm)

    def pass_cot(k):
        (_, ql, low_here), (_, qh, high_here) = chain(k)
        for q, here, sem, to, more in ((ql, low_here, cu_s, up, has_up), (qh, high_here, cd_s, down, has_down)):
            wait_in(cotb.at[q], cb_r.at[q], here)
            if k + 1 < nm:
                send(cotb.at[q], cotb.at[q], sem.at[0], cb_r.at[q], to, here & more)

    def picker(position, factor):
        hit = slot_tok == position
        pick = jnp.where(hit, 1.0, 0.0).astype(jnp.bfloat16)
        scale = jnp.sum(jnp.where(hit, factor, 0.0), axis=1, keepdims=True)

        def pack(rows):
            rows = jnp.dot(pick, rows, preferred_element_type=jnp.float32)
            return (scale * rows).astype(jnp.bfloat16)

        return pack

    pack_own = picker(tok_pos[0:1, :], tok_weight[0:1, :])
    sa[m, me] = pack_own(cot_ref[:, :ca])

    def to_partner(q, src, guard=None):
        send(sa.at[q, src], sa.at[q, src], S_A, a_r.at[q, src], dev(dd=side), guard)

    def spread(ej):
        src = slot(d, ej)
        block = sa.at[m, src]
        send(block, block, up_s.at[0], a_r.at[m, src], up, has_up)
        send(block, block, dn_s.at[0], a_r.at[m, src], down, has_down)
        to_partner(m, src)

    def pass_on(k, ej):
        (_, ql, low_here), (_, qh, high_here) = chain(k)
        src = slot(d, ej)
        for q, here, sem, to, more in ((ql, low_here, up_s, up, has_up), (qh, high_here, dn_s, down, has_down)):
            block = sa.at[q, src]
            wait_in(block, a_r.at[q, src], here)
            if k + 1 < nm:
                send(block, block, sem.at[0], a_r.at[q, src], to, here & more)
            to_partner(q, src, here)

    spread(e)
    pack_second = picker(tok_pos[2:3, :], tok_weight[2:3, :])
    sas[...] = pack_second(cot_ref[:, :ca])
    send(sas, sa.at[m, me], S_A, a_r.at[m, me], dev(ee=second))

    slot_flat = lax.broadcasted_iota(jnp.int32, (most, 2 * toks), 0)
    gap = lax.broadcasted_iota(jnp.int32, (toks, 2 * toks), 1) - 2 * lax.broadcasted_iota(
        jnp.int32, (toks, 2 * toks), 0
    )
    flat_pos = -1.0
    for k, hit in enumerate((hit0, hit1)):
        place_k = jnp.where(gap == k, 1.0, 0.0).astype(jnp.bfloat16)
        value = jnp.where(hit, tok_rank + 1.0, 0.0)
        high = jnp.floor(value * (1.0 / 16.0))
        for part, unit in ((high, 16.0), (value - 16.0 * high, 1.0)):
            flat_pos += unit * jnp.dot(part.astype(jnp.bfloat16), place_k, preferred_element_type=jnp.float32)
    flat_pos = flat_pos.astype(jnp.int32)
    loads[-1].wait()
    flat = (2 * toks, half)
    h_rows = [h_in[:, :, c * half : (c + 1) * half].reshape(flat) for c in range(nd)]

    def pack_h(j):
        pick = jnp.where(slot_flat == flat_pos[j : j + 1, :], 1.0, 0.0).astype(jnp.bfloat16)
        for c in range(nd):
            hs[j, c] = jnp.dot(pick, h_rows[c], preferred_element_type=jnp.float32).astype(jnp.bfloat16)

    whole = most // 256 * 256
    main, rest = pl.ds(0, whole), pl.ds(whole, most - whole)
    pack_h(3)
    for c in range(nd):
        send(hs.at[3, c], relay_h.at[c], S_H, rh_r.at[c], dev(ee=first))
    pass_cot(1)
    pack_h(2)
    wait_in(sa.at[m, slot(d, second)], a_r.at[m, slot(d, second)])
    spread(second)
    wait_in(meta_in, rw_r.at[1])
    wait_in(raw_a, rw_r.at[0])
    from_first = slot(d, first)
    pack_relay = picker(meta_in[3:4, :].astype(jnp.int32), meta_in[ne + 3 : ne + 4, :])
    relay_a[...] = pack_relay(raw_a[...])
    send(relay_a, sa.at[m, from_first], S_A, a_r.at[m, from_first], dev(ee=second))
    send(hs.at[2, d, main], hr.at[me, main], S_Q, h_r.at[H_SECOND], dev(dd=d, ee=second))
    pack_first = picker(meta_in[1:2, :].astype(jnp.int32), meta_in[ne + 1 : ne + 2, :])
    sa[m, from_first] = pack_first(raw_a[...])
    spread(first)
    pack_h(0)
    send(hs.at[0, side], hr.at[me], S_H, h_r.at[H_OWN], dev(dd=side))
    hr[me] = hs[0, d]
    pack_h(1)

    in_order = (routes_ref[0:1, :] == row_id) | (routes_ref[1:2, :] == row_id)
    counts = jnp.sum(jnp.where(in_order, live, 0.0), axis=1, keepdims=True)
    lanes8 = lax.broadcasted_iota(jnp.int32, (rows8, LANES), 1) == row_id
    load_out[0] = jnp.broadcast_to(jnp.sum(jnp.where(lanes8, counts, 0.0), axis=0, keepdims=True), (rows8, LANES))
    partners = (dev(dd=side), dev(ee=first), dev(ee=second))

    def add_load(n):
        wait_in(load_in.at[n], l_r.at[n])
        total = load_out[n] + load_in[n]
        if n + 1 < len(partners):
            load_out[n + 1] = total
            send(load_out.at[n + 1], load_in.at[n + 1], S_LOAD + n + 1, l_r.at[n + 1], partners[n + 1])
        else:
            load_ref[...] = total

    send(load_out.at[0], load_in.at[0], S_LOAD, l_r.at[0], partners[0])
    pass_cot(2)
    pass_cot(3)
    send(cotb, raw_b, S_RAW_B, rw_r.at[2], dev(ee=first))
    dense = jnp.concatenate([cotb[q] for q in range(nm)], axis=1)
    sbs[...] = pack_second(dense)
    send(sbs, sb.at[me], S_B, b_r.at[me], dev(ee=second))
    sb[me] = pack_own(dense)
    send(sb.at[me], sb.at[me], S_B, b_r.at[me], dev(dd=side))

    def share_b(ej):
        src = slot(d, ej)
        wait_in(sb.at[src], b_r.at[src])
        send(sb.at[src], sb.at[src], S_B, b_r.at[src], dev(dd=side))

    for c, role in ((d, H_FIRST), (side, H_FAR_FIRST)):
        send(hs.at[1, c], hr.at[me], S_H, h_r.at[role], dev(dd=c, ee=first))

    def nearest(r):
        near = jnp.minimum(m, nm - 1 - m)
        both = m + (r + 1) // 2 * (1 if r % 2 == 0 else -1)
        far = jnp.where(m < nm - 1 - m, m + r - near, m - r + near)
        return jnp.where(r <= 2 * near, both, far)

    def put(ref, index, value, fresh):
        if fresh:
            ref[index] = value
        else:
            ref[index] = ref[index] + value

    def unit(r, left, cut, fresh=False):
        if r < nm:
            q = nearest(r)
            put(acc_a, q, jnp.dot(left[...], cut(sa.at[q]), preferred_element_type=jnp.float32), fresh)
        else:
            put(acc_b, ..., jnp.dot(left[...], cut(sb), preferred_element_type=jnp.float32), fresh)

    def rows_of(s0, s1, at, rows):
        def cut(ref):
            return jnp.concatenate([ref[s0, at : at + rows], ref[s1, at : at + rows]], axis=0)

        return cut

    def turn(s0, s1, at, rows):
        return jnp.concatenate([hr[s0, at : at + rows], hr[s1, at : at + rows]], axis=0).T

    def partner_a(r, ej):
        q = nearest(r)
        src = slot(side, ej)
        wait_in(sa.at[q, src], a_r.at[q, src])

    def partner_b(ej):
        src = slot(side, ej)
        wait_in(sb.at[src], b_r.at[src])

    def wait_h(src, role):
        wait_in(hr.at[src], h_r.at[role])

    def wait_main(src, role):
        wait_in(hr.at[src, main], h_r.at[role])

    B = nm
    own = rows_of(slot(0, e), slot(1, e), 0, whole)
    diag = rows_of(slot(0, eg), slot(1, eg), 0, whole)
    same = rows_of(slot(d, ex), slot(d, ey), 0, whole)

    pass_on(1, e)
    wait_in(sa.at[m, slot(d, eg)], a_r.at[m, slot(d, eg)])
    spread(eg)
    pass_on(1, first)
    pass_on(1, second)
    wait_h(slot(side, e), H_OWN)
    ht[0] = turn(slot(0, e), slot(1, e), 0, whole)
    partner_a(0, e)
    unit(0, ht.at[0], own, True)
    wait_in(relay_h.at[0], rh_r.at[0])
    send(relay_h.at[0, main], hr.at[from_first, main], S_Q, h_r.at[H_DIAG], dev(dd=0, ee=second))
    partner_b(e)
    unit(B, ht.at[0], own, True)
    pass_on(1, eg)
    share_b(second)
    partner_a(1, e)
    unit(1, ht.at[0], own, True)
    add_load(0)
    pass_on(2, e)
    wait_in(relay_h.at[1], rh_r.at[1])
    send(relay_h.at[1, main], hr.at[from_first, main], S_Q, h_r.at[H_DIAG], dev(dd=1, ee=second))
    pass_on(2, first)
    wait_in(raw_b, rw_r.at[2])
    dense = jnp.concatenate([raw_b[q] for q in range(nm)], axis=1)
    relay_b[...] = pack_relay(dense)
    send(relay_b, sb.at[from_first], S_B, b_r.at[from_first], dev(ee=second))
    send(hs.at[2, side, main], hr.at[me, main], S_Q, h_r.at[H_FAR_SECOND], dev(dd=side, ee=second))
    for c in range(nd):
        send(hs.at[2, c, rest], hr.at[me, rest], S_Q, he_r.at[0], dev(dd=c, ee=second))
    for c in range(nd):
        send(relay_h.at[c, rest], hr.at[from_first, rest], S_Q, he_r.at[0], dev(dd=c, ee=second))
    sb[from_first] = pack_first(dense)
    send(sb.at[from_first], sb.at[from_first], S_B, b_r.at[from_first], dev(dd=side))
    pass_on(2, second)
    pass_on(2, eg)
    partner_a(2, e)
    unit(2, ht.at[0], own, True)
    add_load(1)
    pass_on(3, e)
    partner_a(3, e)
    unit(3, ht.at[0], own, True)
    add_load(2)
    wait_h(slot(d, first), H_FIRST)
    wait_main(slot(d, second), H_SECOND)
    ht[2] = turn(slot(d, ex), slot(d, ey), 0, whole)
    for r in range(nm - 1):
        unit(r, ht.at[2], same)
    unit(B, ht.at[2], same)
    pairs = hr.at[pl.ds(slot(0, eg), nd), main]
    wait_in(pairs, h_r.at[H_DIAG])
    ht[1] = turn(slot(0, eg), slot(1, eg), 0, whole)
    for r in range(nm - 1):
        partner_a(r, eg)
        unit(r, ht.at[1], diag)
    share_b(eg)
    partner_b(eg)
    unit(B, ht.at[1], diag)
    ends = (slot(side, second), second), (slot(side, first), first)

    def far(n, r):
        src, ej = ends[n]
        if n == 0 and r == B:
            partner_b(ej)
        elif n == 0 or r == nm - 1:
            partner_a(r, ej)
        unit(r, ht_far.at[n], lambda ref: ref[src, :whole])

    wait_h(ends[0][0], H_FAR_FIRST)
    ht_far[0] = hr[ends[0][0], :whole].T
    for r in (0, 1, 2, B):
        far(0, r)
    pass_on(3, first)
    pass_on(3, second)
    unit(nm - 1, ht.at[2], same)
    far(0, nm - 1)
    depth = nd * ne * (most - whole)

    def keep_end(r):
        q = nearest(r)
        end_a[q] = sa[q, :, whole:, :].reshape(depth, ca)

    for r in range(nm - 1):
        partner_a(r, first)
        keep_end(r)
    partner_b(first)
    end_b[...] = sb[:, whole:, :].reshape(depth, nm * cb)

    def last_unit():
        partner_a(nm - 1, eg)
        unit(nm - 1, ht.at[1], diag)

    middle = has_up & has_down
    pl.when(middle)(last_unit)
    wait_main(ends[1][0], H_FAR_SECOND)
    ht_far[1] = hr[ends[1][0], :whole].T
    far(1, 0)
    far(1, 1)
    pass_on(3, eg)
    for r in (2, B, 3):
        far(1, r)
    pl.when(jnp.logical_not(middle))(last_unit)
    keep_end(nm - 1)
    wait_in(hr.at[pl.ds(0, 2 * nd), rest], he_r.at[0])
    ht_end[...] = hr[:, whole:, :].reshape(depth, half).T

    for ref, sem in (
        (cot_ref.at[:, pl.ds(0, ca)], S_RAW_A), (meta_out, S_META), (cotb, S_RAW_B),
        (sa.at[pl.ds(0, nm - 1), pl.ds(0, ne + 2)], S_A), (sb.at[pl.ds(0, ne + 2)], S_B),
        (hr.at[pl.ds(0, 2 * nd + 1)], S_H), (hr.at[pl.ds(0, 2 * nd)], S_Q),
        (load_out.at[0], S_LOAD), (load_out.at[1], S_LOAD + 1), (load_out.at[2], S_LOAD + 2),
    ):
        wait_in(ref, s_s.at[sem])
    for k in range(nm - 1):
        hops = pl.ds(0, k + 1)
        for at, end, blocks, cols in ((m, nm - 1, up_s, cu_s), (nm - 1 - m, nm - 1, dn_s, cd_s)):
            wait_in(sa.at[hops, pl.ds(0, ne)], blocks.at[0], at == k)
            wait_in(cotb.at[hops], cols.at[0], at == k)


def finish_kernel(
    nm, a_ref, b_ref, ht_ref, end_a, end_b, load_ref, out_ref, total_ref, stage_a, stage_b, sem
):
    ca, cb = a_ref.shape[2], b_ref.shape[1] // nm
    width = ca + cb
    copies = []

    def write(src, rows, at, cols):
        copy = pltpu.make_async_copy(src, out_ref.at[0, rows, pl.ds(at, cols)], sem.at[len(copies)])
        copy.start()
        copies.append(copy)

    def rows_a(q, parts):
        rows = a_ref.shape[1] // parts
        for p in range(parts):
            cut = pl.ds(p * rows, rows)
            stage_a[q, cut] = a_ref[q, cut] + jnp.dot(ht_ref[cut, :], end_a[q], preferred_element_type=jnp.float32)
            write(stage_a.at[q, cut], cut, q * width, ca)

    half = pl.ds(0, b_ref.shape[0])
    rows_a(0, 2)
    stage_b[...] = b_ref[...] + jnp.dot(ht_ref[...], end_b[...], preferred_element_type=jnp.float32)
    for q in range(nm):
        write(stage_b.at[:, pl.ds(q * cb, cb)], half, q * width + ca, cb)
    for q in range(1, nm):
        rows_a(q, 2 if q == nm - 1 else 1)
    total_ref[...] = load_ref[0:1, : total_ref.shape[1]]
    for copy in copies:
        copy.wait()


def fast_body(hidden, cotangent, routes, combine, block_pair, lengths, log_ratio):
    nd, ne, nm = lax.axis_size("dp"), lax.axis_size("expert"), lax.axis_size("mp")
    toks, top, ff = hidden.shape
    width = cotangent.shape[1]
    most = 3 * toks // 4
    cb = width // 4 // LANES * LANES
    ca = width - cb
    half = ff // nd
    srcs = nd * ne
    rows8 = -(-ne // 8) * 8
    whole = most // 256 * 256
    dims = (nd, ne, nm, most, ca, cb)
    bf16, f32 = jnp.bfloat16, jnp.float32
    vmem = pl.BlockSpec(memory_space=pltpu.VMEM)
    hbm = pl.BlockSpec(memory_space=pltpu.HBM)
    dma = pltpu.SemaphoreType.DMA
    depth = srcs * (most - whole)
    results = pl.pallas_call(
        functools.partial(exchange_kernel, dims),
        out_shape=(
            pltpu.VMEM((nm, half, ca), f32),
            pltpu.VMEM((half, nm * cb), f32),
            pltpu.VMEM((half, depth), bf16),
            pltpu.VMEM((nm, depth, ca), bf16),
            pltpu.VMEM((depth, nm * cb), bf16),
            pltpu.VMEM((rows8, LANES), f32),
        ),
        in_specs=[hbm] * 7,
        out_specs=(vmem,) * 6,
        scratch_shapes=[
            pltpu.VMEM((toks, top, ff), bf16),
            pltpu.VMEM(cotangent.shape, bf16),
            pltpu.VMEM((top, toks), jnp.int32),
            pltpu.VMEM((top, toks), f32),
            pltpu.VMEM(block_pair.shape, jnp.int32),
            pltpu.VMEM(lengths.shape, jnp.int32),
            pltpu.VMEM(log_ratio.shape, f32),
            pltpu.VMEM((srcs, most, half), bf16),
            pltpu.VMEM((nm, srcs, most, ca), bf16),
            pltpu.VMEM((srcs, most, nm * cb), bf16),
            pltpu.VMEM((ne, nd, most, half), bf16),
            pltpu.VMEM((most, ca), bf16),
            pltpu.VMEM((most, nm * cb), bf16),
            pltpu.VMEM((nm, toks, cb), bf16),
            pltpu.VMEM((3, rows8, LANES), f32),
            pltpu.VMEM((3, rows8, LANES), f32),
            pltpu.VMEM((nd, most, half), bf16),
            pltpu.VMEM((most, ca), bf16),
            pltpu.VMEM((most, nm * cb), bf16),
            pltpu.VMEM((toks, ca), bf16),
            pltpu.VMEM((nm, toks, cb), bf16),
            pltpu.VMEM((2 * ne, toks), f32),
            pltpu.VMEM((2 * ne, toks), f32),
            pltpu.VMEM((3, half, 2 * whole), bf16),
            pltpu.VMEM((2, half, whole), bf16),
            dma((7,)),
            dma((10,)),
            dma((1,)),
            dma((1,)),
            dma((1,)),
            dma((1,)),
            dma((nm, srcs)),
            dma((3,)),
            dma((nm,)),
            dma((srcs,)),
            dma((6,)),
            dma((1,)),
            dma((nd,)),
            dma((3,)),
        ],
        compiler_params=pltpu.CompilerParams(
            collective_id=0, has_side_effects=True, vmem_limit_bytes=VMEM_MOST - 12 * 1024 * 1024
        ),
    )(hidden, cotangent, routes.T, combine.T, block_pair, lengths, log_ratio)
    grad_down, total = pl.pallas_call(
        functools.partial(finish_kernel, nm),
        out_shape=(jax.ShapeDtypeStruct((1, half, nm * width), f32), jax.ShapeDtypeStruct((1, ne), f32)),
        in_specs=[vmem] * 6,
        out_specs=(hbm, vmem),
        scratch_shapes=[pltpu.VMEM((nm, half, ca), f32), pltpu.VMEM((half, nm * cb), f32), dma((2 * nm + 2,))],
        compiler_params=pltpu.CompilerParams(vmem_limit_bytes=VMEM_MOST // 4),
    )(*results)
    return grad_down, total.reshape(ne)


def plain_body(hidden, cotangent, routes, combine, block_pair, lengths, log_ratio):
    per_token, within = token_factors(block_pair, lengths, log_ratio, LEN)
    weight = combine * per_token[:, None]
    tok_rows = routes.shape[0]
    route_top = routes.shape[1]
    ff_local = hidden.shape[2]
    groups = lax.axis_size("expert")
    experts = groups * EXP_DEV
    most_rows = 3 * tok_rows // 4
    labels = jnp.arange(experts, dtype=jnp.int32)
    routed = routes[:, :, None] == labels[None, None, :]
    local_load = jnp.sum(jnp.where(routed & within[:, None, None], 1.0, 0.0), axis=(0, 1)).astype(
        jnp.float32
    )
    flat_rows = tok_rows * route_top
    flat_hits = routed.reshape(flat_rows, experts).astype(jnp.int32)
    rank_of = jnp.sum((jnp.cumsum(flat_hits, axis=0) - 1) * flat_hits, axis=1)
    slot_of = routes.reshape(flat_rows) * most_rows + rank_of
    source = (
        jnp.zeros((experts * most_rows,), jnp.int32)
        .at[slot_of]
        .set(jnp.arange(flat_rows, dtype=jnp.int32))
    )
    filled = jnp.zeros((experts * most_rows,), jnp.float32).at[slot_of].set(1.0)
    token_of = source // route_top
    slot_weight = jnp.take(weight.reshape(flat_rows), source) * filled
    packed_h = jnp.take(hidden.reshape(flat_rows, ff_local), source, axis=0).reshape(
        groups, EXP_DEV * most_rows, ff_local
    )
    narrow_s = (
        slot_weight[:, None] * jnp.take(cotangent, token_of, axis=0).astype(jnp.float32)
    ).astype(jnp.bfloat16)
    moved_h, narrow = (
        lax.all_to_all(packed_h, "expert", split_axis=0, concat_axis=0, tiled=True),
        lax.all_to_all(
            narrow_s.reshape(groups, EXP_DEV * most_rows, cotangent.shape[1]),
            "expert",
            split_axis=0,
            concat_axis=0,
            tiled=True,
        ),
    )
    moved_s = lax.all_gather(narrow, "mp", axis=2, tiled=True)
    moved_h = moved_h.reshape(groups, EXP_DEV, most_rows, ff_local)
    moved_s = moved_s.reshape(groups, EXP_DEV, most_rows, moved_s.shape[2])
    products = [
        lax.dot_general(
            moved_h[:, 0],
            moved_s[:, 0],
            (((0, 1), (0, 1)), ((), ())),
            preferred_element_type=jnp.float32,
        )
    ]
    owned = lax.psum_scatter(jnp.stack(products, axis=1), "dp", scatter_dimension=0, tiled=True)
    grad_down = jnp.transpose(owned, (1, 0, 2))
    expert_load = lax.psum(local_load, ("dp", "expert"))
    return (grad_down, expert_load)


def solution(mesh):
    in_specs = (
        P(("dp", "expert"), None, "mp"),
        P(("dp", "expert"), "mp"),
        P(("dp", "expert"), None),
        P(("dp", "expert"), None),
        P(("dp", "expert"), None),
        P(("dp", "expert"), None),
        P(("dp", "expert"), None),
    )
    out_specs = (P("expert", ("mp", "dp"), None), P())

    def body(hidden, cotangent, *rest):
        rows = mesh.shape["dp"] * mesh.shape["expert"] * (3 * hidden.shape[0] // 4)
        bytes_in = 2 * rows * (cotangent.shape[1] * mesh.shape["mp"] + hidden.shape[2])
        most = 3 * hidden.shape[0] // 4
        whole = most // 256 * 256
        square = mesh.shape["dp"] == 2 and mesh.shape["expert"] == 4 and mesh.shape["mp"] == 4
        fits = square and whole and 8 * (most - whole) == whole
        run = fast_body if fits and 2 * bytes_in < VMEM_ROOM else plain_body
        return run(hidden, cotangent, *rest)

    return jax.shard_map(body, mesh=mesh, in_specs=in_specs, out_specs=out_specs, check_vma=False)
```

```python
import functools

import jax
import jax.numpy as jnp
from jax import lax
from jax.experimental import pallas as pl
from jax.experimental.pallas import tpu as pltpu
from jax.sharding import PartitionSpec as P

EXP_DEV = 1
LEN = 32
LANES = 128
VMEM_ROOM = 48 * 1024 * 1024
VMEM_MOST = 67043328
MESH = pl.DeviceIdType.MESH


beta_scale = 0.1


def token_factors(block_pair, lengths, log_ratio, block_len):
    blocks = block_pair.shape[1]
    labels = jnp.arange(blocks, dtype=jnp.int32)
    matches = block_pair[:, :, None] == labels[None, None, :]
    by_label = jnp.sum(jnp.where(matches, log_ratio[:, :, None], 0.0), axis=1)
    margin = by_label[:, 0::2] - by_label[:, 1::2]
    pair_coef = beta_scale * jax.nn.sigmoid(-beta_scale * margin)
    owners = block_pair // 2
    pair_ids = jnp.arange(blocks // 2, dtype=jnp.int32)
    picked = owners[:, :, None] == pair_ids[None, None, :]
    block_coef = jnp.sum(jnp.where(picked, pair_coef[:, None, :], 0.0), axis=2)
    block_weight = jnp.where(block_pair % 2 == 0, -block_coef, block_coef)
    position = jnp.arange(block_len, dtype=jnp.int32)
    within = position[None, None, :] < lengths[:, :, None]
    per_token = jnp.where(within, block_weight[:, :, None], 0.0).reshape(-1)
    return per_token, within.reshape(-1)


def exchange_kernel(
    dims, h_hbm, cot_hbm, routes_hbm, combine_hbm, pair_hbm, len_hbm, ratio_hbm,
    acc_a, acc_b, ht_end, end_a, end_b, load_ref,
    h_in, cot_ref, routes_ref, combine_ref, pair_ref, len_ref, ratio_ref,
    hr, sa, sb, hs, sas, sbs, cotb, load_out, load_in, relay_h, relay_a, relay_b, raw_a, raw_b, meta_out, meta_in, ht, ht_far,
    in_sem, s_s, up_s, dn_s, cu_s, cd_s, a_r, rw_r, cb_r, b_r, h_r, he_r, rh_r, l_r,
):
    nd, ne, nm, most, ca, cb = dims
    d, e, m = lax.axis_index("dp"), lax.axis_index("expert"), lax.axis_index("mp")
    toks, top, ff = h_in.shape
    half = ff // nd
    side = 1 - d
    ex, ey, eg = e + 1 - 2 * lax.rem(e, 2), lax.rem(e + 2, ne), ne - 1 - e
    first, second = ex + d * (ey - ex), ey + d * (ex - ey)
    dests = (e, first, second, eg)

    def slot(dd, ee):
        return ee * nd + dd

    me = slot(d, e)

    def dev(dd=None, ee=None, mm=None):
        return {"dp": d if dd is None else dd, "expert": e if ee is None else ee, "mp": m if mm is None else mm}

    S_RAW_A, S_META, S_RAW_B, S_A, S_B, S_H, S_Q, S_LOAD = range(8)
    H_OWN, H_FIRST, H_SECOND, H_FAR_FIRST, H_FAR_SECOND, H_DIAG = range(6)

    def remote(src, dst, ssem, rsem, where):
        return pltpu.make_async_remote_copy(
            src_ref=src, dst_ref=dst, send_sem=ssem, recv_sem=rsem, device_id=where, device_id_type=MESH
        )

    def send(src, dst, ssem, rsem, where, go=None):
        copy = remote(src, dst, s_s.at[ssem] if isinstance(ssem, int) else ssem, rsem, where)
        if go is None:
            copy.start()
        else:
            pl.when(go)(copy.start)

    def wait_in(buf, sem, guard=None):
        c = pltpu.make_async_copy(buf, buf, sem)
        if guard is None:
            c.wait()
        else:
            pl.when(guard)(c.wait)

    loads = [
        pltpu.make_async_copy(src, dst, in_sem.at[i])
        for i, (src, dst) in enumerate((
            (routes_hbm, routes_ref), (cot_hbm, cot_ref), (pair_hbm, pair_ref), (len_hbm, len_ref),
            (ratio_hbm, ratio_ref), (combine_hbm, combine_ref), (h_hbm, h_in),
        ))
    ]
    for load in loads:
        load.start()
    barrier = pltpu.get_barrier_semaphore()
    peers = [dev(dd=side)] + [dev(dd=i, ee=to) for i in range(nd) for to in (first, second)]
    for peer in peers:
        pl.semaphore_signal(barrier, inc=1, device_id=peer, device_id_type=MESH)
    has_up, has_down = m + 1 < nm, m > 0
    up, down = dev(mm=lax.rem(m + 1, nm)), dev(mm=lax.rem(m + nm - 1, nm))
    for go, peer in ((has_up, up), (has_down, down)):
        pl.when(go)(
            functools.partial(pl.semaphore_signal, barrier, inc=1, device_id=peer, device_id_type=MESH)
        )
    n_peers = len(peers) + jnp.where(has_up, 1, 0) + jnp.where(has_down, 1, 0)

    loads[0].wait()
    rows8 = -(-ne // 8) * 8
    row_id = lax.broadcasted_iota(jnp.int32, (rows8, 1), 0)
    owner = jnp.full((rows8, 1), -1, jnp.int32)
    for j, to in enumerate(dests):
        owner = jnp.where(row_id == j, to, owner)
    hit0 = routes_ref[0:1, :] == owner
    hit1 = routes_ref[1:2, :] == owner
    named = hit0 | hit1
    before = lax.broadcasted_iota(jnp.int32, (toks, toks), 0) < lax.broadcasted_iota(jnp.int32, (toks, toks), 1)
    tok_rank = jnp.dot(
        jnp.where(named, 1.0, 0.0).astype(jnp.bfloat16),
        jnp.where(before, 1.0, 0.0).astype(jnp.bfloat16),
        preferred_element_type=jnp.float32,
    )
    tok_rank = jnp.where(named, tok_rank, -1.0)
    tok_pos = tok_rank.astype(jnp.int32)

    for load in loads[2:-1]:
        load.wait()

    blocks = pair_ref.shape[1]
    block_len = toks // blocks
    square = (blocks, blocks)
    diagonal = lax.broadcasted_iota(jnp.int32, square, 0) == lax.broadcasted_iota(jnp.int32, square, 1)

    def column(row):
        return jnp.sum(jnp.where(diagonal, row, 0.0), axis=1, keepdims=True)

    pair, ratio = pair_ref[...], ratio_ref[...]
    chosen = lax.rem(pair, 2) == 0
    other_side = jnp.where(chosen, pair + 1, pair - 1)
    is_other = column(pair.astype(jnp.float32)) == other_side.astype(jnp.float32)
    other_ratio = jnp.sum(jnp.where(is_other, column(ratio), 0.0), axis=0, keepdims=True)
    margin = jnp.where(chosen, ratio - other_ratio, other_ratio - ratio)
    coef = beta_scale * (1.0 / (1.0 + jnp.exp(beta_scale * margin)))
    block_weight = column(jnp.where(chosen, -coef, coef))
    token_id = lax.broadcasted_iota(jnp.int32, (blocks, toks), 1)
    place = token_id - block_len * lax.broadcasted_iota(jnp.int32, (blocks, toks), 0)
    inside = (place >= 0) & (place < block_len)
    alive = inside & (place.astype(jnp.float32) < column(len_ref[...].astype(jnp.float32)))
    live = jnp.sum(jnp.where(alive, 1.0, 0.0), axis=0, keepdims=True)
    per_token = jnp.sum(jnp.where(alive, block_weight, 0.0), axis=0, keepdims=True)
    weight = combine_ref[...] * per_token
    tok_weight = jnp.where(hit0, weight[0:1, :], 0.0) + jnp.where(hit1, weight[1:2, :], 0.0)

    loads[1].wait()
    cotb[m] = cot_ref[:, ca:]
    meta_out[...] = jnp.concatenate([tok_rank[:ne], tok_weight[:ne]], axis=0)
    slot_tok = lax.broadcasted_iota(jnp.int32, (most, toks), 0)
    pl.semaphore_wait(barrier, n_peers)
    send(cot_ref.at[:, pl.ds(0, ca)], raw_a, S_RAW_A, rw_r.at[0], dev(ee=first))
    own_cols = cot_ref.at[:, pl.ds(ca, cb)]
    send(own_cols, cotb.at[m], cu_s.at[0], cb_r.at[m], up, has_up)
    send(own_cols, cotb.at[m], cd_s.at[0], cb_r.at[m], down, has_down)
    send(meta_out, meta_in, S_META, rw_r.at[1], dev(ee=first))

    def chain(k):
        return (m - k, lax.rem(m - k + nm, nm), m - k >= 0), (m + k, lax.rem(m + k, nm), m + k < nm)

    def pass_cot(k):
        (_, ql, low_here), (_, qh, high_here) = chain(k)
        for q, here, sem, to, more in ((ql, low_here, cu_s, up, has_up), (qh, high_here, cd_s, down, has_down)):
            wait_in(cotb.at[q], cb_r.at[q], here)
            if k + 1 < nm:
                send(cotb.at[q], cotb.at[q], sem.at[0], cb_r.at[q], to, here & more)

    def picker(position, factor):
        hit = slot_tok == position
        pick = jnp.where(hit, 1.0, 0.0).astype(jnp.bfloat16)
        scale = jnp.sum(jnp.where(hit, factor, 0.0), axis=1, keepdims=True)

        def pack(rows):
            rows = jnp.dot(pick, rows, preferred_element_type=jnp.float32)
            return (scale * rows).astype(jnp.bfloat16)

        return pack

    pack_own = picker(tok_pos[0:1, :], tok_weight[0:1, :])
    sa[m, me] = pack_own(cot_ref[:, :ca])

    def to_partner(q, src, guard=None):
        send(sa.at[q, src], sa.at[q, src], S_A, a_r.at[q, src], dev(dd=side), guard)

    def spread(ej):
        src = slot(d, ej)
        block = sa.at[m, src]
        send(block, block, up_s.at[0], a_r.at[m, src], up, has_up)
        send(block, block, dn_s.at[0], a_r.at[m, src], down, has_down)
        to_partner(m, src)

    def pass_on(k, ej):
        (_, ql, low_here), (_, qh, high_here) = chain(k)
        src = slot(d, ej)
        for q, here, sem, to, more in ((ql, low_here, up_s, up, has_up), (qh, high_here, dn_s, down, has_down)):
            block = sa.at[q, src]
            wait_in(block, a_r.at[q, src], here)
            if k + 1 < nm:
                send(block, block, sem.at[0], a_r.at[q, src], to, here & more)
            to_partner(q, src, here)

    spread(e)
    pack_second = picker(tok_pos[2:3, :], tok_weight[2:3, :])
    sas[...] = pack_second(cot_ref[:, :ca])
    send(sas, sa.at[m, me], S_A, a_r.at[m, me], dev(ee=second))
    in_order = (routes_ref[0:1, :] == row_id) | (routes_ref[1:2, :] == row_id)
    counts = jnp.sum(jnp.where(in_order, live, 0.0), axis=1, keepdims=True)
    lanes8 = lax.broadcasted_iota(jnp.int32, (rows8, LANES), 1) == row_id
    load_out[0] = jnp.broadcast_to(jnp.sum(jnp.where(lanes8, counts, 0.0), axis=0, keepdims=True), (rows8, LANES))
    send(load_out.at[0], load_in.at[0], S_LOAD, l_r.at[0], dev(ee=first))
    send(load_out.at[0], load_in.at[1], S_LOAD, l_r.at[1], dev(ee=second))

    slot_flat = lax.broadcasted_iota(jnp.int32, (most, 2 * toks), 0)
    gap = lax.broadcasted_iota(jnp.int32, (toks, 2 * toks), 1) - 2 * lax.broadcasted_iota(
        jnp.int32, (toks, 2 * toks), 0
    )
    flat_pos = -1.0
    for k, hit in enumerate((hit0, hit1)):
        place_k = jnp.where(gap == k, 1.0, 0.0).astype(jnp.bfloat16)
        value = jnp.where(hit, tok_rank + 1.0, 0.0)
        high = jnp.floor(value * (1.0 / 16.0))
        for part, unit in ((high, 16.0), (value - 16.0 * high, 1.0)):
            flat_pos += unit * jnp.dot(part.astype(jnp.bfloat16), place_k, preferred_element_type=jnp.float32)
    flat_pos = flat_pos.astype(jnp.int32)
    loads[-1].wait()
    flat = (2 * toks, half)
    h_rows = [h_in[:, :, c * half : (c + 1) * half].reshape(flat) for c in range(nd)]

    def pack_h(j):
        pick = jnp.where(slot_flat == flat_pos[j : j + 1, :], 1.0, 0.0).astype(jnp.bfloat16)
        for c in range(nd):
            hs[j, c] = jnp.dot(pick, h_rows[c], preferred_element_type=jnp.float32).astype(jnp.bfloat16)

    whole = most // 256 * 256
    main, rest = pl.ds(0, whole), pl.ds(whole, most - whole)
    pack_h(3)
    for c in range(nd):
        send(hs.at[3, c], relay_h.at[c], S_H, rh_r.at[c], dev(ee=first))
    pass_cot(1)
    pack_h(2)
    wait_in(sa.at[m, slot(d, second)], a_r.at[m, slot(d, second)])
    spread(second)
    wait_in(meta_in, rw_r.at[1])
    wait_in(raw_a, rw_r.at[0])
    from_first = slot(d, first)
    pack_relay = picker(meta_in[3:4, :].astype(jnp.int32), meta_in[ne + 3 : ne + 4, :])
    relay_a[...] = pack_relay(raw_a[...])
    send(relay_a, sa.at[m, from_first], S_A, a_r.at[m, from_first], dev(ee=second))
    wait_in(load_in.at[0], l_r.at[0])
    send(load_in.at[0], load_in.at[2], S_LOAD, l_r.at[2], dev(ee=second))
    send(hs.at[2, d, main], hr.at[me, main], S_Q, h_r.at[H_SECOND], dev(dd=d, ee=second))
    pack_first = picker(meta_in[1:2, :].astype(jnp.int32), meta_in[ne + 1 : ne + 2, :])
    sa[m, from_first] = pack_first(raw_a[...])
    spread(first)
    pack_h(0)
    send(hs.at[0, side], hr.at[me], S_H, h_r.at[H_OWN], dev(dd=side))
    hr[me] = hs[0, d]
    pack_h(1)

    pass_cot(2)
    pass_cot(3)
    send(cotb, raw_b, S_RAW_B, rw_r.at[2], dev(ee=first))
    dense = jnp.concatenate([cotb[q] for q in range(nm)], axis=1)
    sbs[...] = pack_second(dense)
    send(sbs, sb.at[me], S_B, b_r.at[me], dev(ee=second))
    sb[me] = pack_own(dense)
    send(sb.at[me], sb.at[me], S_B, b_r.at[me], dev(dd=side))

    def share_b(ej):
        src = slot(d, ej)
        wait_in(sb.at[src], b_r.at[src])
        send(sb.at[src], sb.at[src], S_B, b_r.at[src], dev(dd=side))

    for c, role in ((d, H_FIRST), (side, H_FAR_FIRST)):
        send(hs.at[1, c], hr.at[me], S_H, h_r.at[role], dev(dd=c, ee=first))

    def nearest(r):
        near = jnp.minimum(m, nm - 1 - m)
        both = m + (r + 1) // 2 * (1 if r % 2 == 0 else -1)
        far = jnp.where(m < nm - 1 - m, m + r - near, m - r + near)
        return jnp.where(r <= 2 * near, both, far)

    def put(ref, index, value, fresh):
        if fresh:
            ref[index] = value
        else:
            ref[index] = ref[index] + value

    def unit(r, left, cut, fresh=False):
        if r < nm:
            q = nearest(r)
            put(acc_a, q, jnp.dot(left[...], cut(sa.at[q]), preferred_element_type=jnp.float32), fresh)
        else:
            put(acc_b, ..., jnp.dot(left[...], cut(sb), preferred_element_type=jnp.float32), fresh)

    def rows_of(s0, s1, at, rows):
        def cut(ref):
            return jnp.concatenate([ref[s0, at : at + rows], ref[s1, at : at + rows]], axis=0)

        return cut

    def turn(s0, s1, at, rows):
        return jnp.concatenate([hr[s0, at : at + rows], hr[s1, at : at + rows]], axis=0).T

    def partner_a(r, ej):
        q = nearest(r)
        src = slot(side, ej)
        wait_in(sa.at[q, src], a_r.at[q, src])

    def partner_b(ej):
        src = slot(side, ej)
        wait_in(sb.at[src], b_r.at[src])

    def wait_h(src, role):
        wait_in(hr.at[src], h_r.at[role])

    def wait_main(src, role):
        wait_in(hr.at[src, main], h_r.at[role])

    B = nm
    own = rows_of(slot(0, e), slot(1, e), 0, whole)
    diag = rows_of(slot(0, eg), slot(1, eg), 0, whole)
    same = rows_of(slot(d, ex), slot(d, ey), 0, whole)

    pass_on(1, e)
    wait_in(sa.at[m, slot(d, eg)], a_r.at[m, slot(d, eg)])
    spread(eg)
    pass_on(1, first)
    pass_on(1, second)
    wait_h(slot(side, e), H_OWN)
    ht[0] = turn(slot(0, e), slot(1, e), 0, whole)
    partner_a(0, e)
    unit(0, ht.at[0], own, True)
    wait_in(relay_h.at[0], rh_r.at[0])
    send(relay_h.at[0, main], hr.at[from_first, main], S_Q, h_r.at[H_DIAG], dev(dd=0, ee=second))
    partner_b(e)
    unit(B, ht.at[0], own, True)
    pass_on(1, eg)
    share_b(second)
    partner_a(1, e)
    unit(1, ht.at[0], own, True)
    for n in (1, 2):
        wait_in(load_in.at[n], l_r.at[n])
    load_out[1] = (load_out[0] + load_in[0]) + (load_in[1] + load_in[2])
    send(load_out.at[1], load_in.at[3], S_LOAD, l_r.at[3], dev(dd=side))
    pass_on(2, e)
    wait_in(relay_h.at[1], rh_r.at[1])
    send(relay_h.at[1, main], hr.at[from_first, main], S_Q, h_r.at[H_DIAG], dev(dd=1, ee=second))
    pass_on(2, first)
    wait_in(raw_b, rw_r.at[2])
    dense = jnp.concatenate([raw_b[q] for q in range(nm)], axis=1)
    relay_b[...] = pack_relay(dense)
    send(relay_b, sb.at[from_first], S_B, b_r.at[from_first], dev(ee=second))
    send(hs.at[2, side, main], hr.at[me, main], S_Q, h_r.at[H_FAR_SECOND], dev(dd=side, ee=second))
    for c in range(nd):
        send(hs.at[2, c, rest], hr.at[me, rest], S_Q, he_r.at[0], dev(dd=c, ee=second))
    for c in range(nd):
        send(relay_h.at[c, rest], hr.at[from_first, rest], S_Q, he_r.at[0], dev(dd=c, ee=second))
    sb[from_first] = pack_first(dense)
    send(sb.at[from_first], sb.at[from_first], S_B, b_r.at[from_first], dev(dd=side))
    pass_on(2, second)
    pass_on(2, eg)
    partner_a(2, e)
    unit(2, ht.at[0], own, True)
    pass_on(3, e)
    partner_a(3, e)
    unit(3, ht.at[0], own, True)
    wait_in(load_in.at[3], l_r.at[3])
    load_ref[...] = load_out[1] + load_in[3]
    wait_h(slot(d, first), H_FIRST)
    wait_main(slot(d, second), H_SECOND)
    ht[2] = turn(slot(d, ex), slot(d, ey), 0, whole)
    for r in range(nm - 1):
        unit(r, ht.at[2], same)
    unit(B, ht.at[2], same)
    pairs = hr.at[pl.ds(slot(0, eg), nd), main]
    wait_in(pairs, h_r.at[H_DIAG])
    ht[1] = turn(slot(0, eg), slot(1, eg), 0, whole)
    for r in range(nm - 1):
        partner_a(r, eg)
        unit(r, ht.at[1], diag)
    share_b(eg)
    partner_b(eg)
    unit(B, ht.at[1], diag)
    ends = (slot(side, second), second), (slot(side, first), first)

    def far(n, r):
        src, ej = ends[n]
        if n == 0 and r == B:
            partner_b(ej)
        elif n == 0 or r == nm - 1:
            partner_a(r, ej)
        unit(r, ht_far.at[n], lambda ref: ref[src, :whole])

    wait_h(ends[0][0], H_FAR_FIRST)
    ht_far[0] = hr[ends[0][0], :whole].T
    for r in (0, 1, 2, B):
        far(0, r)
    pass_on(3, first)
    pass_on(3, second)
    unit(nm - 1, ht.at[2], same)
    far(0, nm - 1)
    depth = nd * ne * (most - whole)

    def keep_end(r):
        q = nearest(r)
        end_a[q] = sa[q, :, whole:, :].reshape(depth, ca)

    for r in range(nm - 1):
        partner_a(r, first)
        keep_end(r)
    partner_b(first)
    end_b[...] = sb[:, whole:, :].reshape(depth, nm * cb)

    def last_unit():
        partner_a(nm - 1, eg)
        unit(nm - 1, ht.at[1], diag)

    middle = has_up & has_down
    pl.when(middle)(last_unit)
    wait_main(ends[1][0], H_FAR_SECOND)
    ht_far[1] = hr[ends[1][0], :whole].T
    far(1, 0)
    far(1, 1)
    pass_on(3, eg)
    for r in (2, B, 3):
        far(1, r)
    pl.when(jnp.logical_not(middle))(last_unit)
    keep_end(nm - 1)
    wait_in(hr.at[pl.ds(0, 2 * nd), rest], he_r.at[0])
    ht_end[...] = hr[:, whole:, :].reshape(depth, half).T

    for ref, sem in (
        (cot_ref.at[:, pl.ds(0, ca)], S_RAW_A), (meta_out, S_META), (cotb, S_RAW_B),
        (sa.at[pl.ds(0, nm - 1), pl.ds(0, ne + 2)], S_A), (sb.at[pl.ds(0, ne + 2)], S_B),
        (hr.at[pl.ds(0, 2 * nd + 1)], S_H), (hr.at[pl.ds(0, 2 * nd)], S_Q),
        (load_in, S_LOAD),
    ):
        wait_in(ref, s_s.at[sem])
    for k in range(nm - 1):
        hops = pl.ds(0, k + 1)
        for at, end, blocks, cols in ((m, nm - 1, up_s, cu_s), (nm - 1 - m, nm - 1, dn_s, cd_s)):
            wait_in(sa.at[hops, pl.ds(0, ne)], blocks.at[0], at == k)
            wait_in(cotb.at[hops], cols.at[0], at == k)


def finish_kernel(
    nm, a_ref, b_ref, ht_ref, end_a, end_b, load_ref, out_ref, total_ref, stage_a, stage_b, sem
):
    ca, cb = a_ref.shape[2], b_ref.shape[1] // nm
    width = ca + cb
    copies = []

    def write(src, rows, at, cols):
        copy = pltpu.make_async_copy(src, out_ref.at[0, rows, pl.ds(at, cols)], sem.at[len(copies)])
        copy.start()
        copies.append(copy)

    def rows_a(q, parts):
        rows = a_ref.shape[1] // parts
        for p in range(parts):
            cut = pl.ds(p * rows, rows)
            stage_a[q, cut] = a_ref[q, cut] + jnp.dot(ht_ref[cut, :], end_a[q], preferred_element_type=jnp.float32)
            write(stage_a.at[q, cut], cut, q * width, ca)

    half = pl.ds(0, b_ref.shape[0])
    rows_a(0, 2)
    stage_b[...] = b_ref[...] + jnp.dot(ht_ref[...], end_b[...], preferred_element_type=jnp.float32)
    for q in range(nm):
        write(stage_b.at[:, pl.ds(q * cb, cb)], half, q * width + ca, cb)
    for q in range(1, nm):
        rows_a(q, 2 if q == nm - 1 else 1)
    total_ref[...] = load_ref[0:1, : total_ref.shape[1]]
    for copy in copies:
        copy.wait()


def fast_body(hidden, cotangent, routes, combine, block_pair, lengths, log_ratio):
    nd, ne, nm = lax.axis_size("dp"), lax.axis_size("expert"), lax.axis_size("mp")
    toks, top, ff = hidden.shape
    width = cotangent.shape[1]
    most = 3 * toks // 4
    cb = width // 4 // LANES * LANES
    ca = width - cb
    half = ff // nd
    srcs = nd * ne
    rows8 = -(-ne // 8) * 8
    whole = most // 256 * 256
    dims = (nd, ne, nm, most, ca, cb)
    bf16, f32 = jnp.bfloat16, jnp.float32
    vmem = pl.BlockSpec(memory_space=pltpu.VMEM)
    hbm = pl.BlockSpec(memory_space=pltpu.HBM)
    dma = pltpu.SemaphoreType.DMA
    depth = srcs * (most - whole)
    results = pl.pallas_call(
        functools.partial(exchange_kernel, dims),
        out_shape=(
            pltpu.VMEM((nm, half, ca), f32),
            pltpu.VMEM((half, nm * cb), f32),
            pltpu.VMEM((half, depth), bf16),
            pltpu.VMEM((nm, depth, ca), bf16),
            pltpu.VMEM((depth, nm * cb), bf16),
            pltpu.VMEM((rows8, LANES), f32),
        ),
        in_specs=[hbm] * 7,
        out_specs=(vmem,) * 6,
        scratch_shapes=[
            pltpu.VMEM((toks, top, ff), bf16),
            pltpu.VMEM(cotangent.shape, bf16),
            pltpu.VMEM((top, toks), jnp.int32),
            pltpu.VMEM((top, toks), f32),
            pltpu.VMEM(block_pair.shape, jnp.int32),
            pltpu.VMEM(lengths.shape, jnp.int32),
            pltpu.VMEM(log_ratio.shape, f32),
            pltpu.VMEM((srcs, most, half), bf16),
            pltpu.VMEM((nm, srcs, most, ca), bf16),
            pltpu.VMEM((srcs, most, nm * cb), bf16),
            pltpu.VMEM((ne, nd, most, half), bf16),
            pltpu.VMEM((most, ca), bf16),
            pltpu.VMEM((most, nm * cb), bf16),
            pltpu.VMEM((nm, toks, cb), bf16),
            pltpu.VMEM((2, rows8, LANES), f32),
            pltpu.VMEM((4, rows8, LANES), f32),
            pltpu.VMEM((nd, most, half), bf16),
            pltpu.VMEM((most, ca), bf16),
            pltpu.VMEM((most, nm * cb), bf16),
            pltpu.VMEM((toks, ca), bf16),
            pltpu.VMEM((nm, toks, cb), bf16),
            pltpu.VMEM((2 * ne, toks), f32),
            pltpu.VMEM((2 * ne, toks), f32),
            pltpu.VMEM((3, half, 2 * whole), bf16),
            pltpu.VMEM((2, half, whole), bf16),
            dma((7,)),
            dma((8,)),
            dma((1,)),
            dma((1,)),
            dma((1,)),
            dma((1,)),
            dma((nm, srcs)),
            dma((3,)),
            dma((nm,)),
            dma((srcs,)),
            dma((6,)),
            dma((1,)),
            dma((nd,)),
            dma((4,)),
        ],
        compiler_params=pltpu.CompilerParams(
            collective_id=0, has_side_effects=True, vmem_limit_bytes=VMEM_MOST - 12 * 1024 * 1024
        ),
    )(hidden, cotangent, routes.T, combine.T, block_pair, lengths, log_ratio)
    grad_down, total = pl.pallas_call(
        functools.partial(finish_kernel, nm),
        out_shape=(jax.ShapeDtypeStruct((1, half, nm * width), f32), jax.ShapeDtypeStruct((1, ne), f32)),
        in_specs=[vmem] * 6,
        out_specs=(hbm, vmem),
        scratch_shapes=[pltpu.VMEM((nm, half, ca), f32), pltpu.VMEM((half, nm * cb), f32), dma((2 * nm + 2,))],
        compiler_params=pltpu.CompilerParams(vmem_limit_bytes=VMEM_MOST // 4),
    )(*results)
    return grad_down, total.reshape(ne)


def plain_body(hidden, cotangent, routes, combine, block_pair, lengths, log_ratio):
    per_token, within = token_factors(block_pair, lengths, log_ratio, LEN)
    weight = combine * per_token[:, None]
    tok_rows = routes.shape[0]
    route_top = routes.shape[1]
    ff_local = hidden.shape[2]
    groups = lax.axis_size("expert")
    experts = groups * EXP_DEV
    most_rows = 3 * tok_rows // 4
    labels = jnp.arange(experts, dtype=jnp.int32)
    routed = routes[:, :, None] == labels[None, None, :]
    local_load = jnp.sum(jnp.where(routed & within[:, None, None], 1.0, 0.0), axis=(0, 1)).astype(
        jnp.float32
    )
    flat_rows = tok_rows * route_top
    flat_hits = routed.reshape(flat_rows, experts).astype(jnp.int32)
    rank_of = jnp.sum((jnp.cumsum(flat_hits, axis=0) - 1) * flat_hits, axis=1)
    slot_of = routes.reshape(flat_rows) * most_rows + rank_of
    source = (
        jnp.zeros((experts * most_rows,), jnp.int32)
        .at[slot_of]
        .set(jnp.arange(flat_rows, dtype=jnp.int32))
    )
    filled = jnp.zeros((experts * most_rows,), jnp.float32).at[slot_of].set(1.0)
    token_of = source // route_top
    slot_weight = jnp.take(weight.reshape(flat_rows), source) * filled
    packed_h = jnp.take(hidden.reshape(flat_rows, ff_local), source, axis=0).reshape(
        groups, EXP_DEV * most_rows, ff_local
    )
    narrow_s = (
        slot_weight[:, None] * jnp.take(cotangent, token_of, axis=0).astype(jnp.float32)
    ).astype(jnp.bfloat16)
    moved_h, narrow = (
        lax.all_to_all(packed_h, "expert", split_axis=0, concat_axis=0, tiled=True),
        lax.all_to_all(
            narrow_s.reshape(groups, EXP_DEV * most_rows, cotangent.shape[1]),
            "expert",
            split_axis=0,
            concat_axis=0,
            tiled=True,
        ),
    )
    moved_s = lax.all_gather(narrow, "mp", axis=2, tiled=True)
    moved_h = moved_h.reshape(groups, EXP_DEV, most_rows, ff_local)
    moved_s = moved_s.reshape(groups, EXP_DEV, most_rows, moved_s.shape[2])
    products = [
        lax.dot_general(
            moved_h[:, 0],
            moved_s[:, 0],
            (((0, 1), (0, 1)), ((), ())),
            preferred_element_type=jnp.float32,
        )
    ]
    owned = lax.psum_scatter(jnp.stack(products, axis=1), "dp", scatter_dimension=0, tiled=True)
    grad_down = jnp.transpose(owned, (1, 0, 2))
    expert_load = lax.psum(local_load, ("dp", "expert"))
    return (grad_down, expert_load)


def solution(mesh):
    in_specs = (
        P(("dp", "expert"), None, "mp"),
        P(("dp", "expert"), "mp"),
        P(("dp", "expert"), None),
        P(("dp", "expert"), None),
        P(("dp", "expert"), None),
        P(("dp", "expert"), None),
        P(("dp", "expert"), None),
    )
    out_specs = (P("expert", ("mp", "dp"), None), P())

    def body(hidden, cotangent, *rest):
        rows = mesh.shape["dp"] * mesh.shape["expert"] * (3 * hidden.shape[0] // 4)
        bytes_in = 2 * rows * (cotangent.shape[1] * mesh.shape["mp"] + hidden.shape[2])
        most = 3 * hidden.shape[0] // 4
        whole = most // 256 * 256
        square = mesh.shape["dp"] == 2 and mesh.shape["expert"] == 4 and mesh.shape["mp"] == 4
        fits = square and whole and 8 * (most - whole) == whole
        run = fast_body if fits and 2 * bytes_in < VMEM_ROOM else plain_body
        return run(hidden, cotangent, *rest)

    return jax.shard_map(body, mesh=mesh, in_specs=in_specs, out_specs=out_specs, check_vma=False)
```

```python
import functools

import jax
import jax.numpy as jnp
from jax import lax
from jax.experimental import pallas as pl
from jax.experimental.pallas import tpu as pltpu
from jax.sharding import PartitionSpec as P

EXP_DEV = 1
LEN = 32
LANES = 128
VMEM_ROOM = 48 * 1024 * 1024
VMEM_MOST = 67043328
MESH = pl.DeviceIdType.MESH


beta_scale = 0.1


def token_factors(block_pair, lengths, log_ratio, block_len):
    blocks = block_pair.shape[1]
    labels = jnp.arange(blocks, dtype=jnp.int32)
    matches = block_pair[:, :, None] == labels[None, None, :]
    by_label = jnp.sum(jnp.where(matches, log_ratio[:, :, None], 0.0), axis=1)
    margin = by_label[:, 0::2] - by_label[:, 1::2]
    pair_coef = beta_scale * jax.nn.sigmoid(-beta_scale * margin)
    owners = block_pair // 2
    pair_ids = jnp.arange(blocks // 2, dtype=jnp.int32)
    picked = owners[:, :, None] == pair_ids[None, None, :]
    block_coef = jnp.sum(jnp.where(picked, pair_coef[:, None, :], 0.0), axis=2)
    block_weight = jnp.where(block_pair % 2 == 0, -block_coef, block_coef)
    position = jnp.arange(block_len, dtype=jnp.int32)
    within = position[None, None, :] < lengths[:, :, None]
    per_token = jnp.where(within, block_weight[:, :, None], 0.0).reshape(-1)
    return per_token, within.reshape(-1)


def exchange_kernel(
    dims, h_hbm, cot_hbm, routes_hbm, combine_hbm, pair_hbm, len_hbm, ratio_hbm,
    acc_a, acc_b, ht_end, end_a, end_b, load_ref,
    h_in, cot_ref, routes_ref, combine_ref, pair_ref, len_ref, ratio_ref,
    hr, sa, sb, hs, sas, sbs, cotb, load_out, load_in, relay_h, relay_a, relay_b, raw_a, raw_b, meta_out, meta_in, ht, ht_far,
    in_sem, s_s, up_s, dn_s, cu_s, cd_s, a_r, rw_r, cb_r, b_r, h_r, he_r, rh_r, l_r,
):
    nd, ne, nm, most, ca, cb = dims
    d, e, m = lax.axis_index("dp"), lax.axis_index("expert"), lax.axis_index("mp")
    toks, top, ff = h_in.shape
    half = ff // nd
    side = 1 - d
    ex, ey, eg = e + 1 - 2 * lax.rem(e, 2), lax.rem(e + 2, ne), ne - 1 - e
    first, second = ex + d * (ey - ex), ey + d * (ex - ey)
    dests = (e, first, second, eg)

    def slot(dd, ee):
        return ee * nd + dd

    me = slot(d, e)

    def dev(dd=None, ee=None, mm=None):
        return {"dp": d if dd is None else dd, "expert": e if ee is None else ee, "mp": m if mm is None else mm}

    S_RAW_A, S_META, S_RAW_B, S_A, S_B, S_H, S_Q, S_LOAD = range(8)
    H_OWN, H_FIRST, H_SECOND, H_FAR_FIRST, H_FAR_SECOND, H_DIAG = range(6)

    def remote(src, dst, ssem, rsem, where):
        return pltpu.make_async_remote_copy(
            src_ref=src, dst_ref=dst, send_sem=ssem, recv_sem=rsem, device_id=where, device_id_type=MESH
        )

    def send(src, dst, ssem, rsem, where, go=None):
        copy = remote(src, dst, s_s.at[ssem] if isinstance(ssem, int) else ssem, rsem, where)
        if go is None:
            copy.start()
        else:
            pl.when(go)(copy.start)

    def wait_in(buf, sem, guard=None):
        c = pltpu.make_async_copy(buf, buf, sem)
        if guard is None:
            c.wait()
        else:
            pl.when(guard)(c.wait)

    loads = [
        pltpu.make_async_copy(src, dst, in_sem.at[i])
        for i, (src, dst) in enumerate((
            (routes_hbm, routes_ref), (cot_hbm, cot_ref), (pair_hbm, pair_ref), (len_hbm, len_ref),
            (ratio_hbm, ratio_ref), (combine_hbm, combine_ref), (h_hbm, h_in),
        ))
    ]
    for load in loads:
        load.start()
    barrier = pltpu.get_barrier_semaphore()
    peers = [dev(dd=side)] + [dev(dd=i, ee=to) for i in range(nd) for to in (first, second)]
    for peer in peers:
        pl.semaphore_signal(barrier, inc=1, device_id=peer, device_id_type=MESH)
    has_up, has_down = m + 1 < nm, m > 0
    up, down = dev(mm=lax.rem(m + 1, nm)), dev(mm=lax.rem(m + nm - 1, nm))
    for go, peer in ((has_up, up), (has_down, down)):
        pl.when(go)(
            functools.partial(pl.semaphore_signal, barrier, inc=1, device_id=peer, device_id_type=MESH)
        )
    n_peers = len(peers) + jnp.where(has_up, 1, 0) + jnp.where(has_down, 1, 0)

    loads[0].wait()
    rows8 = -(-ne // 8) * 8
    row_id = lax.broadcasted_iota(jnp.int32, (rows8, 1), 0)
    owner = jnp.full((rows8, 1), -1, jnp.int32)
    for j, to in enumerate(dests):
        owner = jnp.where(row_id == j, to, owner)
    hit0 = routes_ref[0:1, :] == owner
    hit1 = routes_ref[1:2, :] == owner
    named = hit0 | hit1
    before = lax.broadcasted_iota(jnp.int32, (toks, toks), 0) < lax.broadcasted_iota(jnp.int32, (toks, toks), 1)
    tok_rank = jnp.dot(
        jnp.where(named, 1.0, 0.0).astype(jnp.bfloat16),
        jnp.where(before, 1.0, 0.0).astype(jnp.bfloat16),
        preferred_element_type=jnp.float32,
    )
    tok_rank = jnp.where(named, tok_rank, -1.0)
    tok_pos = tok_rank.astype(jnp.int32)

    for load in loads[2:-1]:
        load.wait()

    blocks = pair_ref.shape[1]
    block_len = toks // blocks
    square = (blocks, blocks)
    diagonal = lax.broadcasted_iota(jnp.int32, square, 0) == lax.broadcasted_iota(jnp.int32, square, 1)

    def column(row):
        return jnp.sum(jnp.where(diagonal, row, 0.0), axis=1, keepdims=True)

    pair, ratio = pair_ref[...], ratio_ref[...]
    chosen = lax.rem(pair, 2) == 0
    other_side = jnp.where(chosen, pair + 1, pair - 1)
    is_other = column(pair.astype(jnp.float32)) == other_side.astype(jnp.float32)
    other_ratio = jnp.sum(jnp.where(is_other, column(ratio), 0.0), axis=0, keepdims=True)
    margin = jnp.where(chosen, ratio - other_ratio, other_ratio - ratio)
    coef = beta_scale * (1.0 / (1.0 + jnp.exp(beta_scale * margin)))
    block_weight = column(jnp.where(chosen, -coef, coef))
    token_id = lax.broadcasted_iota(jnp.int32, (blocks, toks), 1)
    place = token_id - block_len * lax.broadcasted_iota(jnp.int32, (blocks, toks), 0)
    inside = (place >= 0) & (place < block_len)
    alive = inside & (place.astype(jnp.float32) < column(len_ref[...].astype(jnp.float32)))
    live = jnp.sum(jnp.where(alive, 1.0, 0.0), axis=0, keepdims=True)
    per_token = jnp.sum(jnp.where(alive, block_weight, 0.0), axis=0, keepdims=True)
    weight = combine_ref[...] * per_token
    tok_weight = jnp.where(hit0, weight[0:1, :], 0.0) + jnp.where(hit1, weight[1:2, :], 0.0)

    loads[1].wait()
    cotb[m] = cot_ref[:, ca:]
    meta_out[...] = jnp.concatenate([tok_rank[:ne], tok_weight[:ne]], axis=0)
    slot_tok = lax.broadcasted_iota(jnp.int32, (most, toks), 0)
    pl.semaphore_wait(barrier, n_peers)
    send(cot_ref.at[:, pl.ds(0, ca)], raw_a, S_RAW_A, rw_r.at[0], dev(ee=first))
    own_cols = cot_ref.at[:, pl.ds(ca, cb)]
    send(own_cols, cotb.at[m], cu_s.at[0], cb_r.at[m], up, has_up)
    send(own_cols, cotb.at[m], cd_s.at[0], cb_r.at[m], down, has_down)
    send(meta_out, meta_in, S_META, rw_r.at[1], dev(ee=first))

    def chain(k):
        return (m - k, lax.rem(m - k + nm, nm), m - k >= 0), (m + k, lax.rem(m + k, nm), m + k < nm)

    def pass_cot(k):
        (_, ql, low_here), (_, qh, high_here) = chain(k)
        for q, here, sem, to, more in ((ql, low_here, cu_s, up, has_up), (qh, high_here, cd_s, down, has_down)):
            wait_in(cotb.at[q], cb_r.at[q], here)
            if k + 1 < nm:
                send(cotb.at[q], cotb.at[q], sem.at[0], cb_r.at[q], to, here & more)

    def picker(position, factor):
        hit = slot_tok == position
        pick = jnp.where(hit, 1.0, 0.0).astype(jnp.bfloat16)
        scale = jnp.sum(jnp.where(hit, factor, 0.0), axis=1, keepdims=True)

        def pack(rows):
            rows = jnp.dot(pick, rows, preferred_element_type=jnp.float32)
            return (scale * rows).astype(jnp.bfloat16)

        return pack

    pack_own = picker(tok_pos[0:1, :], tok_weight[0:1, :])
    sa[m, me] = pack_own(cot_ref[:, :ca])

    def to_partner(q, src, guard=None):
        send(sa.at[q, src], sa.at[q, src], S_A, a_r.at[q, src], dev(dd=side), guard)

    def spread(ej):
        src = slot(d, ej)
        block = sa.at[m, src]
        send(block, block, up_s.at[0], a_r.at[m, src], up, has_up)
        send(block, block, dn_s.at[0], a_r.at[m, src], down, has_down)
        to_partner(m, src)

    def pass_on(k, ej):
        (_, ql, low_here), (_, qh, high_here) = chain(k)
        src = slot(d, ej)
        for q, here, sem, to, more in ((ql, low_here, up_s, up, has_up), (qh, high_here, dn_s, down, has_down)):
            block = sa.at[q, src]
            wait_in(block, a_r.at[q, src], here)
            if k + 1 < nm:
                send(block, block, sem.at[0], a_r.at[q, src], to, here & more)
            to_partner(q, src, here)

    spread(e)
    pack_second = picker(tok_pos[2:3, :], tok_weight[2:3, :])
    sas[...] = pack_second(cot_ref[:, :ca])
    send(sas, sa.at[m, me], S_A, a_r.at[m, me], dev(ee=second))
    in_order = (routes_ref[0:1, :] == row_id) | (routes_ref[1:2, :] == row_id)
    counts = jnp.sum(jnp.where(in_order, live, 0.0), axis=1, keepdims=True)
    lanes8 = lax.broadcasted_iota(jnp.int32, (rows8, LANES), 1) == row_id
    load_out[0] = jnp.broadcast_to(jnp.sum(jnp.where(lanes8, counts, 0.0), axis=0, keepdims=True), (rows8, LANES))
    send(load_out.at[0], load_in.at[0], S_LOAD, l_r.at[0], dev(ee=first))
    send(load_out.at[0], load_in.at[1], S_LOAD, l_r.at[1], dev(ee=second))

    slot_flat = lax.broadcasted_iota(jnp.int32, (most, 2 * toks), 0)
    gap = lax.broadcasted_iota(jnp.int32, (toks, 2 * toks), 1) - 2 * lax.broadcasted_iota(
        jnp.int32, (toks, 2 * toks), 0
    )
    flat_pos = -1.0
    for k, hit in enumerate((hit0, hit1)):
        place_k = jnp.where(gap == k, 1.0, 0.0).astype(jnp.bfloat16)
        value = jnp.where(hit, tok_rank + 1.0, 0.0)
        high = jnp.floor(value * (1.0 / 16.0))
        for part, unit in ((high, 16.0), (value - 16.0 * high, 1.0)):
            flat_pos += unit * jnp.dot(part.astype(jnp.bfloat16), place_k, preferred_element_type=jnp.float32)
    flat_pos = flat_pos.astype(jnp.int32)
    loads[-1].wait()
    flat = (2 * toks, half)
    h_rows = [h_in[:, :, c * half : (c + 1) * half].reshape(flat) for c in range(nd)]

    def pack_h(j):
        pick = jnp.where(slot_flat == flat_pos[j : j + 1, :], 1.0, 0.0).astype(jnp.bfloat16)
        for c in range(nd):
            hs[j, c] = jnp.dot(pick, h_rows[c], preferred_element_type=jnp.float32).astype(jnp.bfloat16)

    whole = most // 256 * 256
    main, rest = pl.ds(0, whole), pl.ds(whole, most - whole)
    pack_h(3)
    for c in range(nd):
        send(hs.at[3, c], relay_h.at[c], S_H, rh_r.at[c], dev(ee=first))
    pass_cot(1)
    pack_h(2)
    wait_in(sa.at[m, slot(d, second)], a_r.at[m, slot(d, second)])
    spread(second)
    wait_in(meta_in, rw_r.at[1])
    wait_in(raw_a, rw_r.at[0])
    from_first = slot(d, first)
    pack_relay = picker(meta_in[3:4, :].astype(jnp.int32), meta_in[ne + 3 : ne + 4, :])
    relay_a[...] = pack_relay(raw_a[...])
    send(relay_a, sa.at[m, from_first], S_A, a_r.at[m, from_first], dev(ee=second))
    wait_in(load_in.at[0], l_r.at[0])
    send(load_in.at[0], load_in.at[2], S_LOAD, l_r.at[2], dev(ee=second))
    send(hs.at[2, d, main], hr.at[me, main], S_Q, h_r.at[H_SECOND], dev(dd=d, ee=second))
    pack_first = picker(meta_in[1:2, :].astype(jnp.int32), meta_in[ne + 1 : ne + 2, :])
    sa[m, from_first] = pack_first(raw_a[...])
    spread(first)
    pack_h(0)
    send(hs.at[0, side], hr.at[me], S_H, h_r.at[H_OWN], dev(dd=side))
    hr[me] = hs[0, d]
    pack_h(1)

    pass_cot(2)
    pass_cot(3)
    send(cotb, raw_b, S_RAW_B, rw_r.at[2], dev(ee=first))
    dense = jnp.concatenate([cotb[q] for q in range(nm)], axis=1)
    sbs[...] = pack_second(dense)
    send(sbs, sb.at[me], S_B, b_r.at[me], dev(ee=second))
    sb[me] = pack_own(dense)
    send(sb.at[me], sb.at[me], S_B, b_r.at[me], dev(dd=side))

    def share_b(ej):
        src = slot(d, ej)
        wait_in(sb.at[src], b_r.at[src])
        send(sb.at[src], sb.at[src], S_B, b_r.at[src], dev(dd=side))

    for c, role in ((d, H_FIRST), (side, H_FAR_FIRST)):
        send(hs.at[1, c], hr.at[me], S_H, h_r.at[role], dev(dd=c, ee=first))

    def nearest(r):
        near = jnp.minimum(m, nm - 1 - m)
        both = m + (r + 1) // 2 * (1 if r % 2 == 0 else -1)
        far = jnp.where(m < nm - 1 - m, m + r - near, m - r + near)
        return jnp.where(r <= 2 * near, both, far)

    def put(ref, index, value, fresh):
        if fresh:
            ref[index] = value
        else:
            ref[index] = ref[index] + value

    def unit(r, left, cut, fresh=False):
        if r < nm:
            q = nearest(r)
            put(acc_a, q, jnp.dot(left[...], cut(sa.at[q]), preferred_element_type=jnp.float32), fresh)
        else:
            put(acc_b, ..., jnp.dot(left[...], cut(sb), preferred_element_type=jnp.float32), fresh)

    def rows_of(s0, s1, at, rows):
        def cut(ref):
            return jnp.concatenate([ref[s0, at : at + rows], ref[s1, at : at + rows]], axis=0)

        return cut

    def turn(s0, s1, at, rows):
        return jnp.concatenate([hr[s0, at : at + rows], hr[s1, at : at + rows]], axis=0).T

    def partner_a(r, ej):
        q = nearest(r)
        src = slot(side, ej)
        wait_in(sa.at[q, src], a_r.at[q, src])

    def partner_b(ej):
        src = slot(side, ej)
        wait_in(sb.at[src], b_r.at[src])

    def wait_h(src, role):
        wait_in(hr.at[src], h_r.at[role])

    def wait_main(src, role):
        wait_in(hr.at[src, main], h_r.at[role])

    B = nm
    own = rows_of(slot(0, e), slot(1, e), 0, whole)
    diag = rows_of(slot(0, eg), slot(1, eg), 0, whole)
    same = rows_of(slot(d, ex), slot(d, ey), 0, whole)

    pass_on(1, e)
    wait_in(sa.at[m, slot(d, eg)], a_r.at[m, slot(d, eg)])
    spread(eg)
    pass_on(1, first)
    pass_on(1, second)
    wait_h(slot(side, e), H_OWN)
    ht[0] = turn(slot(0, e), slot(1, e), 0, whole)
    partner_a(0, e)
    unit(0, ht.at[0], own, True)
    wait_in(relay_h.at[0], rh_r.at[0])
    send(relay_h.at[0, main], hr.at[from_first, main], S_Q, h_r.at[H_DIAG], dev(dd=0, ee=second))
    partner_b(e)
    unit(B, ht.at[0], own, True)
    pass_on(1, eg)
    share_b(second)
    partner_a(1, e)
    unit(1, ht.at[0], own, True)
    for n in (1, 2):
        wait_in(load_in.at[n], l_r.at[n])
    load_out[1] = (load_out[0] + load_in[0]) + (load_in[1] + load_in[2])
    send(load_out.at[1], load_in.at[3], S_LOAD, l_r.at[3], dev(dd=side))
    pass_on(2, e)
    wait_in(relay_h.at[1], rh_r.at[1])
    send(relay_h.at[1, main], hr.at[from_first, main], S_Q, h_r.at[H_DIAG], dev(dd=1, ee=second))
    pass_on(2, first)
    wait_in(raw_b, rw_r.at[2])
    dense = jnp.concatenate([raw_b[q] for q in range(nm)], axis=1)
    relay_b[...] = pack_relay(dense)
    send(relay_b, sb.at[from_first], S_B, b_r.at[from_first], dev(ee=second))
    send(hs.at[2, side, main], hr.at[me, main], S_Q, h_r.at[H_FAR_SECOND], dev(dd=side, ee=second))
    for c in range(nd):
        send(hs.at[2, c, rest], hr.at[me, rest], S_Q, he_r.at[0], dev(dd=c, ee=second))
    for c in range(nd):
        send(relay_h.at[c, rest], hr.at[from_first, rest], S_Q, he_r.at[0], dev(dd=c, ee=second))
    sb[from_first] = pack_first(dense)
    send(sb.at[from_first], sb.at[from_first], S_B, b_r.at[from_first], dev(dd=side))
    pass_on(2, second)
    pass_on(2, eg)
    partner_a(2, e)
    unit(2, ht.at[0], own, True)
    pass_on(3, e)
    wait_in(load_in.at[3], l_r.at[3])
    load_ref[...] = load_out[1] + load_in[3]
    wait_h(slot(d, first), H_FIRST)
    wait_main(slot(d, second), H_SECOND)
    ht[2] = turn(slot(d, ex), slot(d, ey), 0, whole)
    for r in range(nm - 1):
        unit(r, ht.at[2], same)
    unit(B, ht.at[2], same)
    partner_a(3, e)
    unit(3, ht.at[0], own, True)
    pairs = hr.at[pl.ds(slot(0, eg), nd), main]
    wait_in(pairs, h_r.at[H_DIAG])
    ht[1] = turn(slot(0, eg), slot(1, eg), 0, whole)
    for r in range(nm - 1):
        partner_a(r, eg)
        unit(r, ht.at[1], diag)
    share_b(eg)
    pass_on(3, first)

    def diag_b():
        partner_b(eg)
        unit(B, ht.at[1], diag)

    pl.when(d == 1)(diag_b)
    ends = (slot(side, second), second), (slot(side, first), first)

    def far(n, r):
        src, ej = ends[n]
        if n == 0 and r == B:
            partner_b(ej)
        elif n == 0 or r == nm - 1:
            partner_a(r, ej)
        unit(r, ht_far.at[n], lambda ref: ref[src, :whole])

    wait_h(ends[0][0], H_FAR_FIRST)
    ht_far[0] = hr[ends[0][0], :whole].T
    for r in (0, 1, 2, B):
        far(0, r)
    pl.when(d == 0)(diag_b)
    pass_on(3, second)
    unit(nm - 1, ht.at[2], same)
    far(0, nm - 1)
    depth = nd * ne * (most - whole)

    def keep_end(r):
        q = nearest(r)
        end_a[q] = sa[q, :, whole:, :].reshape(depth, ca)

    for r in range(nm - 1):
        partner_a(r, first)
        keep_end(r)
    partner_b(first)
    end_b[...] = sb[:, whole:, :].reshape(depth, nm * cb)

    def last_unit():
        partner_a(nm - 1, eg)
        unit(nm - 1, ht.at[1], diag)

    middle = has_up & has_down
    pl.when(middle)(last_unit)
    wait_main(ends[1][0], H_FAR_SECOND)
    ht_far[1] = hr[ends[1][0], :whole].T
    far(1, 0)
    far(1, 1)
    pass_on(3, eg)
    for r in (2, B, 3):
        far(1, r)
    pl.when(jnp.logical_not(middle))(last_unit)
    keep_end(nm - 1)
    wait_in(hr.at[pl.ds(0, 2 * nd), rest], he_r.at[0])
    ht_end[...] = hr[:, whole:, :].reshape(depth, half).T

    for ref, sem in (
        (cot_ref.at[:, pl.ds(0, ca)], S_RAW_A), (meta_out, S_META), (cotb, S_RAW_B),
        (sa.at[pl.ds(0, nm - 1), pl.ds(0, ne + 2)], S_A), (sb.at[pl.ds(0, ne + 2)], S_B),
        (hr.at[pl.ds(0, 2 * nd + 1)], S_H), (hr.at[pl.ds(0, 2 * nd)], S_Q),
        (load_in, S_LOAD),
    ):
        wait_in(ref, s_s.at[sem])
    for k in range(nm - 1):
        hops = pl.ds(0, k + 1)
        for at, end, blocks, cols in ((m, nm - 1, up_s, cu_s), (nm - 1 - m, nm - 1, dn_s, cd_s)):
            wait_in(sa.at[hops, pl.ds(0, ne)], blocks.at[0], at == k)
            wait_in(cotb.at[hops], cols.at[0], at == k)


def finish_kernel(
    nm, a_ref, b_ref, ht_ref, end_a, end_b, load_ref, out_ref, total_ref, stage_a, stage_b, sem
):
    ca, cb = a_ref.shape[2], b_ref.shape[1] // nm
    width = ca + cb
    copies = []

    def write(src, rows, at, cols):
        copy = pltpu.make_async_copy(src, out_ref.at[0, rows, pl.ds(at, cols)], sem.at[len(copies)])
        copy.start()
        copies.append(copy)

    def rows_a(q, parts):
        rows = a_ref.shape[1] // parts
        for p in range(parts):
            cut = pl.ds(p * rows, rows)
            stage_a[q, cut] = a_ref[q, cut] + jnp.dot(ht_ref[cut, :], end_a[q], preferred_element_type=jnp.float32)
            write(stage_a.at[q, cut], cut, q * width, ca)

    half = pl.ds(0, b_ref.shape[0])
    rows_a(0, 2)
    stage_b[...] = b_ref[...] + jnp.dot(ht_ref[...], end_b[...], preferred_element_type=jnp.float32)
    for q in range(nm):
        write(stage_b.at[:, pl.ds(q * cb, cb)], half, q * width + ca, cb)
    for q in range(1, nm):
        rows_a(q, 2 if q == nm - 1 else 1)
    total_ref[...] = load_ref[0:1, : total_ref.shape[1]]
    for copy in copies:
        copy.wait()


def fast_body(hidden, cotangent, routes, combine, block_pair, lengths, log_ratio):
    nd, ne, nm = lax.axis_size("dp"), lax.axis_size("expert"), lax.axis_size("mp")
    toks, top, ff = hidden.shape
    width = cotangent.shape[1]
    most = 3 * toks // 4
    cb = width // 4 // LANES * LANES
    ca = width - cb
    half = ff // nd
    srcs = nd * ne
    rows8 = -(-ne // 8) * 8
    whole = most // 256 * 256
    dims = (nd, ne, nm, most, ca, cb)
    bf16, f32 = jnp.bfloat16, jnp.float32
    vmem = pl.BlockSpec(memory_space=pltpu.VMEM)
    hbm = pl.BlockSpec(memory_space=pltpu.HBM)
    dma = pltpu.SemaphoreType.DMA
    depth = srcs * (most - whole)
    results = pl.pallas_call(
        functools.partial(exchange_kernel, dims),
        out_shape=(
            pltpu.VMEM((nm, half, ca), f32),
            pltpu.VMEM((half, nm * cb), f32),
            pltpu.VMEM((half, depth), bf16),
            pltpu.VMEM((nm, depth, ca), bf16),
            pltpu.VMEM((depth, nm * cb), bf16),
            pltpu.VMEM((rows8, LANES), f32),
        ),
        in_specs=[hbm] * 7,
        out_specs=(vmem,) * 6,
        scratch_shapes=[
            pltpu.VMEM((toks, top, ff), bf16),
            pltpu.VMEM(cotangent.shape, bf16),
            pltpu.VMEM((top, toks), jnp.int32),
            pltpu.VMEM((top, toks), f32),
            pltpu.VMEM(block_pair.shape, jnp.int32),
            pltpu.VMEM(lengths.shape, jnp.int32),
            pltpu.VMEM(log_ratio.shape, f32),
            pltpu.VMEM((srcs, most, half), bf16),
            pltpu.VMEM((nm, srcs, most, ca), bf16),
            pltpu.VMEM((srcs, most, nm * cb), bf16),
            pltpu.VMEM((ne, nd, most, half), bf16),
            pltpu.VMEM((most, ca), bf16),
            pltpu.VMEM((most, nm * cb), bf16),
            pltpu.VMEM((nm, toks, cb), bf16),
            pltpu.VMEM((2, rows8, LANES), f32),
            pltpu.VMEM((4, rows8, LANES), f32),
            pltpu.VMEM((nd, most, half), bf16),
            pltpu.VMEM((most, ca), bf16),
            pltpu.VMEM((most, nm * cb), bf16),
            pltpu.VMEM((toks, ca), bf16),
            pltpu.VMEM((nm, toks, cb), bf16),
            pltpu.VMEM((2 * ne, toks), f32),
            pltpu.VMEM((2 * ne, toks), f32),
            pltpu.VMEM((3, half, 2 * whole), bf16),
            pltpu.VMEM((2, half, whole), bf16),
            dma((7,)),
            dma((8,)),
            dma((1,)),
            dma((1,)),
            dma((1,)),
            dma((1,)),
            dma((nm, srcs)),
            dma((3,)),
            dma((nm,)),
            dma((srcs,)),
            dma((6,)),
            dma((1,)),
            dma((nd,)),
            dma((4,)),
        ],
        compiler_params=pltpu.CompilerParams(
            collective_id=0, has_side_effects=True, vmem_limit_bytes=VMEM_MOST - 12 * 1024 * 1024
        ),
    )(hidden, cotangent, routes.T, combine.T, block_pair, lengths, log_ratio)
    grad_down, total = pl.pallas_call(
        functools.partial(finish_kernel, nm),
        out_shape=(jax.ShapeDtypeStruct((1, half, nm * width), f32), jax.ShapeDtypeStruct((1, ne), f32)),
        in_specs=[vmem] * 6,
        out_specs=(hbm, vmem),
        scratch_shapes=[pltpu.VMEM((nm, half, ca), f32), pltpu.VMEM((half, nm * cb), f32), dma((2 * nm + 2,))],
        compiler_params=pltpu.CompilerParams(vmem_limit_bytes=VMEM_MOST // 4),
    )(*results)
    return grad_down, total.reshape(ne)


def plain_body(hidden, cotangent, routes, combine, block_pair, lengths, log_ratio):
    per_token, within = token_factors(block_pair, lengths, log_ratio, LEN)
    weight = combine * per_token[:, None]
    tok_rows = routes.shape[0]
    route_top = routes.shape[1]
    ff_local = hidden.shape[2]
    groups = lax.axis_size("expert")
    experts = groups * EXP_DEV
    most_rows = 3 * tok_rows // 4
    labels = jnp.arange(experts, dtype=jnp.int32)
    routed = routes[:, :, None] == labels[None, None, :]
    local_load = jnp.sum(jnp.where(routed & within[:, None, None], 1.0, 0.0), axis=(0, 1)).astype(
        jnp.float32
    )
    flat_rows = tok_rows * route_top
    flat_hits = routed.reshape(flat_rows, experts).astype(jnp.int32)
    rank_of = jnp.sum((jnp.cumsum(flat_hits, axis=0) - 1) * flat_hits, axis=1)
    slot_of = routes.reshape(flat_rows) * most_rows + rank_of
    source = (
        jnp.zeros((experts * most_rows,), jnp.int32)
        .at[slot_of]
        .set(jnp.arange(flat_rows, dtype=jnp.int32))
    )
    filled = jnp.zeros((experts * most_rows,), jnp.float32).at[slot_of].set(1.0)
    token_of = source // route_top
    slot_weight = jnp.take(weight.reshape(flat_rows), source) * filled
    packed_h = jnp.take(hidden.reshape(flat_rows, ff_local), source, axis=0).reshape(
        groups, EXP_DEV * most_rows, ff_local
    )
    narrow_s = (
        slot_weight[:, None] * jnp.take(cotangent, token_of, axis=0).astype(jnp.float32)
    ).astype(jnp.bfloat16)
    moved_h, narrow = (
        lax.all_to_all(packed_h, "expert", split_axis=0, concat_axis=0, tiled=True),
        lax.all_to_all(
            narrow_s.reshape(groups, EXP_DEV * most_rows, cotangent.shape[1]),
            "expert",
            split_axis=0,
            concat_axis=0,
            tiled=True,
        ),
    )
    moved_s = lax.all_gather(narrow, "mp", axis=2, tiled=True)
    moved_h = moved_h.reshape(groups, EXP_DEV, most_rows, ff_local)
    moved_s = moved_s.reshape(groups, EXP_DEV, most_rows, moved_s.shape[2])
    products = [
        lax.dot_general(
            moved_h[:, 0],
            moved_s[:, 0],
            (((0, 1), (0, 1)), ((), ())),
            preferred_element_type=jnp.float32,
        )
    ]
    owned = lax.psum_scatter(jnp.stack(products, axis=1), "dp", scatter_dimension=0, tiled=True)
    grad_down = jnp.transpose(owned, (1, 0, 2))
    expert_load = lax.psum(local_load, ("dp", "expert"))
    return (grad_down, expert_load)


def solution(mesh):
    in_specs = (
        P(("dp", "expert"), None, "mp"),
        P(("dp", "expert"), "mp"),
        P(("dp", "expert"), None),
        P(("dp", "expert"), None),
        P(("dp", "expert"), None),
        P(("dp", "expert"), None),
        P(("dp", "expert"), None),
    )
    out_specs = (P("expert", ("mp", "dp"), None), P())

    def body(hidden, cotangent, *rest):
        rows = mesh.shape["dp"] * mesh.shape["expert"] * (3 * hidden.shape[0] // 4)
        bytes_in = 2 * rows * (cotangent.shape[1] * mesh.shape["mp"] + hidden.shape[2])
        most = 3 * hidden.shape[0] // 4
        whole = most // 256 * 256
        square = mesh.shape["dp"] == 2 and mesh.shape["expert"] == 4 and mesh.shape["mp"] == 4
        fits = square and whole and 8 * (most - whole) == whole
        run = fast_body if fits and 2 * bytes_in < VMEM_ROOM else plain_body
        return run(hidden, cotangent, *rest)

    return jax.shard_map(body, mesh=mesh, in_specs=in_specs, out_specs=out_specs, check_vma=False)
```
